32 devices in a mesh: dp: 8 (over z, x), rep: 4 (over y, core).
Axes of the slice: x: 2, y: 2, z: 4, core: 2. Of those that a mesh axis runs over, the one named last changes fastest.
Arguments:
- features: bfloat16 [5120, 8192], P('dp', 'rep'), may hold values from -6 to 6
- out_grads: bfloat16 [5120, 1024], P('dp'), may hold values from -12 to 12, as said below
- cold_sums: bfloat16 [8, 8192, 1024], P('dp', 'rep'), may hold values from -96 to 96
- weight: float32 [8192, 1024], P(('rep', 'dp')), may hold values from -3 to 3
- moment: float32 [8192, 1024], P(('rep', 'dp')), may hold values from -6 to 6
- second: float32 [8192, 1024], P(('rep', 'dp')), may hold values from 0.01 to 4
- ranks: int32 [8], replicated, may hold values from 0 to 7, each once
Outputs:
- new_weight: float32 [8192, 1024], P(('rep', 'dp'))
- new_moment: float32 [8192, 1024], P(('rep', 'dp'))
- new_second: float32 [8192, 1024], P(('rep', 'dp'))
- new_cold: bfloat16 [8, 8192, 1024], P('dp', 'rep')
- column_sq: float32 [1024], replicated
The draws below stay inside these ranges and needn't reach their ends.
Inputs may be any that keep to these rules, and one draw needn't show every extreme that they name: `ranks`: each block number appears once. `out_grads`: column scales differ from column to column.
All inputs are finite; a program needn't handle non-finite values.
Results may differ from the reference program's by a relative error of at most 0.001.
Values sent between devices are 32-bit elements; how exact they have to be, the bound alone decides.
A program may use at most 128 MiB of HBM per device.

```python
import math
import jax
import jax.numpy as jnp
from jax import lax

D = 8192
C = 1024
TOK_DEV = 640
BLOCK = 128
NB = 8
HOT = 4
TOKENS = 5120
N_DP = 8


def draw_out_grads(key, part):
    first, second_key = jax.random.split(key, 2)
    base = jax.random.normal(first, (TOKENS, C), jnp.float32)
    col_scale = jnp.exp(jax.random.uniform(second_key, (1, C), jnp.float32, -1.4, 1.4))
    values = base * col_scale
    return jnp.clip(values, -12.0, 12.0).astype(jnp.bfloat16)


def level_of(key, shape, pieces, smallest, high):
    level, own = 1.0, jax.random.fold_in(key, 6)
    for position, shards_of in pieces:
        heights = jnp.exp(jax.random.uniform(jax.random.fold_in(own, position), (shards_of,), jnp.float32, smallest / len(pieces), high / len(pieces)))
        level = level * jnp.repeat(heights, shape[position] // shards_of).reshape([-1 if axis == position else 1 for axis in range(len(shape))])
    return level


def centred(key, dims, width, bound, cuts=(), dtype=jnp.bfloat16):
    gain = level_of(key, dims, cuts, -0.22, 0.18) if cuts else 1.0
    result = jax.random.normal(key, dims, jnp.float32) * width * gain
    return jnp.minimum(jnp.maximum(result, -bound), bound).astype(dtype)


def setup_inputs(seed: int = 0) -> dict:
    keys = jax.random.split(jax.random.key(seed), 8)
    return {
        "features": centred(keys[0], (TOKENS, D), 1.0, 6.0, ((0, 8), (1, 4))),
        "out_grads": draw_out_grads(jax.random.fold_in(keys[7], 71), 0),
        "cold_sums": centred(keys[2], (N_DP, D, C), 16.0, 96.0, ((0, 8), (1, 4))),
        "weight": centred(keys[3], (D, C), 0.5, 3.0, ((0, 32),), jnp.float32),
        "moment": centred(keys[4], (D, C), 1.0, 6.0, ((0, 32),), jnp.float32),
        "second": jnp.clip(jnp.exp(math.log(4.0) - 5.9914646 * jax.random.uniform(keys[5], (D, C), jnp.float32) ** level_of(keys[5], (D, C), ((0, 32),), -0.2, 0.2)), 0.01, 4.0),
        "ranks": jax.random.permutation(keys[6], NB).astype(jnp.int32),
    }


def reference(features, out_grads, cold_sums, weight, moment, second, ranks):
    hot_block = ranks < HOT
    hot_col = jnp.repeat(hot_block, BLOCK)
    feats = features.reshape(N_DP, TOK_DEV, D)
    grads = out_grads.reshape(N_DP, TOK_DEV, C)

    def one_group(carry, inputs):
        summed, squares = carry
        feat, cot, cold = inputs
        local = cold.astype(jnp.float32) + jnp.dot(feat.T, cot, preferred_element_type=jnp.float32)
        kept = jnp.where(hot_col[None, :], jnp.float32(0.0), local).astype(jnp.bfloat16)
        return ((summed + local, squares + lax.optimization_barrier(jnp.sum(local * local, axis=0))), kept)
    start = (jnp.zeros((D, C), jnp.float32), jnp.zeros((C,), jnp.float32))
    (summed, column_sq), new_cold = lax.scan(one_group, start, (feats, grads, cold_sums))
    rms = jnp.sqrt(column_sq / jnp.float32(D * N_DP * TOK_DEV))
    clip = 1.0 / jnp.maximum(jnp.float32(1.0), rms)
    grad_mean = summed * clip[None, :] / jnp.float32(N_DP)
    moved = 0.9 * moment + 0.1 * grad_mean
    squared = 0.95 * second + 0.05 * grad_mean * grad_mean
    step_size = 0.05 * (moved / (1.0 - 0.9 ** 10)) / (jnp.sqrt(squared / (1.0 - 0.95 ** 10)) + 1e-08)
    new_moment = jnp.where(hot_col[None, :], moved, moment)
    new_second = jnp.where(hot_col[None, :], squared, second)
    new_weight = jnp.where(hot_col[None, :], weight - step_size, weight)
    return (new_weight, new_moment, new_second, new_cold, column_sq)
```

```python
import functools
import jax
import jax.numpy as jnp
from jax import lax
from jax.experimental import pallas as pl
from jax.experimental.pallas import tpu as pltpu
from jax.sharding import PartitionSpec as P

LANES = 128
FRONT = 5
VMEM_GRANT = 57 * 2**20
MESH = pl.DeviceIdType.MESH


def split_of(own):
    line = 8 * max(round(own / 48), 1)
    cross = own - line
    pieces = next(s for s in (3, 2, 1) if cross % (8 * s) == 0)
    return cross, line, pieces


def block_of(ranks, blocks, rank):
    found = 0
    for b in range(blocks):
        gap = ranks[b] - rank
        found = found + b * (1 - jnp.minimum(gap * gap, 1))
    return pl.multiple_of(found * LANES, LANES)


def exchange_kernel(
    n, reps, hot,
    ranks, feat, og, cold, weight, moment, second,
    summed, sq_out, kept, w_out, m_out, s_out,
    feat_v, og_v, og_p, cold_v, pack_a, pack_b, rx_a, rx_b, la, ra, lb, rb, sq, reps_sq, dp_sq,
    in_sem, state_sem, x_send, x_recv, za_send, la_recv, ra_recv, zb_send, lb_recv, rb_recv,
    b_send, b_recv, n1_send, n1_recv, n2_send, n2_recv,
):
    m = n // 2
    tokens = feat.shape[0]
    rows, width = cold.shape[1], cold.shape[2]
    blocks = width // LANES
    packed = hot * LANES
    own = rows // n
    chunk = max(own, LANES)
    chunks = rows // chunk
    inner = chunk // own
    cross_rows, line_rows, pieces = split_of(own)
    part = cross_rows // pieces
    me = lax.axis_index("dp")
    rep = lax.axis_index("rep")
    x = me % 2
    p = me // 2
    partner = me + 1 - 2 * x

    half = max(m // 2, 1)
    flip = p // half if m > 1 else 0
    pr = p + flip * (m - 1 - 2 * p)
    lone = m - 1 - 2 * pr

    def dest(k):
        late = (k - lone + 2 * m) // (2 * m)
        pair = late * (k - lone)
        odd = pair % 2
        near = (1 - late) * (m - 1 - k) + late * ((1 - odd) * (pair // 2) + odd * (2 * pr - pair // 2))
        return near + flip * (m - 1 - 2 * near)

    def chunk_at(i):
        if chunk != own:
            return i
        side = i % 2
        return 2 * dest(i // 2) + (1 - side) * (1 - x) + side * x

    def loop(count, step):
        if count <= 8:
            for k in range(count):
                step(k)
        else:
            def walk(k, carry):
                step(k)
                return carry

            lax.fori_loop(0, count, walk, 0)

    def rolled(count, step):
        def walk(k, carry):
            step(k)
            return carry

        lax.fori_loop(0, count, walk, 0)

    barrier = pltpu.get_barrier_semaphore()

    def peers(count, step):
        if count <= 8:
            for t in range(1, count):
                step(t)
        else:
            def walk(t, carry):
                step(t)
                return carry

            lax.fori_loop(1, count, walk, 0)

    peers(n, lambda t: pl.semaphore_signal(
        barrier, inc=1, device_id={"dp": (me + t) % n}, device_id_type=MESH))
    peers(reps, lambda t: pl.semaphore_signal(
        barrier, inc=1, device_id={"rep": (rep + t) % reps}, device_id_type=MESH))

    def feat_copy(i):
        cols = pl.ds(pl.multiple_of(chunk_at(i) * chunk, LANES), chunk)
        return pltpu.make_async_copy(feat.at[:, cols], feat_v.at[i], in_sem.at[0, i])

    def cold_copy(i):
        at = pl.ds(pl.multiple_of(chunk_at(i) * chunk, LANES), chunk)
        return pltpu.make_async_copy(cold.at[0, at], cold_v.at[i], in_sem.at[1, i])

    state = [
        pltpu.make_async_copy(src, dst, state_sem.at[i])
        for i, (src, dst) in enumerate(
            ((weight, w_out), (moment, m_out), (second, s_out), (og, og_v))
        )
    ]
    state[3].start()

    def fetch(i):
        feat_copy(i).start()
        cold_copy(i).start()

    rolled(chunks, fetch)
    for copy in state[:3]:
        copy.start()

    sq[...] = jnp.zeros_like(sq)
    picks = []
    for r in range(blocks):
        row = []
        for b in range(blocks):
            gap = ranks[b] - r
            row.append((1 - jnp.minimum(gap * gap, 1)).astype(jnp.float32))
        picks.append(row)

    def ranked(ref, index, r):
        held = None
        for b in range(blocks):
            part_b = ref[index + (slice(b * LANES, (b + 1) * LANES),)]
            part_b = part_b * jnp.full(part_b.shape, picks[r][b]).astype(part_b.dtype)
            held = part_b if held is None else held + part_b
        return held

    def cross(k, sub):
        d = dest(k)
        at = pl.ds(pl.multiple_of(sub * part, 8), part)
        return pltpu.make_async_remote_copy(
            src_ref=pack_a.at[2 * d + 1 - x, at], dst_ref=rx_a.at[d, at],
            send_sem=x_send.at[d, sub], recv_sem=x_recv.at[d, sub],
            device_id={"dp": partner}, device_id_type=MESH,
        )

    def along_a(d, sub, right):
        at = pl.ds(pl.multiple_of(sub * part, 8), part)
        return pltpu.make_async_remote_copy(
            src_ref=pack_a.at[2 * d + x, at], dst_ref=(la if right else ra).at[d, at],
            send_sem=za_send.at[d, sub], recv_sem=(la_recv if right else ra_recv).at[d, sub],
            device_id={"dp": me + 2 if right else me - 2}, device_id_type=MESH,
        )

    def along_b(d, right):
        return pltpu.make_async_remote_copy(
            src_ref=pack_b.at[d], dst_ref=(lb if right else rb).at[d],
            send_sem=zb_send.at[d], recv_sem=(lb_recv if right else rb_recv).at[d],
            device_id={"dp": me + 2 if right else me - 2}, device_id_type=MESH,
        )

    def cross_b():
        return pltpu.make_async_remote_copy(
            src_ref=pack_b.at[p, pl.ds(pl.multiple_of((1 - x) * line_rows, 8), line_rows)],
            dst_ref=rx_b, send_sem=b_send, recv_sem=b_recv,
            device_id={"dp": partner}, device_id_type=MESH,
        )

    def norm_rep(t):
        return pltpu.make_async_remote_copy(
            src_ref=sq, dst_ref=reps_sq.at[rep],
            send_sem=n1_send.at[t], recv_sem=n1_recv.at[rep],
            device_id={"rep": (rep + t) % reps}, device_id_type=MESH,
        )

    def norm_rep_in(t):
        j = (rep + t) % reps
        return pltpu.make_async_remote_copy(
            src_ref=sq, dst_ref=reps_sq.at[j],
            send_sem=n1_send.at[t], recv_sem=n1_recv.at[j],
            device_id={"rep": j}, device_id_type=MESH,
        )

    def norm_dp(t):
        return pltpu.make_async_remote_copy(
            src_ref=dp_sq.at[me], dst_ref=dp_sq.at[me],
            send_sem=n2_send.at[t], recv_sem=n2_recv.at[me],
            device_id={"dp": (me + t) % n}, device_id_type=MESH,
        )

    def norm_dp_in(t):
        j = (me + t) % n
        return pltpu.make_async_remote_copy(
            src_ref=dp_sq.at[j], dst_ref=dp_sq.at[j],
            send_sem=n2_send.at[t], recv_sem=n2_recv.at[j],
            device_id={"dp": j}, device_id_type=MESH,
        )

    def raw_b(k):
        d = dest(k)

        @pl.when(jnp.logical_and(d > p, p == 0))
        def _():
            along_b(d, True).start()

        @pl.when(jnp.logical_and(d < p, p == m - 1))
        def _():
            along_b(d, False).start()

    state[3].wait()
    for r in range(blocks):
        og_p[:, r * LANES:(r + 1) * LANES] = ranked(og_v, (slice(None),), r)
    pl.semaphore_wait(barrier, (n - 1) + (reps - 1))

    def product(i, lo, hi):
        grad = lax.dot_general(
            feat_v[i], og_p[:, lo * LANES:hi * LANES], (((0,), (0,)), ((), ())),
            preferred_element_type=jnp.float32,
        )
        pairs = []
        for r in range(lo, hi):
            held = ranked(cold_v, (i, slice(None)), r).astype(jnp.float32)
            value = grad[:, (r - lo) * LANES:(r - lo + 1) * LANES] + held
            sq[r:r + 1, :] += jnp.sum(value * value, axis=0, keepdims=True)
            pairs.append((r, value))
        return pairs

    def hot_step(i):
        feat_copy(i).wait()
        cold_copy(i).wait()
        c = chunk_at(i)
        for r, value in product(i, 0, hot):
            cols = slice(r * LANES, (r + 1) * LANES)
            for j in range(inner):
                owner = c * inner + j
                q, s = owner // 2, owner % 2
                pack_a[owner, :, cols] = value[j * own:j * own + cross_rows]
                pack_b[q, pl.ds(pl.multiple_of(s * line_rows, 8), line_rows), cols] = (
                    value[j * own + cross_rows:(j + 1) * own])
        if chunk == own:
            k = i // 2
            for sub in range(pieces):
                @pl.when(jnp.logical_and(i % 2 == 0, k * pieces + sub < FRONT))
                def _():
                    cross(k, sub).start()

            @pl.when(i % 2 == 1)
            def _():
                raw_b(k)

    def cold_step(i):
        at = pl.ds(pl.multiple_of(chunk_at(i) * chunk, LANES), chunk)
        for r, value in product(i, hot, blocks):
            cols = slice((r - hot) * LANES, (r - hot + 1) * LANES)
            kept[at, cols] = value.astype(jnp.bfloat16)

    rolled(chunks, hot_step)
    rolled(chunks, cold_step)
    if chunk != own:
        def launch(k):
            for sub in range(pieces):
                @pl.when(k * pieces + sub < FRONT)
                def _():
                    cross(k, sub).start()
            raw_b(k)

        rolled(m, launch)
    peers(reps, lambda t: norm_rep(t).start())

    def line_step(k):
        d = dest(k)

        @pl.when(jnp.logical_and(d >= p, p > 0))
        def _():
            along_b(d, True).wait_recv()
            pack_b[d] += lb[d]

        @pl.when(jnp.logical_and(d <= p, p < m - 1))
        def _():
            along_b(d, False).wait_recv()
            pack_b[d] += rb[d]

        @pl.when(jnp.logical_and(d > p, p > 0))
        def _():
            along_b(d, True).start()

        @pl.when(jnp.logical_and(d < p, p < m - 1))
        def _():
            along_b(d, False).start()

    peers(reps, lambda t: norm_rep_in(t).wait_recv())
    reps_sq[rep] = sq[...]
    total = reps_sq[0]
    for j in range(1, reps):
        total = total + reps_sq[j]
    dp_sq[me] = total
    peers(n, lambda t: norm_dp(t).start())

    def rest(k):
        for sub in range(pieces):
            @pl.when(k * pieces + sub >= FRONT)
            def _():
                cross(k, sub).start()

    rolled(m, rest)
    loop(m, line_step)
    cross_b().start()

    def cross_step(k):
        d = dest(k)
        for sub in range(pieces):
            at = slice(sub * part, (sub + 1) * part)
            cross(k, sub).wait_recv()
            pack_a[2 * d + x, at] += rx_a[d, at]

            @pl.when(jnp.logical_and(d >= p, p > 0))
            def _():
                along_a(d, sub, True).wait_recv()
                pack_a[2 * d + x, at] += la[d, at]

            @pl.when(jnp.logical_and(d <= p, p < m - 1))
            def _():
                along_a(d, sub, False).wait_recv()
                pack_a[2 * d + x, at] += ra[d, at]

            @pl.when(d > p)
            def _():
                along_a(d, sub, True).start()

            @pl.when(d < p)
            def _():
                along_a(d, sub, False).start()

            @pl.when(d == p)
            def _():
                summed[at] = pack_a[2 * d + x, at]

    loop(m - 1, cross_step)
    peers(n, lambda t: norm_dp_in(t).wait_recv())
    everything = dp_sq[0]
    for j in range(1, n):
        everything = everything + dp_sq[j]
    sq_out[...] = everything
    for copy in state[:3]:
        copy.wait()
    cross_b().wait_recv()
    mine = pl.ds(pl.multiple_of(x * line_rows, 8), line_rows)
    summed[cross_rows:] = pack_b[p, mine] + rx_b[...]
    cross_step(m - 1)

    def drain(k):
        d = dest(k)
        for sub in range(pieces):
            cross(k, sub).wait_send()

        @pl.when(d > p)
        def _():
            along_b(d, True).wait_send()
            for sub in range(pieces):
                along_a(d, sub, True).wait_send()

        @pl.when(d < p)
        def _():
            along_b(d, False).wait_send()
            for sub in range(pieces):
                along_a(d, sub, False).wait_send()

    rolled(m, drain)
    cross_b().wait_send()
    peers(reps, lambda t: norm_rep(t).wait_send())
    peers(n, lambda t: norm_dp(t).wait_send())


def update_kernel(
    n, total_rows, tokens, hot,
    ranks, summed, sq, kept, weight, moment, second,
    w_hbm, m_hbm, s_hbm, nc_hbm, sq_hbm,
    fresh, none, sq_v, nc_sem, state_sem, sq_sem,
):
    width = weight.shape[1]
    blocks = width // LANES
    where = [pl.ds(block_of(ranks, blocks, r), LANES) for r in range(blocks)]
    outs = (w_hbm, m_hbm, s_hbm)
    copies = []

    def send(src, dst, sem):
        copies.append(pltpu.make_async_copy(src, dst, sem))
        copies[-1].start()

    for r in range(hot, blocks):
        cols = pl.ds((r - hot) * LANES, LANES)
        send(kept.at[:, cols], nc_hbm.at[0, :, where[r]], nc_sem.at[r])
        for i, src in enumerate((weight, moment, second)):
            send(src.at[:, where[r]], outs[i].at[:, where[r]], state_sem.at[i, r])
    none[...] = jnp.zeros_like(none)
    for r in range(hot):
        send(none, nc_hbm.at[0, :, where[r]], nc_sem.at[r])
    for b in range(blocks):
        sq_v[b:b + 1, :] = sq[pl.ds(ranks[b], 1), :]
    send(sq_v, sq_hbm, sq_sem)
    for r in range(hot):
        cols = slice(r * LANES, (r + 1) * LANES)
        rms = jnp.sqrt(sq[r:r + 1, :] / jnp.float32(total_rows * n * tokens))
        clip = 1.0 / jnp.maximum(jnp.float32(1.0), rms)
        grad = summed[:, cols] * clip / jnp.float32(n)
        moved = 0.9 * moment[:, where[r]] + 0.1 * grad
        squared = 0.95 * second[:, where[r]] + 0.05 * grad * grad
        fresh[1, :, cols] = moved
        fresh[2, :, cols] = squared
        step = 0.05 * (moved / (1.0 - 0.9**10)) / (
            jnp.sqrt(squared / (1.0 - 0.95**10)) + 1e-08
        )
        fresh[0, :, cols] = weight[:, where[r]] - step
        for i in range(3):
            send(fresh.at[i, :, pl.ds(r * LANES, LANES)], outs[i].at[:, where[r]], state_sem.at[i, r])
    for copy in copies:
        copy.wait()


def body(n, reps, features, out_grads, cold_sums, weight, moment, second, ranks):
    tokens, rows = features.shape
    width = out_grads.shape[1]
    blocks = ranks.shape[0]
    hot = blocks // 2
    packed = hot * LANES
    m = n // 2
    own = rows // n
    chunk = max(own, LANES)
    chunks = rows // chunk
    cross_rows, line_rows, pieces = split_of(own)
    f32, bf16 = jnp.float32, jnp.bfloat16
    vmem = pl.BlockSpec(memory_space=pltpu.VMEM)
    smem = pl.BlockSpec(memory_space=pltpu.SMEM)
    hbm = pl.BlockSpec(memory_space=pl.ANY)
    dma = pltpu.SemaphoreType.DMA
    summed, sq, kept, w, mo, se = pl.pallas_call(
        functools.partial(exchange_kernel, n, reps, hot),
        out_shape=(
            pltpu.VMEM((own, packed), f32),
            pltpu.VMEM((blocks, LANES), f32),
            pltpu.VMEM((rows, width - packed), bf16),
            pltpu.VMEM(weight.shape, f32),
            pltpu.VMEM(weight.shape, f32),
            pltpu.VMEM(weight.shape, f32),
        ),
        in_specs=[smem] + [pl.BlockSpec(memory_space=pltpu.HBM)] * 6,
        out_specs=(vmem,) * 6,
        scratch_shapes=[
            pltpu.VMEM((chunks, tokens, chunk), bf16),
            pltpu.VMEM((tokens, width), bf16),
            pltpu.VMEM((tokens, width), bf16),
            pltpu.VMEM((chunks, chunk, width), bf16),
            pltpu.VMEM((n, cross_rows, packed), f32),
            pltpu.VMEM((m, 2 * line_rows, packed), f32),
            pltpu.VMEM((m, cross_rows, packed), f32),
            pltpu.VMEM((line_rows, packed), f32),
            pltpu.VMEM((m, cross_rows, packed), f32),
            pltpu.VMEM((m, cross_rows, packed), f32),
            pltpu.VMEM((m, 2 * line_rows, packed), f32),
            pltpu.VMEM((m, 2 * line_rows, packed), f32),
            pltpu.VMEM((blocks, LANES), f32),
            pltpu.VMEM((reps, blocks, LANES), f32),
            pltpu.VMEM((n, blocks, LANES), f32),
            dma((2, chunks)),
            dma((4,)),
            dma((m, pieces)),
            dma((m, pieces)),
            dma((m, pieces)),
            dma((m, pieces)),
            dma((m, pieces)),
            dma((m,)),
            dma((m,)),
            dma((m,)),
            dma,
            dma,
            dma((reps,)),
            dma((reps,)),
            dma((n,)),
            dma((n,)),
        ],
        compiler_params=pltpu.CompilerParams(
            collective_id=0, has_side_effects=True, vmem_limit_bytes=VMEM_GRANT
        ),
        name="exchange",
    )(ranks, features, out_grads, cold_sums, weight, moment, second)
    new_weight, new_moment, new_second, new_cold, column_sq = pl.pallas_call(
        functools.partial(update_kernel, n, rows * reps, tokens, hot),
        out_shape=(
            jax.ShapeDtypeStruct(weight.shape, f32),
            jax.ShapeDtypeStruct(weight.shape, f32),
            jax.ShapeDtypeStruct(weight.shape, f32),
            jax.ShapeDtypeStruct(cold_sums.shape, bf16),
            jax.ShapeDtypeStruct((blocks, LANES), f32),
        ),
        in_specs=[smem] + [vmem] * 6,
        out_specs=(hbm,) * 5,
        scratch_shapes=[
            pltpu.VMEM((3, weight.shape[0], packed), f32),
            pltpu.VMEM((rows, LANES), bf16),
            pltpu.VMEM((blocks, LANES), f32),
            dma((blocks,)),
            dma((3, blocks)),
            dma,
        ],
        compiler_params=pltpu.CompilerParams(vmem_limit_bytes=VMEM_GRANT // 2),
        name="update",
    )(ranks, summed, sq, kept, w, mo, se)
    return new_weight, new_moment, new_second, new_cold, column_sq.reshape(width)


def solution(mesh):
    owned = P(("rep", "dp"), None)
    placed = (P("dp", "rep"), P("dp", None), P("dp", "rep", None), owned, owned, owned, P())
    return jax.shard_map(
        functools.partial(body, mesh.shape["dp"], mesh.shape["rep"]),
        mesh=mesh,
        in_specs=placed,
        out_specs=(owned, owned, owned, P("dp", "rep", None), P()),
        check_vma=False,
    )
```

```python
import functools
import jax
import jax.numpy as jnp
from jax import lax
from jax.experimental import pallas as pl
from jax.experimental.pallas import tpu as pltpu
from jax.sharding import PartitionSpec as P

LANES = 128
FRONT = 9
VMEM_GRANT = 57 * 2**20
MESH = pl.DeviceIdType.MESH


def split_of(own):
    line = 8 * max(round(own / 48), 1)
    cross = own - line
    pieces = next(s for s in (3, 2, 1) if cross % (8 * s) == 0)
    return cross, line, pieces


def block_of(ranks, blocks, rank):
    found = 0
    for b in range(blocks):
        gap = ranks[b] - rank
        found = found + b * (1 - jnp.minimum(gap * gap, 1))
    return pl.multiple_of(found * LANES, LANES)


def exchange_kernel(
    n, reps, hot,
    ranks, feat, og, cold, weight, moment, second,
    summed, sq_out, kept, w_out, m_out, s_out,
    feat_v, og_v, og_p, cold_v, pack_a, pack_b, rx_a, rx_b, la, ra, lb, rb, sq, reps_sq, dp_sq,
    in_sem, state_sem, x_send, x_recv, za_send, la_recv, ra_recv, zb_send, lb_recv, rb_recv,
    b_send, b_recv, n1_send, n1_recv, n2_send, n2_recv,
):
    m = n // 2
    tokens = feat.shape[0]
    rows, width = cold.shape[1], cold.shape[2]
    blocks = width // LANES
    packed = hot * LANES
    own = rows // n
    chunk = max(own, LANES)
    chunks = rows // chunk
    inner = chunk // own
    cross_rows, line_rows, pieces = split_of(own)
    part = cross_rows // pieces
    me = lax.axis_index("dp")
    rep = lax.axis_index("rep")
    x = me % 2
    p = me // 2
    partner = me + 1 - 2 * x

    half = max(m // 2, 1)
    flip = p // half if m > 1 else 0
    pr = p + flip * (m - 1 - 2 * p)
    lone = m - 1 - 2 * pr

    def dest(k):
        late = (k - lone + 2 * m) // (2 * m)
        pair = late * (k - lone)
        odd = pair % 2
        near = (1 - late) * (m - 1 - k) + late * ((1 - odd) * (pair // 2) + odd * (2 * pr - pair // 2))
        return near + flip * (m - 1 - 2 * near)

    def chunk_at(i):
        if chunk != own:
            return i
        side = i % 2
        return 2 * dest(i // 2) + (1 - side) * (1 - x) + side * x

    def span(lo, hi, step):
        if hi - lo <= 8:
            for k in range(lo, hi):
                step(k)
        else:
            lax.fori_loop(lo, hi, lambda k, carry: step(k) or carry, 0)

    def rolled(lo, hi, step):
        lax.fori_loop(lo, hi, lambda k, carry: step(k) or carry, 0)

    barrier = pltpu.get_barrier_semaphore()

    def feat_copy(i):
        cols = pl.ds(pl.multiple_of(chunk_at(i) * chunk, LANES), chunk)
        return pltpu.make_async_copy(feat.at[:, cols], feat_v.at[i], in_sem.at[0, i])

    def cold_copy(i):
        at = pl.ds(pl.multiple_of(chunk_at(i) * chunk, LANES), chunk)
        return pltpu.make_async_copy(cold.at[0, at], cold_v.at[i], in_sem.at[1, i])

    state = [
        pltpu.make_async_copy(src, dst, state_sem.at[i])
        for i, (src, dst) in enumerate(
            ((weight, w_out), (moment, m_out), (second, s_out), (og, og_v))
        )
    ]
    def fetch(i):
        feat_copy(i).start()
        cold_copy(i).start()

    state[3].start()
    fetch(0)
    span(1, n, lambda t: pl.semaphore_signal(
        barrier, inc=1, device_id={"dp": (me + t) % n}, device_id_type=MESH))
    span(1, reps, lambda t: pl.semaphore_signal(
        barrier, inc=1, device_id={"rep": (rep + t) % reps}, device_id_type=MESH))
    rolled(1, chunks, fetch)

    sq[...] = jnp.zeros_like(sq)
    picks = []
    for r in range(blocks):
        row = []
        for b in range(blocks):
            gap = ranks[b] - r
            row.append((1 - jnp.minimum(gap * gap, 1)).astype(jnp.float32))
        picks.append(row)

    def ranked(ref, index, r):
        held = None
        for b in range(blocks):
            part_b = ref[index + (slice(b * LANES, (b + 1) * LANES),)]
            part_b = part_b * jnp.full(part_b.shape, picks[r][b]).astype(part_b.dtype)
            held = part_b if held is None else held + part_b
        return held

    def cross(k, sub):
        d = dest(k)
        at = pl.ds(pl.multiple_of(sub * part, 8), part)
        return pltpu.make_async_remote_copy(
            src_ref=pack_a.at[2 * d + 1 - x, at], dst_ref=rx_a.at[d, at],
            send_sem=x_send.at[d, sub], recv_sem=x_recv.at[d, sub],
            device_id={"dp": partner}, device_id_type=MESH,
        )

    def along_a(d, sub, right):
        at = pl.ds(pl.multiple_of(sub * part, 8), part)
        return pltpu.make_async_remote_copy(
            src_ref=pack_a.at[2 * d + x, at], dst_ref=(la if right else ra).at[d, at],
            send_sem=za_send.at[d, sub], recv_sem=(la_recv if right else ra_recv).at[d, sub],
            device_id={"dp": me + 2 if right else me - 2}, device_id_type=MESH,
        )

    def along_b(d, right):
        return pltpu.make_async_remote_copy(
            src_ref=pack_b.at[d], dst_ref=(lb if right else rb).at[d],
            send_sem=zb_send.at[d], recv_sem=(lb_recv if right else rb_recv).at[d],
            device_id={"dp": me + 2 if right else me - 2}, device_id_type=MESH,
        )

    def cross_b():
        return pltpu.make_async_remote_copy(
            src_ref=pack_b.at[p, pl.ds(pl.multiple_of((1 - x) * line_rows, 8), line_rows)],
            dst_ref=rx_b, send_sem=b_send, recv_sem=b_recv,
            device_id={"dp": partner}, device_id_type=MESH,
        )

    def norm_rep(t):
        return pltpu.make_async_remote_copy(
            src_ref=sq, dst_ref=reps_sq.at[rep],
            send_sem=n1_send.at[t], recv_sem=n1_recv.at[rep],
            device_id={"rep": (rep + t) % reps}, device_id_type=MESH,
        )

    def norm_rep_in(t):
        j = (rep + t) % reps
        return pltpu.make_async_remote_copy(
            src_ref=sq, dst_ref=reps_sq.at[j],
            send_sem=n1_send.at[t], recv_sem=n1_recv.at[j],
            device_id={"rep": j}, device_id_type=MESH,
        )

    def norm_dp(t):
        return pltpu.make_async_remote_copy(
            src_ref=dp_sq.at[me], dst_ref=dp_sq.at[me],
            send_sem=n2_send.at[t], recv_sem=n2_recv.at[me],
            device_id={"dp": (me + t) % n}, device_id_type=MESH,
        )

    def norm_dp_in(t):
        j = (me + t) % n
        return pltpu.make_async_remote_copy(
            src_ref=dp_sq.at[j], dst_ref=dp_sq.at[j],
            send_sem=n2_send.at[t], recv_sem=n2_recv.at[j],
            device_id={"dp": j}, device_id_type=MESH,
        )

    def raw_b(k):
        d = dest(k)

        @pl.when(jnp.logical_and(d > p, p == 0))
        def _():
            along_b(d, True).start()

        @pl.when(jnp.logical_and(d < p, p == m - 1))
        def _():
            along_b(d, False).start()

    state[3].wait()
    for r in range(hot):
        og_p[:, r * LANES:(r + 1) * LANES] = ranked(og_v, (slice(None),), r)
    pl.semaphore_wait(barrier, (n - 1) + (reps - 1))

    def product(i, lo, hi):
        grad = lax.dot_general(
            feat_v[i], og_p[:, lo * LANES:hi * LANES], (((0,), (0,)), ((), ())),
            preferred_element_type=jnp.float32,
        )
        pairs = []
        for r in range(lo, hi):
            held = ranked(cold_v, (i, slice(None)), r).astype(jnp.float32)
            value = grad[:, (r - lo) * LANES:(r - lo + 1) * LANES] + held
            sq[r:r + 1, :] += jnp.sum(value * value, axis=0, keepdims=True)
            pairs.append((r, value))
        return pairs

    def hot_step(i):
        feat_copy(i).wait()
        cold_copy(i).wait()
        c = chunk_at(i)
        for r, value in product(i, 0, hot):
            cols = slice(r * LANES, (r + 1) * LANES)
            for j in range(inner):
                owner = c * inner + j
                q, s = owner // 2, owner % 2
                pack_a[owner, :, cols] = value[j * own:j * own + cross_rows]
                pack_b[q, pl.ds(pl.multiple_of(s * line_rows, 8), line_rows), cols] = (
                    value[j * own + cross_rows:(j + 1) * own])
        if chunk == own:
            k = i // 2
            for sub in range(pieces):
                @pl.when(jnp.logical_and(i % 2 == 0, k * pieces + sub < FRONT))
                def _():
                    cross(k, sub).start()

            @pl.when(i % 2 == 1)
            def _():
                raw_b(k)

    def cold_step(i):
        at = pl.ds(pl.multiple_of(chunk_at(i) * chunk, LANES), chunk)
        for r, value in product(i, hot, blocks):
            cols = slice((r - hot) * LANES, (r - hot + 1) * LANES)
            kept[at, cols] = value.astype(jnp.bfloat16)

    rolled(0, chunks, hot_step)
    for copy in state[:3]:
        copy.start()
    for r in range(hot, blocks):
        og_p[:, r * LANES:(r + 1) * LANES] = ranked(og_v, (slice(None),), r)
    rolled(0, chunks, cold_step)
    if chunk != own:
        def launch(k):
            for sub in range(pieces):
                @pl.when(k * pieces + sub < FRONT)
                def _():
                    cross(k, sub).start()
            raw_b(k)

        rolled(0, m, launch)
    span(1, reps, lambda t: norm_rep(t).start())

    def line_step(k):
        d = dest(k)

        @pl.when(jnp.logical_and(d >= p, p > 0))
        def _():
            along_b(d, True).wait_recv()
            pack_b[d] += lb[d]

        @pl.when(jnp.logical_and(d <= p, p < m - 1))
        def _():
            along_b(d, False).wait_recv()
            pack_b[d] += rb[d]

        @pl.when(jnp.logical_and(d > p, p > 0))
        def _():
            along_b(d, True).start()

        @pl.when(jnp.logical_and(d < p, p < m - 1))
        def _():
            along_b(d, False).start()

    def rest(k):
        for sub in range(pieces):
            @pl.when(k * pieces + sub >= FRONT)
            def _():
                cross(k, sub).start()

    def cross_step(k):
        d = dest(k)
        for sub in range(pieces):
            at = slice(sub * part, (sub + 1) * part)
            cross(k, sub).wait_recv()
            pack_a[2 * d + x, at] += rx_a[d, at]

            @pl.when(jnp.logical_and(d >= p, p > 0))
            def _():
                along_a(d, sub, True).wait_recv()
                pack_a[2 * d + x, at] += la[d, at]

            @pl.when(jnp.logical_and(d <= p, p < m - 1))
            def _():
                along_a(d, sub, False).wait_recv()
                pack_a[2 * d + x, at] += ra[d, at]

            @pl.when(d > p)
            def _():
                along_a(d, sub, True).start()

            @pl.when(d < p)
            def _():
                along_a(d, sub, False).start()

            @pl.when(d == p)
            def _():
                summed[at] = pack_a[2 * d + x, at]

    span(0, m - 1, line_step)
    if m > 1:
        cross_step(0)
    span(1, reps, lambda t: norm_rep_in(t).wait_recv())
    reps_sq[rep] = sq[...]
    total = reps_sq[0]
    for j in range(1, reps):
        total = total + reps_sq[j]
    dp_sq[me] = total
    span(1, n, lambda t: norm_dp(t).start())
    rolled(0, m, rest)
    span(1, m - 2, cross_step)
    line_step(m - 1)
    cross_b().start()
    if m > 2:
        cross_step(m - 2)
    span(1, n, lambda t: norm_dp_in(t).wait_recv())
    everything = dp_sq[0]
    for j in range(1, n):
        everything = everything + dp_sq[j]
    sq_out[...] = everything
    for copy in state[:3]:
        copy.wait()
    cross_step(m - 1)
    cross_b().wait_recv()
    mine = pl.ds(pl.multiple_of(x * line_rows, 8), line_rows)
    summed[cross_rows:] = pack_b[p, mine] + rx_b[...]

    def drain(k):
        d = dest(k)
        for sub in range(pieces):
            cross(k, sub).wait_send()

        @pl.when(d > p)
        def _():
            along_b(d, True).wait_send()
            for sub in range(pieces):
                along_a(d, sub, True).wait_send()

        @pl.when(d < p)
        def _():
            along_b(d, False).wait_send()
            for sub in range(pieces):
                along_a(d, sub, False).wait_send()

    rolled(0, m, drain)
    cross_b().wait_send()
    span(1, reps, lambda t: norm_rep(t).wait_send())
    span(1, n, lambda t: norm_dp(t).wait_send())


def update_kernel(
    n, total_rows, tokens, hot,
    ranks, summed, sq, kept, weight, moment, second,
    w_hbm, m_hbm, s_hbm, nc_hbm, sq_hbm,
    fresh, none, sq_v, nc_sem, state_sem, sq_sem,
):
    width = weight.shape[1]
    blocks = width // LANES
    where = [pl.ds(block_of(ranks, blocks, r), LANES) for r in range(blocks)]
    outs = (w_hbm, m_hbm, s_hbm)
    copies = []

    def send(src, dst, sem):
        copies.append(pltpu.make_async_copy(src, dst, sem))
        copies[-1].start()

    for r in range(hot, blocks):
        cols = pl.ds((r - hot) * LANES, LANES)
        send(kept.at[:, cols], nc_hbm.at[0, :, where[r]], nc_sem.at[r])
        for i, src in enumerate((weight, moment, second)):
            send(src.at[:, where[r]], outs[i].at[:, where[r]], state_sem.at[i, r])
    none[...] = jnp.zeros_like(none)
    for r in range(hot):
        send(none, nc_hbm.at[0, :, where[r]], nc_sem.at[r])
    for b in range(blocks):
        sq_v[b:b + 1, :] = sq[pl.ds(ranks[b], 1), :]
    send(sq_v, sq_hbm, sq_sem)
    for r in range(hot):
        cols = slice(r * LANES, (r + 1) * LANES)
        rms = jnp.sqrt(sq[r:r + 1, :] / jnp.float32(total_rows * n * tokens))
        clip = 1.0 / jnp.maximum(jnp.float32(1.0), rms)
        grad = summed[:, cols] * clip / jnp.float32(n)
        moved = 0.9 * moment[:, where[r]] + 0.1 * grad
        squared = 0.95 * second[:, where[r]] + 0.05 * grad * grad
        fresh[1, :, cols] = moved
        fresh[2, :, cols] = squared
        step = 0.05 * (moved / (1.0 - 0.9**10)) / (
            jnp.sqrt(squared / (1.0 - 0.95**10)) + 1e-08
        )
        fresh[0, :, cols] = weight[:, where[r]] - step
        for i in range(3):
            send(fresh.at[i, :, pl.ds(r * LANES, LANES)], outs[i].at[:, where[r]], state_sem.at[i, r])
    for copy in copies:
        copy.wait()


def body(n, reps, features, out_grads, cold_sums, weight, moment, second, ranks):
    tokens, rows = features.shape
    width = out_grads.shape[1]
    blocks = ranks.shape[0]
    hot = blocks // 2
    packed = hot * LANES
    m = n // 2
    own = rows // n
    chunk = max(own, LANES)
    chunks = rows // chunk
    cross_rows, line_rows, pieces = split_of(own)
    f32, bf16 = jnp.float32, jnp.bfloat16
    vmem = pl.BlockSpec(memory_space=pltpu.VMEM)
    smem = pl.BlockSpec(memory_space=pltpu.SMEM)
    hbm = pl.BlockSpec(memory_space=pl.ANY)
    dma = pltpu.SemaphoreType.DMA
    summed, sq, kept, w, mo, se = pl.pallas_call(
        functools.partial(exchange_kernel, n, reps, hot),
        out_shape=(
            pltpu.VMEM((own, packed), f32),
            pltpu.VMEM((blocks, LANES), f32),
            pltpu.VMEM((rows, width - packed), bf16),
            pltpu.VMEM(weight.shape, f32),
            pltpu.VMEM(weight.shape, f32),
            pltpu.VMEM(weight.shape, f32),
        ),
        in_specs=[smem] + [pl.BlockSpec(memory_space=pltpu.HBM)] * 6,
        out_specs=(vmem,) * 6,
        scratch_shapes=[
            pltpu.VMEM((chunks, tokens, chunk), bf16),
            pltpu.VMEM((tokens, width), bf16),
            pltpu.VMEM((tokens, width), bf16),
            pltpu.VMEM((chunks, chunk, width), bf16),
            pltpu.VMEM((n, cross_rows, packed), f32),
            pltpu.VMEM((m, 2 * line_rows, packed), f32),
            pltpu.VMEM((m, cross_rows, packed), f32),
            pltpu.VMEM((line_rows, packed), f32),
            pltpu.VMEM((m, cross_rows, packed), f32),
            pltpu.VMEM((m, cross_rows, packed), f32),
            pltpu.VMEM((m, 2 * line_rows, packed), f32),
            pltpu.VMEM((m, 2 * line_rows, packed), f32),
            pltpu.VMEM((blocks, LANES), f32),
            pltpu.VMEM((reps, blocks, LANES), f32),
            pltpu.VMEM((n, blocks, LANES), f32),
            dma((2, chunks)),
            dma((4,)),
            dma((m, pieces)),
            dma((m, pieces)),
            dma((m, pieces)),
            dma((m, pieces)),
            dma((m, pieces)),
            dma((m,)),
            dma((m,)),
            dma((m,)),
            dma,
            dma,
            dma((reps,)),
            dma((reps,)),
            dma((n,)),
            dma((n,)),
        ],
        compiler_params=pltpu.CompilerParams(
            collective_id=0, has_side_effects=True, vmem_limit_bytes=VMEM_GRANT
        ),
        name="exchange",
    )(ranks, features, out_grads, cold_sums, weight, moment, second)
    new_weight, new_moment, new_second, new_cold, column_sq = pl.pallas_call(
        functools.partial(update_kernel, n, rows * reps, tokens, hot),
        out_shape=(
            jax.ShapeDtypeStruct(weight.shape, f32),
            jax.ShapeDtypeStruct(weight.shape, f32),
            jax.ShapeDtypeStruct(weight.shape, f32),
            jax.ShapeDtypeStruct(cold_sums.shape, bf16),
            jax.ShapeDtypeStruct((blocks, LANES), f32),
        ),
        in_specs=[smem] + [vmem] * 6,
        out_specs=(hbm,) * 5,
        scratch_shapes=[
            pltpu.VMEM((3, weight.shape[0], packed), f32),
            pltpu.VMEM((rows, LANES), bf16),
            pltpu.VMEM((blocks, LANES), f32),
            dma((blocks,)),
            dma((3, blocks)),
            dma,
        ],
        compiler_params=pltpu.CompilerParams(vmem_limit_bytes=VMEM_GRANT // 2),
        name="update",
    )(ranks, summed, sq, kept, w, mo, se)
    return new_weight, new_moment, new_second, new_cold, column_sq.reshape(width)


def solution(mesh):
    owned = P(("rep", "dp"), None)
    placed = (P("dp", "rep"), P("dp", None), P("dp", "rep", None), owned, owned, owned, P())
    return jax.shard_map(
        functools.partial(body, mesh.shape["dp"], mesh.shape["rep"]),
        mesh=mesh,
        in_specs=placed,
        out_specs=(owned, owned, owned, P("dp", "rep", None), P()),
        check_vma=False,
    )
```

```python
import functools
import jax
import jax.numpy as jnp
from jax import lax
from jax.experimental import pallas as pl
from jax.experimental.pallas import tpu as pltpu
from jax.sharding import PartitionSpec as P

LANES = 128
GROUP = 32
FRONT = 6
VMEM_GRANT = 55 * 2**20
MESH = pl.DeviceIdType.MESH


def split_of(own):
    line = 8 * max(round(own / 48), 1)
    cross = own - line
    pieces = next(s for s in (3, 2, 1) if cross % (8 * s) == 0)
    return cross, line, pieces


def block_of(ranks, blocks, rank):
    found = 0
    for b in range(blocks):
        gap = ranks[b] - rank
        found = found + b * (1 - jnp.minimum(gap * gap, 1))
    return pl.multiple_of(found * LANES, LANES)


def exchange_kernel(
    n, reps, hot,
    ranks_hbm, feat, og, cold, weight, moment, second,
    summed, sq_out, kept, w_out, m_out, s_out,
    ranks, feat_v, og_v, og_p, cold_v, pack_a, pack_b, rx_a, rx_b, zin_a, zin_b, sq, reps_sq, pair_sq, line_sq,
    in_sem, state_sem, x_send, x_recv, za_send, za_recv, zb_send, zb_recv, b_send, b_recv,
    nr_send, nr_recv, nx_send, nx_recv, nz_send, nz_recv, from_left, from_right,
):
    m = n // 2
    tokens = feat.shape[0]
    rows, width = cold.shape[1], cold.shape[2]
    blocks = width // LANES
    packed = hot * LANES
    own = rows // n
    chunk = max(own, LANES)
    chunks = rows // chunk
    inner = chunk // own
    cross_rows, line_rows, pieces = split_of(own)
    part = cross_rows // pieces
    me = lax.axis_index("dp")
    rep = lax.axis_index("rep")
    x = me % 2
    p = me // 2
    partner = me + 1 - 2 * x

    half = max(m // 2, 1)
    flip = p // half if m > 1 else 0
    pr = p + flip * (m - 1 - 2 * p)
    lone = m - 1 - 2 * pr

    def dest(k):
        late = (k - lone + 2 * m) // (2 * m)
        pair = late * (k - lone)
        odd = pair % 2
        near = (1 - late) * (m - 1 - k) + late * ((1 - odd) * (pair // 2) + odd * (2 * pr - pair // 2))
        return near + flip * (m - 1 - 2 * near)

    def chunk_at(i):
        if chunk != own:
            return i
        side = i % 2
        return 2 * dest(i // 2) + (1 - side) * (1 - x) + side * x

    def span(lo, hi, step):
        if hi - lo <= 8:
            for k in range(lo, hi):
                step(k)
        else:
            lax.fori_loop(lo, hi, lambda k, carry: step(k) or carry, 0)

    def rolled(lo, hi, step):
        lax.fori_loop(lo, hi, lambda k, carry: step(k) or carry, 0)

    barrier = pltpu.get_barrier_semaphore()

    def feat_copy(i):
        cols = pl.ds(pl.multiple_of(chunk_at(i) * chunk, LANES), chunk)
        return pltpu.make_async_copy(feat.at[:, cols], feat_v.at[i], in_sem.at[0, i])

    def cold_copy(i):
        at = pl.ds(pl.multiple_of(chunk_at(i) * chunk, LANES), chunk)
        return pltpu.make_async_copy(cold.at[0, at], cold_v.at[i], in_sem.at[1, i])

    state = [
        pltpu.make_async_copy(src, dst, state_sem.at[i])
        for i, (src, dst) in enumerate(
            ((weight, w_out), (moment, m_out), (second, s_out), (og, og_v), (ranks_hbm, ranks))
        )
    ]
    def fetch(i):
        feat_copy(i).start()
        cold_copy(i).start()

    state[3].start()
    state[4].start()
    fetch(0)
    pl.semaphore_signal(barrier, inc=1, device_id={"dp": partner}, device_id_type=MESH)

    @pl.when(p > 0)
    def _():
        pl.semaphore_signal(barrier, inc=1, device_id={"dp": me - 2}, device_id_type=MESH)

    @pl.when(p < m - 1)
    def _():
        pl.semaphore_signal(barrier, inc=1, device_id={"dp": me + 2}, device_id_type=MESH)

    span(1, reps, lambda t: pl.semaphore_signal(
        barrier, inc=1, device_id={"rep": (rep + t) % reps}, device_id_type=MESH))
    rolled(1, chunks, fetch)

    sq[...] = jnp.zeros_like(sq)

    def ranked(load, lo, hi):
        parts = [load(slice(b * LANES, (b + 1) * LANES)) for b in range(blocks)]
        found = []
        for r in range(lo, hi):
            held = parts[0]
            for b in range(1, blocks):
                held = jnp.where(ranks[b] == r, parts[b], held)
            found.append(held)
        return found

    def cross(k, sub):
        d = dest(k)
        at = pl.ds(pl.multiple_of(sub * part, 8), part)
        return pltpu.make_async_remote_copy(
            src_ref=pack_a.at[2 * d + 1 - x, at], dst_ref=rx_a.at[d, at],
            send_sem=x_send, recv_sem=x_recv.at[d, sub],
            device_id={"dp": partner}, device_id_type=MESH,
        )

    def along_a(d, sub, right):
        at = pl.ds(pl.multiple_of(sub * part, 8), part)
        slot = d + 1 if right else d
        return pltpu.make_async_remote_copy(
            src_ref=pack_a.at[2 * d + x, at], dst_ref=zin_a.at[slot, at],
            send_sem=za_send, recv_sem=za_recv.at[slot, sub],
            device_id={"dp": me + 2 if right else me - 2}, device_id_type=MESH,
        )

    def along_b(d, right):
        slot = d + 1 if right else d
        return pltpu.make_async_remote_copy(
            src_ref=pack_b.at[d], dst_ref=zin_b.at[slot],
            send_sem=zb_send, recv_sem=zb_recv.at[slot],
            device_id={"dp": me + 2 if right else me - 2}, device_id_type=MESH,
        )

    def cross_b():
        return pltpu.make_async_remote_copy(
            src_ref=pack_b.at[p, pl.ds(pl.multiple_of((1 - x) * line_rows, 8), line_rows)],
            dst_ref=rx_b, send_sem=b_send, recv_sem=b_recv,
            device_id={"dp": partner}, device_id_type=MESH,
        )

    def norm_rep(t):
        return pltpu.make_async_remote_copy(
            src_ref=reps_sq.at[rep], dst_ref=reps_sq.at[rep], send_sem=nr_send, recv_sem=nr_recv,
            device_id={"rep": (rep + t) % reps}, device_id_type=MESH,
        )

    def norm_x():
        return pltpu.make_async_remote_copy(
            src_ref=pair_sq.at[x], dst_ref=pair_sq.at[x], send_sem=nx_send, recv_sem=nx_recv,
            device_id={"dp": partner}, device_id_type=MESH,
        )

    def norm_z(t):
        return pltpu.make_async_remote_copy(
            src_ref=line_sq.at[p], dst_ref=line_sq.at[p], send_sem=nz_send, recv_sem=nz_recv,
            device_id={"dp": 2 * ((p + t) % m) + x}, device_id_type=MESH,
        )

    def bytes_of(ref, send_sem, recv_sem):
        return pltpu.make_async_remote_copy(
            src_ref=ref, dst_ref=ref, send_sem=send_sem, recv_sem=recv_sem,
            device_id={"dp": partner}, device_id_type=MESH,
        )

    def token(right):
        pl.semaphore_signal(
            from_left if right else from_right, inc=1,
            device_id={"dp": me + 2 if right else me - 2}, device_id_type=MESH,
        )

    def raw_b(k):
        d = dest(k)

        @pl.when(jnp.logical_and(d > p, p == 0))
        def _():
            along_b(d, True).start()

        @pl.when(jnp.logical_and(d < p, p == m - 1))
        def _():
            along_b(d, False).start()

    def permute(lo, hi):
        for g in range(0, tokens, GROUP):
            at = slice(g, min(g + GROUP, tokens))
            for r, held in enumerate(ranked(lambda cols: og_v[at, cols], lo, hi), lo):
                og_p[at, r * LANES:(r + 1) * LANES] = held

    def product(i, lo, hi, store):
        grad = lax.dot_general(
            feat_v[i], og_p[:, lo * LANES:hi * LANES], (((0,), (0,)), ((), ())),
            preferred_element_type=jnp.float32,
        )
        squares = [sq[r] for r in range(lo, hi)]
        for g in range(0, chunk, GROUP):
            at = slice(g, g + GROUP)
            held = ranked(lambda cols: cold_v[i, at, cols], lo, hi)
            values = []
            for t in range(hi - lo):
                value = grad[at, t * LANES:(t + 1) * LANES] + held[t].astype(jnp.float32)
                for h in range(0, GROUP, 8):
                    squares[t] += value[h:h + 8] * value[h:h + 8]
                values.append(value)
            store(g, values)
        for r in range(lo, hi):
            sq[r] = squares[r - lo]

    def hot_fill(i):
        c = chunk_at(i)

        def store(g, values):
            for h in range(0, GROUP, 8):
                owner = c * inner + (g + h) // own
                row = (g + h) % own
                for r in range(hot):
                    cols = slice(r * LANES, (r + 1) * LANES)
                    if row < cross_rows:
                        pack_a[owner, row:row + 8, cols] = values[r][h:h + 8]
                    else:
                        at = pl.ds(pl.multiple_of((owner % 2) * line_rows + row - cross_rows, 8), 8)
                        pack_b[owner // 2, at, cols] = values[r][h:h + 8]

        product(i, 0, hot, store)

    def hot_step(i):
        feat_copy(i).wait()
        cold_copy(i).wait()
        hot_fill(i)
        if chunk == own:
            k = i // 2
            for sub in range(pieces):
                @pl.when(jnp.logical_and(i % 2 == 0, k * pieces + sub < FRONT))
                def _():
                    cross(k, sub).start()

            @pl.when(i % 2 == 1)
            def _():
                raw_b(k)

    def cold_step(i):
        c = chunk_at(i)

        def store(g, values):
            at = pl.ds(pl.multiple_of(c * chunk + g, 16), GROUP)
            values = [value.astype(jnp.bfloat16) for value in values]
            for b in range(blocks):
                new = jnp.zeros_like(values[0])
                for r in range(hot, blocks):
                    new = jnp.where(ranks[b] == r, values[r - hot], new)
                kept[at, b * LANES:(b + 1) * LANES] = new

        product(i, hot, blocks, store)

    state[4].wait()
    feat_copy(0).wait()
    cold_copy(0).wait()
    state[3].wait()
    permute(0, hot)
    hot_fill(0)
    greeted = (p + m - 1) // m + (2 * m - 2 - p) // m + 1 + (reps - 1)
    pl.semaphore_wait(barrier, greeted)

    @pl.when(jnp.logical_and(p == 0, m > 1))
    def _():
        token(True)

    @pl.when(jnp.logical_and(p == m - 1, m > 1))
    def _():
        token(False)

    if chunk == own:
        for sub in range(min(pieces, FRONT)):
            cross(0, sub).start()
    rolled(1, chunks, hot_step)
    for copy in state[:3]:
        copy.start()
    permute(hot, blocks)
    rolled(0, chunks, cold_step)
    if chunk != own:
        def launch(k):
            for sub in range(pieces):
                @pl.when(k * pieces + sub < FRONT)
                def _():
                    cross(k, sub).start()
            raw_b(k)

        rolled(0, m, launch)
    for r in range(blocks):
        reps_sq[rep, r:r + 1] = jnp.sum(sq[r], axis=0, keepdims=True)
    span(1, reps, lambda t: norm_rep(t).start())

    def line_step(k):
        d = dest(k)

        @pl.when(jnp.logical_and(d >= p, p > 0))
        def _():
            along_b(d, True).wait_recv()
            pack_b[d] += zin_b[d + 1]

        @pl.when(jnp.logical_and(d <= p, p < m - 1))
        def _():
            along_b(d, False).wait_recv()
            pack_b[d] += zin_b[d]

        @pl.when(jnp.logical_and(d > p, p > 0))
        def _():
            along_b(d, True).start()

        @pl.when(jnp.logical_and(d < p, p < m - 1))
        def _():
            along_b(d, False).start()

    def rest(k):
        for sub in range(pieces):
            @pl.when(k * pieces + sub >= FRONT)
            def _():
                cross(k, sub).start()

    def cross_step(k, subs=range(pieces)):
        d = dest(k)
        for sub in subs:
            at = slice(sub * part, (sub + 1) * part)
            cross(k, sub).wait_recv()
            pack_a[2 * d + x, at] += rx_a[d, at]

            @pl.when(jnp.logical_and(d >= p, p > 0))
            def _():
                along_a(d, sub, True).wait_recv()
                pack_a[2 * d + x, at] += zin_a[d + 1, at]

            @pl.when(jnp.logical_and(d <= p, p < m - 1))
            def _():
                along_a(d, sub, False).wait_recv()
                pack_a[2 * d + x, at] += zin_a[d, at]

            @pl.when(d > p)
            def _():
                along_a(d, sub, True).start()

            @pl.when(d < p)
            def _():
                along_a(d, sub, False).start()

            @pl.when(d == p)
            def _():
                summed[at] = pack_a[2 * d + x, at]

    span(0, m - 1, line_step)

    @pl.when(jnp.logical_and(p > 0, p < m - 1))
    def _():
        pl.semaphore_wait(from_right, 1)
        token(False)
        pl.semaphore_wait(from_left, 1)
        token(True)

    if m > 1:
        cross_step(0, range(1))
    bytes_of(reps_sq.at[pl.ds(0, reps - 1)], nr_send, nr_recv).wait_recv()
    total = reps_sq[0]
    for j in range(1, reps):
        total = total + reps_sq[j]
    pair_sq[x] = total
    norm_x().start()
    rolled(0, m, rest)
    if m > 1:
        cross_step(0, range(1, pieces))
    if m > 2:
        cross_step(1)
    norm_x().wait_recv()
    line_sq[p] = pair_sq[0] + pair_sq[1]

    @pl.when(jnp.logical_and(p == 0, m > 1))
    def _():
        pl.semaphore_wait(from_right, 1)

    @pl.when(jnp.logical_and(p == m - 1, m > 1))
    def _():
        pl.semaphore_wait(from_left, 1)

    span(1, m, lambda t: norm_z(t).start())
    span(2, m - 2, cross_step)
    line_step(m - 1)
    cross_b().start()
    if m > 3:
        cross_step(m - 2)
    if m > 1:
        bytes_of(line_sq.at[pl.ds(0, m - 1)], nz_send, nz_recv).wait_recv()
    everything = line_sq[0]
    for j in range(1, m):
        everything = everything + line_sq[j]
    sq_out[...] = everything
    for copy in state[:3]:
        copy.wait()
    cross_step(m - 1)
    cross_b().wait_recv()
    mine = pl.ds(pl.multiple_of(x * line_rows, 8), line_rows)
    summed[cross_rows:] = pack_b[p, mine] + rx_b[...]

    bytes_of(rx_a, x_send, x_recv.at[0, 0]).wait_send()
    if m > 1:
        bytes_of(zin_a.at[pl.ds(0, m - 1)], za_send, za_recv.at[0, 0]).wait_send()
        bytes_of(zin_b.at[pl.ds(0, m - 1)], zb_send, zb_recv.at[0]).wait_send()
        bytes_of(line_sq.at[pl.ds(0, m - 1)], nz_send, nz_recv).wait_send()
    cross_b().wait_send()
    norm_x().wait_send()
    bytes_of(reps_sq.at[pl.ds(0, reps - 1)], nr_send, nr_recv).wait_send()


def update_kernel(
    n, total_rows, tokens, hot,
    ranks_any, summed, sq, kept, weight, moment, second,
    w_hbm, m_hbm, s_hbm, nc_hbm, sq_hbm,
    ranks, fresh, sq_v, nc_sem, state_sem, sq_sem, ranks_sem,
):
    width = weight.shape[1]
    blocks = width // LANES
    outs = (w_hbm, m_hbm, s_hbm)
    copies = []

    def send(src, dst, sem):
        copies.append(pltpu.make_async_copy(src, dst, sem))
        copies[-1].start()

    order = pltpu.make_async_copy(ranks_any, ranks, ranks_sem)
    order.start()
    send(kept, nc_hbm.at[0], nc_sem)
    order.wait()
    where = [pl.ds(block_of(ranks, blocks, r), LANES) for r in range(blocks)]
    for r in range(hot, blocks):
        for i, src in enumerate((weight, moment, second)):
            send(src.at[:, where[r]], outs[i].at[:, where[r]], state_sem.at[i, r])
    for b in range(blocks):
        sq_v[b:b + 1, :] = sq[pl.ds(ranks[b], 1), :]
    send(sq_v, sq_hbm, sq_sem)
    for r in range(hot):
        cols = slice(r * LANES, (r + 1) * LANES)
        rms = jnp.sqrt(sq[r:r + 1, :] / jnp.float32(total_rows * n * tokens))
        clip = 1.0 / jnp.maximum(jnp.float32(1.0), rms)
        grad = summed[:, cols] * clip / jnp.float32(n)
        moved = 0.9 * moment[:, where[r]] + 0.1 * grad
        squared = 0.95 * second[:, where[r]] + 0.05 * grad * grad
        fresh[1, :, cols] = moved
        fresh[2, :, cols] = squared
        step = 0.05 * (moved / (1.0 - 0.9**10)) / (
            jnp.sqrt(squared / (1.0 - 0.95**10)) + 1e-08
        )
        fresh[0, :, cols] = weight[:, where[r]] - step
        for i in range(3):
            send(fresh.at[i, :, pl.ds(r * LANES, LANES)], outs[i].at[:, where[r]], state_sem.at[i, r])
    for copy in copies:
        copy.wait()


def body(n, reps, features, out_grads, cold_sums, weight, moment, second, ranks):
    tokens, rows = features.shape
    width = out_grads.shape[1]
    blocks = ranks.shape[0]
    hot = blocks // 2
    packed = hot * LANES
    m = n // 2
    own = rows // n
    chunk = max(own, LANES)
    chunks = rows // chunk
    cross_rows, line_rows, pieces = split_of(own)
    f32, bf16 = jnp.float32, jnp.bfloat16
    vmem = pl.BlockSpec(memory_space=pltpu.VMEM)
    hbm = pl.BlockSpec(memory_space=pl.ANY)
    dma = pltpu.SemaphoreType.DMA
    summed, sq, kept, w, mo, se = pl.pallas_call(
        functools.partial(exchange_kernel, n, reps, hot),
        out_shape=(
            pltpu.VMEM((own, packed), f32),
            pltpu.VMEM((blocks, LANES), f32),
            pltpu.VMEM(cold_sums.shape[1:], bf16),
            pltpu.VMEM(weight.shape, f32),
            pltpu.VMEM(weight.shape, f32),
            pltpu.VMEM(weight.shape, f32),
        ),
        in_specs=[pl.BlockSpec(memory_space=pltpu.HBM)] * 7,
        out_specs=(vmem,) * 6,
        scratch_shapes=[
            pltpu.SMEM(ranks.shape, ranks.dtype),
            pltpu.VMEM((chunks, tokens, chunk), bf16),
            pltpu.VMEM((tokens, width), bf16),
            pltpu.VMEM((tokens, width), bf16),
            pltpu.VMEM((chunks, chunk, width), bf16),
            pltpu.VMEM((n, cross_rows, packed), f32),
            pltpu.VMEM((m, 2 * line_rows, packed), f32),
            pltpu.VMEM((m, cross_rows, packed), f32),
            pltpu.VMEM((line_rows, packed), f32),
            pltpu.VMEM((m + 1, cross_rows, packed), f32),
            pltpu.VMEM((m + 1, 2 * line_rows, packed), f32),
            pltpu.VMEM((blocks, 8, LANES), f32),
            pltpu.VMEM((reps, blocks, LANES), f32),
            pltpu.VMEM((2, blocks, LANES), f32),
            pltpu.VMEM((m, blocks, LANES), f32),
            dma((2, chunks)),
            dma((5,)),
            dma,
            dma((m, pieces)),
            dma,
            dma((m + 1, pieces)),
            dma,
            dma((m + 1,)),
            dma,
            dma,
            dma,
            dma,
            dma,
            dma,
            dma,
            dma,
            pltpu.SemaphoreType.REGULAR,
            pltpu.SemaphoreType.REGULAR,
        ],
        compiler_params=pltpu.CompilerParams(
            collective_id=0, has_side_effects=True, vmem_limit_bytes=VMEM_GRANT
        ),
        name="exchange",
    )(ranks, features, out_grads, cold_sums, weight, moment, second)
    new_weight, new_moment, new_second, new_cold, column_sq = pl.pallas_call(
        functools.partial(update_kernel, n, rows * reps, tokens, hot),
        out_shape=(
            jax.ShapeDtypeStruct(weight.shape, f32),
            jax.ShapeDtypeStruct(weight.shape, f32),
            jax.ShapeDtypeStruct(weight.shape, f32),
            jax.ShapeDtypeStruct(cold_sums.shape, bf16),
            jax.ShapeDtypeStruct((blocks, LANES), f32),
        ),
        in_specs=[hbm] + [vmem] * 6,
        out_specs=(hbm,) * 5,
        scratch_shapes=[
            pltpu.SMEM(ranks.shape, ranks.dtype),
            pltpu.VMEM((3, weight.shape[0], packed), f32),
            pltpu.VMEM((blocks, LANES), f32),
            dma,
            dma((3, blocks)),
            dma,
            dma,
        ],
        compiler_params=pltpu.CompilerParams(vmem_limit_bytes=VMEM_GRANT // 2),
        name="update",
    )(ranks, summed, sq, kept, w, mo, se)
    return new_weight, new_moment, new_second, new_cold, column_sq.reshape(width)


def solution(mesh):
    owned = P(("rep", "dp"), None)
    placed = (P("dp", "rep"), P("dp", None), P("dp", "rep", None), owned, owned, owned, P())
    return jax.shard_map(
        functools.partial(body, mesh.shape["dp"], mesh.shape["rep"]),
        mesh=mesh,
        in_specs=placed,
        out_specs=(owned, owned, owned, P("dp", "rep", None), P()),
        check_vma=False,
    )
```

```python
import functools
import jax
import jax.numpy as jnp
from jax import lax
from jax.experimental import pallas as pl
from jax.experimental.pallas import tpu as pltpu
from jax.sharding import PartitionSpec as P

LANES = 128
GROUP = 32
LAG = 2
FRONT = 6
VMEM_GRANT = 55 * 2**20
MESH = pl.DeviceIdType.MESH


def split_of(own):
    line = 8 * max(round(own / 48), 1)
    cross = own - line
    pieces = next(s for s in (3, 2, 1) if cross % (8 * s) == 0)
    return cross, line, pieces


def block_of(ranks, blocks, rank):
    found = 0
    for b in range(blocks):
        gap = ranks[b] - rank
        found = found + b * (1 - jnp.minimum(gap * gap, 1))
    return found


def exchange_kernel(n, reps, hot, *refs):
    feat = refs[1]
    chunks = feat.shape[1] // max(feat.shape[1] // n, LANES)
    dma = pltpu.SemaphoreType.DMA
    pl.run_scoped(
        functools.partial(exchange_body, n, reps, hot, *refs), dma((2, chunks)), dma((5,))
    )


def exchange_body(
    n, reps, hot,
    ranks_hbm, feat, og, cold, weight, moment, second,
    summed, sq_out, kept, w_out, m_out, s_out,
    ranks, feat_v, og_v, cold_v, pack_a, pack_b, rx_a, rx_b, zin_a, zin_b, sq, reps_sq, pair_sq, line_sq,
    x_send, x_recv, za_send, za_recv, zb_send, zb_recv, b_send, b_recv,
    nr_send, nr_recv, nx_send, nx_recv, nz_send, nz_recv, from_left, from_right,
    in_sem, state_sem,
):
    m = n // 2
    tokens = feat.shape[0]
    rows, width = cold.shape[1], cold.shape[2]
    blocks = width // LANES
    packed = hot * LANES
    own = rows // n
    chunk = max(own, LANES)
    chunks = rows // chunk
    inner = chunk // own
    cross_rows, line_rows, pieces = split_of(own)
    part = cross_rows // pieces
    me = lax.axis_index("dp")
    rep = lax.axis_index("rep")
    x = me % 2
    p = me // 2
    partner = me + 1 - 2 * x

    half = max(m // 2, 1)
    flip = p // half if m > 1 else 0
    pr = p + flip * (m - 1 - 2 * p)
    lone = m - 1 - 2 * pr

    def dest(k):
        late = (k - lone + 2 * m) // (2 * m)
        pair = late * (k - lone)
        odd = pair % 2
        near = (1 - late) * (m - 1 - k) + late * ((1 - odd) * (pair // 2) + odd * (2 * pr - pair // 2))
        return near + flip * (m - 1 - 2 * near)

    def chunk_at(i):
        if chunk != own:
            return i
        side = i % 2
        return 2 * dest(i // 2) + (1 - side) * (1 - x) + side * x

    def span(lo, hi, step):
        if hi - lo <= 8:
            for k in range(lo, hi):
                step(k)
        else:
            lax.fori_loop(lo, hi, lambda k, carry: step(k) or carry, 0)

    def rolled(lo, hi, step):
        lax.fori_loop(lo, hi, lambda k, carry: step(k) or carry, 0)

    barrier = pltpu.get_barrier_semaphore()

    def feat_copy(i):
        cols = pl.ds(pl.multiple_of(chunk_at(i) * chunk, LANES), chunk)
        return pltpu.make_async_copy(feat.at[:, cols], feat_v.at[i], in_sem.at[0, i])

    def cold_copy(i):
        at = pl.ds(pl.multiple_of(chunk_at(i) * chunk, LANES), chunk)
        return pltpu.make_async_copy(cold.at[0, at], cold_v.at[i], in_sem.at[1, i])

    state = [
        pltpu.make_async_copy(src, dst, state_sem.at[i])
        for i, (src, dst) in enumerate(
            ((weight, w_out), (moment, m_out), (second, s_out), (og, og_v), (ranks_hbm, ranks))
        )
    ]
    def fetch(i):
        feat_copy(i).start()
        cold_copy(i).start()

    state[3].start()
    state[4].start()
    fetch(0)
    pl.semaphore_signal(barrier, inc=1, device_id={"dp": partner}, device_id_type=MESH)

    @pl.when(p > 0)
    def _():
        pl.semaphore_signal(barrier, inc=1, device_id={"dp": me - 2}, device_id_type=MESH)

    @pl.when(p < m - 1)
    def _():
        pl.semaphore_signal(barrier, inc=1, device_id={"dp": me + 2}, device_id_type=MESH)

    span(1, reps, lambda t: pl.semaphore_signal(
        barrier, inc=1, device_id={"rep": (rep + t) % reps}, device_id_type=MESH))
    rolled(1, chunks, fetch)

    sq[...] = jnp.zeros_like(sq)

    def cross(k, sub):
        d = dest(k)
        at = pl.ds(pl.multiple_of(sub * part, 8), part)
        return pltpu.make_async_remote_copy(
            src_ref=pack_a.at[2 * d + 1 - x, at], dst_ref=rx_a.at[d, at],
            send_sem=x_send, recv_sem=x_recv.at[d, sub],
            device_id={"dp": partner}, device_id_type=MESH,
        )

    def along_a(d, sub, right):
        at = pl.ds(pl.multiple_of(sub * part, 8), part)
        slot = d + 1 if right else d
        return pltpu.make_async_remote_copy(
            src_ref=pack_a.at[2 * d + x, at], dst_ref=zin_a.at[slot, at],
            send_sem=za_send, recv_sem=za_recv.at[slot, sub],
            device_id={"dp": me + 2 if right else me - 2}, device_id_type=MESH,
        )

    def along_b(d, s, right):
        slot = d + 1 if right else d
        at = pl.ds(pl.multiple_of(s * line_rows, 8), line_rows)
        return pltpu.make_async_remote_copy(
            src_ref=pack_b.at[d, at], dst_ref=zin_b.at[slot, at],
            send_sem=zb_send, recv_sem=zb_recv.at[slot, s],
            device_id={"dp": me + 2 if right else me - 2}, device_id_type=MESH,
        )

    def cross_b():
        return pltpu.make_async_remote_copy(
            src_ref=pack_b.at[p, pl.ds(pl.multiple_of((1 - x) * line_rows, 8), line_rows)],
            dst_ref=rx_b, send_sem=b_send, recv_sem=b_recv,
            device_id={"dp": partner}, device_id_type=MESH,
        )

    def norm_rep(t):
        return pltpu.make_async_remote_copy(
            src_ref=reps_sq.at[rep], dst_ref=reps_sq.at[rep], send_sem=nr_send, recv_sem=nr_recv,
            device_id={"rep": (rep + t) % reps}, device_id_type=MESH,
        )

    def norm_x():
        return pltpu.make_async_remote_copy(
            src_ref=pair_sq.at[x], dst_ref=pair_sq.at[x], send_sem=nx_send, recv_sem=nx_recv,
            device_id={"dp": partner}, device_id_type=MESH,
        )

    def norm_z(t):
        return pltpu.make_async_remote_copy(
            src_ref=line_sq.at[p], dst_ref=line_sq.at[p], send_sem=nz_send, recv_sem=nz_recv,
            device_id={"dp": 2 * ((p + t) % m) + x}, device_id_type=MESH,
        )

    def bytes_of(ref, send_sem, recv_sem):
        return pltpu.make_async_remote_copy(
            src_ref=ref, dst_ref=ref, send_sem=send_sem, recv_sem=recv_sem,
            device_id={"dp": partner}, device_id_type=MESH,
        )

    def token(right):
        pl.semaphore_signal(
            from_left if right else from_right, inc=1,
            device_id={"dp": me + 2 if right else me - 2}, device_id_type=MESH,
        )

    def raw_b(d, s):
        @pl.when(jnp.logical_and(d > p, p == 0))
        def _():
            along_b(d, s, True).start()

        @pl.when(jnp.logical_and(d < p, p == m - 1))
        def _():
            along_b(d, s, False).start()

    def cross_step(k, subs=range(pieces)):
        d = dest(k)
        for sub in subs:
            at = slice(sub * part, (sub + 1) * part)
            cross(k, sub).wait_recv()
            pack_a[2 * d + x, at] += rx_a[d, at]

            @pl.when(jnp.logical_and(d >= p, p > 0))
            def _():
                along_a(d, sub, True).wait_recv()
                pack_a[2 * d + x, at] += zin_a[d + 1, at]

            @pl.when(jnp.logical_and(d <= p, p < m - 1))
            def _():
                along_a(d, sub, False).wait_recv()
                pack_a[2 * d + x, at] += zin_a[d, at]

            @pl.when(d > p)
            def _():
                along_a(d, sub, True).start()

            @pl.when(d < p)
            def _():
                along_a(d, sub, False).start()

            @pl.when(d == p)
            def _():
                summed[at] = pack_a[2 * d + x, at]

    def fill(i, first=0, last=chunk):
        c = chunk_at(i)
        grad = lax.dot_general(
            feat_v[i, :, first:last], og_v[...], (((0,), (0,)), ((), ())),
            preferred_element_type=jnp.float32,
        )
        squares = [sq[b] for b in range(blocks)]
        for g in range(first, last, GROUP):
            values = []
            for b in range(blocks):
                cols = slice(b * LANES, (b + 1) * LANES)
                value = grad[g - first:g - first + GROUP, cols]
                value += cold_v[i, g:g + GROUP, cols].astype(jnp.float32)
                for h in range(0, GROUP, 8):
                    squares[b] += value[h:h + 8] * value[h:h + 8]
                values.append(value)
            at = pl.ds(pl.multiple_of(c * chunk + g, 16), GROUP)
            for b in range(blocks):
                kept[at, b * LANES:(b + 1) * LANES] = jnp.where(
                    ranks[b] < hot, jnp.zeros_like(values[b]), values[b]).astype(jnp.bfloat16)
            for r in range(hot):
                cols = slice(r * LANES, (r + 1) * LANES)
                held = values[0]
                for b in range(1, blocks):
                    held = jnp.where(ranks[b] == r, values[b], held)
                for h in range(0, GROUP, 8):
                    owner = c * inner + (g + h) // own
                    row = (g + h) % own
                    if row < cross_rows:
                        pack_a[owner, row:row + 8, cols] = held[h:h + 8]
                    else:
                        to = pl.ds(pl.multiple_of((owner % 2) * line_rows + row - cross_rows, 8), 8)
                        pack_b[owner // 2, to, cols] = held[h:h + 8]
        for b in range(blocks):
            sq[b] = squares[b]

    def step(i):
        feat_copy(i).wait()
        cold_copy(i).wait()
        fill(i)
        if chunk == own:
            send_cross(i)
            raw_b(dest(i // 2), chunk_at(i) % 2)

    def send_cross(i):
        k = (i - lag) // 2
        for sub in range(pieces):
            @pl.when((i >= lag) & ((i - lag) % 2 == 0) & (k * pieces + sub < FRONT))
            def _():
                cross(k, sub).start()

    state[4].wait()
    state[3].wait()
    feat_copy(0).wait()
    cold_copy(0).wait()
    early = LANES if chunk == own else chunk
    fill(0, 0, early)
    greeted = (p + m - 1) // m + (2 * m - 2 - p) // m + 1 + (reps - 1)
    pl.semaphore_wait(barrier, greeted)

    @pl.when(jnp.logical_and(p == 0, m > 1))
    def _():
        token(True)

    @pl.when(jnp.logical_and(p == m - 1, m > 1))
    def _():
        token(False)

    lag = rep % 2 * LAG
    if chunk == own:
        ready = [sub for sub in range(pieces) if (sub + 1) * part <= early]
        rest_of = [sub for sub in range(pieces) if (sub + 1) * part > early]

        def start_early(subs):
            @pl.when(lag == 0)
            def _():
                for sub in subs:
                    cross(0, sub).start()

        start_early(ready)
        if early < chunk:
            fill(0, early, chunk)
        start_early(rest_of)
        raw_b(dest(0), 1 - x)
    rolled(1, chunks, step)
    for copy in state[:3]:
        copy.start()
    if chunk != own:
        def launch(k):
            for sub in range(pieces):
                @pl.when(k * pieces + sub < FRONT)
                def _():
                    cross(k, sub).start()
            for s in range(2):
                raw_b(dest(k), s)

        rolled(0, m, launch)
    for r in range(blocks):
        reps_sq[rep, r:r + 1] = jnp.sum(sq[r], axis=0, keepdims=True)
    span(1, reps, lambda t: norm_rep(t).start())

    def line_step(k):
        d = dest(k)
        for s in range(2):
            at = slice(s * line_rows, (s + 1) * line_rows)

            @pl.when(jnp.logical_and(d >= p, p > 0))
            def _():
                along_b(d, s, True).wait_recv()
                pack_b[d, at] += zin_b[d + 1, at]

            @pl.when(jnp.logical_and(d <= p, p < m - 1))
            def _():
                along_b(d, s, False).wait_recv()
                pack_b[d, at] += zin_b[d, at]

            @pl.when(jnp.logical_and(d > p, p > 0))
            def _():
                along_b(d, s, True).start()

            @pl.when(jnp.logical_and(d < p, p < m - 1))
            def _():
                along_b(d, s, False).start()

    def rest(k):
        for sub in range(pieces):
            @pl.when(k * pieces + sub >= FRONT)
            def _():
                cross(k, sub).start()

    span(0, m - 1, line_step)

    @pl.when(jnp.logical_and(p > 0, p < m - 1))
    def _():
        pl.semaphore_wait(from_right, 1)
        token(False)
        pl.semaphore_wait(from_left, 1)
        token(True)

    if m > 1:
        cross_step(0, range(1))
    bytes_of(reps_sq.at[pl.ds(0, reps - 1)], nr_send, nr_recv).wait_recv()
    total = reps_sq[0]
    for j in range(1, reps):
        total = total + reps_sq[j]
    pair_sq[x] = total
    norm_x().start()
    rolled(0, m, rest)
    if m > 1:
        cross_step(0, range(1, pieces))
    if m > 2:
        cross_step(1)
    norm_x().wait_recv()
    line_sq[p] = pair_sq[0] + pair_sq[1]

    @pl.when(jnp.logical_and(p == 0, m > 1))
    def _():
        pl.semaphore_wait(from_right, 1)

    @pl.when(jnp.logical_and(p == m - 1, m > 1))
    def _():
        pl.semaphore_wait(from_left, 1)

    span(1, m, lambda t: norm_z(t).start())
    span(2, m - 2, cross_step)
    line_step(m - 1)
    cross_b().start()
    if m > 3:
        cross_step(m - 2)
    if m > 1:
        bytes_of(line_sq.at[pl.ds(0, m - 1)], nz_send, nz_recv).wait_recv()
    everything = line_sq[0]
    for j in range(1, m):
        everything = everything + line_sq[j]
    sq_out[...] = everything
    for copy in state[:3]:
        copy.wait()
    cross_step(m - 1)
    cross_b().wait_recv()
    mine = pl.ds(pl.multiple_of(x * line_rows, 8), line_rows)
    summed[cross_rows:] = pack_b[p, mine] + rx_b[...]

    bytes_of(rx_a, x_send, x_recv.at[0, 0]).wait_send()
    if m > 1:
        bytes_of(zin_a.at[pl.ds(0, m - 1)], za_send, za_recv.at[0, 0]).wait_send()
        bytes_of(zin_b.at[pl.ds(0, m - 1)], zb_send, zb_recv.at[0, 0]).wait_send()
        bytes_of(line_sq.at[pl.ds(0, m - 1)], nz_send, nz_recv).wait_send()
    cross_b().wait_send()
    norm_x().wait_send()
    bytes_of(reps_sq.at[pl.ds(0, reps - 1)], nr_send, nr_recv).wait_send()


def update_kernel(
    n, total_rows, tokens, hot,
    ranks_any, summed, sq, kept, weight, moment, second,
    w_hbm, m_hbm, s_hbm, nc_hbm, sq_hbm,
    ranks, fresh, nc_sem, state_sem, sq_sem, ranks_sem,
):
    width = weight.shape[1]
    blocks = width // LANES
    outs = (w_hbm, m_hbm, s_hbm)
    copies = []

    def send(src, dst, sem):
        copies.append(pltpu.make_async_copy(src, dst, sem))
        copies[-1].start()

    order = pltpu.make_async_copy(ranks_any, ranks, ranks_sem)
    order.start()
    send(kept, nc_hbm.at[0], nc_sem)
    send(sq, sq_hbm, sq_sem)
    order.wait()
    block = [block_of(ranks, blocks, r) for r in range(blocks)]
    where = [pl.ds(pl.multiple_of(b * LANES, LANES), LANES) for b in block]
    for r in range(hot, blocks):
        for i, src in enumerate((weight, moment, second)):
            send(src.at[:, where[r]], outs[i].at[:, where[r]], state_sem.at[i, r])
    for r in range(hot):
        cols = slice(r * LANES, (r + 1) * LANES)
        rms = jnp.sqrt(sq[pl.ds(block[r], 1), :] / jnp.float32(total_rows * n * tokens))
        clip = 1.0 / jnp.maximum(jnp.float32(1.0), rms)
        grad = summed[:, cols] * clip / jnp.float32(n)
        moved = 0.9 * moment[:, where[r]] + 0.1 * grad
        squared = 0.95 * second[:, where[r]] + 0.05 * grad * grad
        fresh[1, :, cols] = moved
        fresh[2, :, cols] = squared
        step = 0.05 * (moved / (1.0 - 0.9**10)) / (
            jnp.sqrt(squared / (1.0 - 0.95**10)) + 1e-08
        )
        fresh[0, :, cols] = weight[:, where[r]] - step
        for i in range(3):
            send(fresh.at[i, :, pl.ds(r * LANES, LANES)], outs[i].at[:, where[r]], state_sem.at[i, r])
    for copy in copies:
        copy.wait()


def body(n, reps, features, out_grads, cold_sums, weight, moment, second, ranks):
    tokens, rows = features.shape
    width = out_grads.shape[1]
    blocks = ranks.shape[0]
    hot = blocks // 2
    packed = hot * LANES
    m = n // 2
    own = rows // n
    chunk = max(own, LANES)
    chunks = rows // chunk
    cross_rows, line_rows, pieces = split_of(own)
    f32, bf16 = jnp.float32, jnp.bfloat16
    vmem = pl.BlockSpec(memory_space=pltpu.VMEM)
    hbm = pl.BlockSpec(memory_space=pl.ANY)
    dma = pltpu.SemaphoreType.DMA
    summed, sq, kept, w, mo, se = pl.pallas_call(
        functools.partial(exchange_kernel, n, reps, hot),
        out_shape=(
            pltpu.VMEM((own, packed), f32),
            pltpu.VMEM((blocks, LANES), f32),
            pltpu.VMEM(cold_sums.shape[1:], bf16),
            pltpu.VMEM(weight.shape, f32),
            pltpu.VMEM(weight.shape, f32),
            pltpu.VMEM(weight.shape, f32),
        ),
        in_specs=[pl.BlockSpec(memory_space=pltpu.HBM)] * 7,
        out_specs=(vmem,) * 6,
        scratch_shapes=[
            pltpu.SMEM(ranks.shape, ranks.dtype),
            pltpu.VMEM((chunks, tokens, chunk), bf16),
            pltpu.VMEM((tokens, width), bf16),
            pltpu.VMEM((chunks, chunk, width), bf16),
            pltpu.VMEM((n, cross_rows, packed), f32),
            pltpu.VMEM((m, 2 * line_rows, packed), f32),
            pltpu.VMEM((m, cross_rows, packed), f32),
            pltpu.VMEM((line_rows, packed), f32),
            pltpu.VMEM((m + 1, cross_rows, packed), f32),
            pltpu.VMEM((m + 1, 2 * line_rows, packed), f32),
            pltpu.VMEM((blocks, 8, LANES), f32),
            pltpu.VMEM((reps, blocks, LANES), f32),
            pltpu.VMEM((2, blocks, LANES), f32),
            pltpu.VMEM((m, blocks, LANES), f32),
            dma,
            dma((m, pieces)),
            dma,
            dma((m + 1, pieces)),
            dma,
            dma((m + 1, 2)),
            dma,
            dma,
            dma,
            dma,
            dma,
            dma,
            dma,
            dma,
            pltpu.SemaphoreType.REGULAR,
            pltpu.SemaphoreType.REGULAR,
        ],
        compiler_params=pltpu.CompilerParams(
            collective_id=0, has_side_effects=True, vmem_limit_bytes=VMEM_GRANT
        ),
        name="exchange",
    )(ranks, features, out_grads, cold_sums, weight, moment, second)
    new_weight, new_moment, new_second, new_cold, column_sq = pl.pallas_call(
        functools.partial(update_kernel, n, rows * reps, tokens, hot),
        out_shape=(
            jax.ShapeDtypeStruct(weight.shape, f32),
            jax.ShapeDtypeStruct(weight.shape, f32),
            jax.ShapeDtypeStruct(weight.shape, f32),
            jax.ShapeDtypeStruct(cold_sums.shape, bf16),
            jax.ShapeDtypeStruct((blocks, LANES), f32),
        ),
        in_specs=[hbm] + [vmem] * 6,
        out_specs=(hbm,) * 5,
        scratch_shapes=[
            pltpu.SMEM(ranks.shape, ranks.dtype),
            pltpu.VMEM((3, weight.shape[0], packed), f32),
            dma,
            dma((3, blocks)),
            dma,
            dma,
        ],
        compiler_params=pltpu.CompilerParams(vmem_limit_bytes=VMEM_GRANT // 2),
        name="update",
    )(ranks, summed, sq, kept, w, mo, se)
    return new_weight, new_moment, new_second, new_cold, column_sq.reshape(width)


def solution(mesh):
    owned = P(("rep", "dp"), None)
    placed = (P("dp", "rep"), P("dp", None), P("dp", "rep", None), owned, owned, owned, P())
    return jax.shard_map(
        functools.partial(body, mesh.shape["dp"], mesh.shape["rep"]),
        mesh=mesh,
        in_specs=placed,
        out_specs=(owned, owned, owned, P("dp", "rep", None), P()),
        check_vma=False,
    )
```

```python
import functools
import jax
import jax.numpy as jnp
from jax import lax
from jax.experimental import pallas as pl
from jax.experimental.pallas import tpu as pltpu
from jax.sharding import PartitionSpec as P

LANES = 128
GROUP = 32
EXTRA = 86
LAG = 2
FRONT = 6
VMEM_GRANT = 55 * 2**20
MESH = pl.DeviceIdType.MESH


def split_of(own):
    line = 8 * max(round(own / 48), 1)
    cross = own - line
    extra = 8 * max(round(own / EXTRA), 1)
    head = 8 * ((cross - extra + 8) // 16)
    return cross, line, ((0, head), (head, cross - extra - head), (cross - extra, extra))


def block_of(ranks, blocks, rank):
    found = 0
    for b in range(blocks):
        gap = ranks[b] - rank
        found = found + b * (1 - jnp.minimum(gap * gap, 1))
    return found


def exchange_kernel(n, reps, hot, *refs):
    feat = refs[1]
    chunks = feat.shape[1] // max(feat.shape[1] // n, LANES)
    dma = pltpu.SemaphoreType.DMA
    pl.run_scoped(
        functools.partial(exchange_body, n, reps, hot, *refs), dma((2, chunks)), dma((5,))
    )


def exchange_body(
    n, reps, hot,
    ranks_hbm, feat, og, cold, weight, moment, second,
    summed, sq_out, kept, w_out, m_out, s_out,
    ranks, feat_v, og_v, cold_v, pack_a, pack_b, rx_a, rx_b, rx_e, zin_a, zin_b, zin_e, sq, reps_sq, pair_sq, line_sq,
    x_send, xe_send, x_recv, zx_send, ze_send, ze_recv, be_send, be_recv, za_send, za_recv, zb_send, zb_recv, b_send, b_recv,
    nr_send, nr_recv, nx_send, nx_recv, nz_send, nz_recv, from_left, from_right,
    in_sem, state_sem,
):
    m = n // 2
    tokens = feat.shape[0]
    rows, width = cold.shape[1], cold.shape[2]
    blocks = width // LANES
    packed = hot * LANES
    own = rows // n
    chunk = max(own, LANES)
    chunks = rows // chunk
    inner = chunk // own
    cross_rows, line_rows, pieces = split_of(own)
    subs_all = range(len(pieces))
    kept_rows, extra_rows = pieces[-1]
    extra = slice(kept_rows, cross_rows)
    me = lax.axis_index("dp")
    rep = lax.axis_index("rep")
    x = me % 2
    p = me // 2
    partner = me + 1 - 2 * x

    half = max(m // 2, 1)
    flip = p // half if m > 1 else 0
    pr = p + flip * (m - 1 - 2 * p)
    lone = m - 1 - 2 * pr

    def dest(k):
        late = (k - lone + 2 * m) // (2 * m)
        pair = late * (k - lone)
        odd = pair % 2
        near = (1 - late) * (m - 1 - k) + late * ((1 - odd) * (pair // 2) + odd * (2 * pr - pair // 2))
        return near + flip * (m - 1 - 2 * near)

    def chunk_at(i):
        if chunk != own:
            return i
        side = i % 2
        return 2 * dest(i // 2) + (1 - side) * (1 - x) + side * x

    def span(lo, hi, step):
        if hi - lo <= 8:
            for k in range(lo, hi):
                step(k)
        else:
            lax.fori_loop(lo, hi, lambda k, carry: step(k) or carry, 0)

    def rolled(lo, hi, step):
        lax.fori_loop(lo, hi, lambda k, carry: step(k) or carry, 0)

    barrier = pltpu.get_barrier_semaphore()

    def feat_copy(i):
        cols = pl.ds(pl.multiple_of(chunk_at(i) * chunk, LANES), chunk)
        return pltpu.make_async_copy(feat.at[:, cols], feat_v.at[i], in_sem.at[0, i])

    def cold_copy(i):
        at = pl.ds(pl.multiple_of(chunk_at(i) * chunk, LANES), chunk)
        return pltpu.make_async_copy(cold.at[0, at], cold_v.at[i], in_sem.at[1, i])

    state = [
        pltpu.make_async_copy(src, dst, state_sem.at[i])
        for i, (src, dst) in enumerate(
            ((weight, w_out), (moment, m_out), (second, s_out), (og, og_v), (ranks_hbm, ranks))
        )
    ]
    def fetch(i):
        feat_copy(i).start()
        cold_copy(i).start()

    state[3].start()
    state[4].start()
    fetch(0)
    pl.semaphore_signal(barrier, inc=1, device_id={"dp": partner}, device_id_type=MESH)

    @pl.when(p > 0)
    def _():
        pl.semaphore_signal(barrier, inc=1, device_id={"dp": me - 2}, device_id_type=MESH)

    @pl.when(p < m - 1)
    def _():
        pl.semaphore_signal(barrier, inc=1, device_id={"dp": me + 2}, device_id_type=MESH)

    span(1, reps, lambda t: pl.semaphore_signal(
        barrier, inc=1, device_id={"rep": (rep + t) % reps}, device_id_type=MESH))
    rolled(1, chunks, fetch)

    sq[...] = jnp.zeros_like(sq)

    def cross(k, sub):
        d = dest(k)
        at = pl.ds(*pieces[sub])
        return pltpu.make_async_remote_copy(
            src_ref=pack_a.at[2 * d + 1 - x, at], dst_ref=rx_a.at[d, at],
            send_sem=xe_send if sub == subs_all[-1] else x_send, recv_sem=x_recv.at[d, sub],
            device_id={"dp": partner}, device_id_type=MESH,
        )

    def start_cross(k, sub):
        if sub == subs_all[-1]:
            @pl.when(dest(k) != m - 1)
            def _():
                cross(k, sub).start()
        else:
            cross(k, sub).start()

    def along_a(d, sub, right):
        at = pl.ds(*pieces[sub])
        slot = d + 1 if right else d
        return pltpu.make_async_remote_copy(
            src_ref=pack_a.at[2 * d + x, at], dst_ref=zin_a.at[slot, at],
            send_sem=zx_send if sub == subs_all[-1] else za_send, recv_sem=za_recv.at[slot, sub],
            device_id={"dp": me + 2 if right else me - 2}, device_id_type=MESH,
        )

    def along_e(s):
        return pltpu.make_async_remote_copy(
            src_ref=pack_a.at[2 * (m - 1) + s, pl.ds(kept_rows, extra_rows)], dst_ref=zin_e.at[s],
            send_sem=ze_send, recv_sem=ze_recv.at[s],
            device_id={"dp": me + 2}, device_id_type=MESH,
        )

    def cross_e():
        return pltpu.make_async_remote_copy(
            src_ref=pack_a.at[2 * (m - 1) + 1 - x, pl.ds(kept_rows, extra_rows)], dst_ref=rx_e,
            send_sem=be_send, recv_sem=be_recv,
            device_id={"dp": partner}, device_id_type=MESH,
        )

    def along_b(d, s, right):
        slot = d + 1 if right else d
        at = pl.ds(pl.multiple_of(s * line_rows, 8), line_rows)
        return pltpu.make_async_remote_copy(
            src_ref=pack_b.at[d, at], dst_ref=zin_b.at[slot, at],
            send_sem=zb_send, recv_sem=zb_recv.at[slot, s],
            device_id={"dp": me + 2 if right else me - 2}, device_id_type=MESH,
        )

    def cross_b():
        return pltpu.make_async_remote_copy(
            src_ref=pack_b.at[p, pl.ds(pl.multiple_of((1 - x) * line_rows, 8), line_rows)],
            dst_ref=rx_b, send_sem=b_send, recv_sem=b_recv,
            device_id={"dp": partner}, device_id_type=MESH,
        )

    def norm_rep(t):
        return pltpu.make_async_remote_copy(
            src_ref=reps_sq.at[rep], dst_ref=reps_sq.at[rep], send_sem=nr_send, recv_sem=nr_recv,
            device_id={"rep": (rep + t) % reps}, device_id_type=MESH,
        )

    def norm_x():
        return pltpu.make_async_remote_copy(
            src_ref=pair_sq.at[x], dst_ref=pair_sq.at[x], send_sem=nx_send, recv_sem=nx_recv,
            device_id={"dp": partner}, device_id_type=MESH,
        )

    def norm_z(t):
        return pltpu.make_async_remote_copy(
            src_ref=line_sq.at[p], dst_ref=line_sq.at[p], send_sem=nz_send, recv_sem=nz_recv,
            device_id={"dp": 2 * ((p + t) % m) + x}, device_id_type=MESH,
        )

    def bytes_of(ref, send_sem, recv_sem):
        return pltpu.make_async_remote_copy(
            src_ref=ref, dst_ref=ref, send_sem=send_sem, recv_sem=recv_sem,
            device_id={"dp": partner}, device_id_type=MESH,
        )

    def token(right):
        pl.semaphore_signal(
            from_left if right else from_right, inc=1,
            device_id={"dp": me + 2 if right else me - 2}, device_id_type=MESH,
        )

    def raw_b(d, s):
        @pl.when(jnp.logical_and(d > p, p == 0))
        def _():
            along_b(d, s, True).start()

        @pl.when((d == m - 1) & (d > p) & (p == 0))
        def _():
            along_e(s).start()

        @pl.when(jnp.logical_and(d < p, p == m - 1))
        def _():
            along_b(d, s, False).start()

    def cross_step(k, subs=subs_all):
        d = dest(k)
        for sub in subs:
            if sub == subs_all[-1]:
                @pl.when(d != m - 1)
                def _():
                    cross_piece(k, d, sub)
            else:
                cross_piece(k, d, sub)

    def cross_piece(k, d, sub):
        at = slice(pieces[sub][0], sum(pieces[sub]))
        cross(k, sub).wait_recv()
        pack_a[2 * d + x, at] += rx_a[d, at]

        @pl.when(jnp.logical_and(d >= p, p > 0))
        def _():
            along_a(d, sub, True).wait_recv()
            pack_a[2 * d + x, at] += zin_a[d + 1, at]

        @pl.when(jnp.logical_and(d <= p, p < m - 1))
        def _():
            along_a(d, sub, False).wait_recv()
            pack_a[2 * d + x, at] += zin_a[d, at]

        @pl.when(d > p)
        def _():
            along_a(d, sub, True).start()

        @pl.when(d < p)
        def _():
            along_a(d, sub, False).start()

        @pl.when(d == p)
        def _():
            summed[at] = pack_a[2 * d + x, at]

    def fill(i, first=0, last=chunk):
        c = chunk_at(i)
        grad = lax.dot_general(
            feat_v[i, :, first:last], og_v[...], (((0,), (0,)), ((), ())),
            preferred_element_type=jnp.float32,
        )
        squares = [sq[b] for b in range(blocks)]
        for g in range(first, last, GROUP):
            values = []
            for b in range(blocks):
                cols = slice(b * LANES, (b + 1) * LANES)
                value = grad[g - first:g - first + GROUP, cols]
                value += cold_v[i, g:g + GROUP, cols].astype(jnp.float32)
                for h in range(0, GROUP, 8):
                    squares[b] += value[h:h + 8] * value[h:h + 8]
                values.append(value)
            at = pl.ds(pl.multiple_of(c * chunk + g, 16), GROUP)
            for b in range(blocks):
                kept[at, b * LANES:(b + 1) * LANES] = jnp.where(
                    ranks[b] < hot, jnp.zeros_like(values[b]), values[b]).astype(jnp.bfloat16)
            for r in range(hot):
                cols = slice(r * LANES, (r + 1) * LANES)
                held = values[0]
                for b in range(1, blocks):
                    held = jnp.where(ranks[b] == r, values[b], held)
                for h in range(0, GROUP, 8):
                    owner = c * inner + (g + h) // own
                    row = (g + h) % own
                    if row < cross_rows:
                        pack_a[owner, row:row + 8, cols] = held[h:h + 8]
                    else:
                        to = pl.ds(pl.multiple_of((owner % 2) * line_rows + row - cross_rows, 8), 8)
                        pack_b[owner // 2, to, cols] = held[h:h + 8]
        for b in range(blocks):
            sq[b] = squares[b]

    def step(i):
        feat_copy(i).wait()
        cold_copy(i).wait()
        fill(i)
        if chunk == own:
            send_cross(i)
            raw_b(dest(i // 2), chunk_at(i) % 2)

    def send_cross(i):
        k = (i - lag) // 2
        for sub in subs_all:
            @pl.when((i >= lag) & ((i - lag) % 2 == 0) & (k * len(pieces) + sub < FRONT))
            def _():
                start_cross(k, sub)

    state[4].wait()
    state[3].wait()
    feat_copy(0).wait()
    cold_copy(0).wait()
    early = LANES if chunk == own else chunk
    fill(0, 0, early)
    greeted = (p + m - 1) // m + (2 * m - 2 - p) // m + 1 + (reps - 1)
    pl.semaphore_wait(barrier, greeted)

    @pl.when(jnp.logical_and(p == 0, m > 1))
    def _():
        token(True)

    @pl.when(jnp.logical_and(p == m - 1, m > 1))
    def _():
        token(False)

    lag = rep % 2 * LAG
    if chunk == own:
        ready = [sub for sub in subs_all if sum(pieces[sub]) <= early]
        rest_of = [sub for sub in subs_all if sum(pieces[sub]) > early]

        def start_early(subs):
            @pl.when(lag == 0)
            def _():
                for sub in subs:
                    start_cross(0, sub)

        start_early(ready)
        if early < chunk:
            fill(0, early, chunk)
        start_early(rest_of)
        raw_b(dest(0), 1 - x)
    rolled(1, chunks, step)
    for copy in state[:3]:
        copy.start()
    if chunk != own:
        def launch(k):
            for sub in subs_all:
                @pl.when(k * len(pieces) + sub < FRONT)
                def _():
                    start_cross(k, sub)
            for s in range(2):
                raw_b(dest(k), s)

        rolled(0, m, launch)
    for r in range(blocks):
        reps_sq[rep, r:r + 1] = jnp.sum(sq[r], axis=0, keepdims=True)
    span(1, reps, lambda t: norm_rep(t).start())

    def line_step(k):
        d = dest(k)
        for s in range(2):
            at = slice(s * line_rows, (s + 1) * line_rows)

            @pl.when(jnp.logical_and(d >= p, p > 0))
            def _():
                along_b(d, s, True).wait_recv()
                pack_b[d, at] += zin_b[d + 1, at]

            @pl.when(jnp.logical_and(d <= p, p < m - 1))
            def _():
                along_b(d, s, False).wait_recv()
                pack_b[d, at] += zin_b[d, at]

            @pl.when(jnp.logical_and(d > p, p > 0))
            def _():
                along_b(d, s, True).start()

            @pl.when(jnp.logical_and(d < p, p < m - 1))
            def _():
                along_b(d, s, False).start()

            @pl.when((d == m - 1) & (p > 0))
            def _():
                along_e(s).wait_recv()
                pack_a[2 * d + s, extra] += zin_e[s]

            @pl.when((d == m - 1) & (p > 0) & (p < m - 1))
            def _():
                along_e(s).start()

    def rest(k):
        for sub in subs_all:
            @pl.when(k * len(pieces) + sub >= FRONT)
            def _():
                start_cross(k, sub)

    span(0, m - 1, line_step)

    @pl.when(jnp.logical_and(p > 0, p < m - 1))
    def _():
        pl.semaphore_wait(from_right, 1)
        token(False)
        pl.semaphore_wait(from_left, 1)
        token(True)

    if m > 1:
        cross_step(0, range(1))
    bytes_of(reps_sq.at[pl.ds(0, reps - 1)], nr_send, nr_recv).wait_recv()
    total = reps_sq[0]
    for j in range(1, reps):
        total = total + reps_sq[j]
    pair_sq[x] = total
    norm_x().start()
    rolled(0, m, rest)
    if m > 1:
        cross_step(0, subs_all[1:])
    if m > 2:
        cross_step(1)
    norm_x().wait_recv()
    line_sq[p] = pair_sq[0] + pair_sq[1]

    @pl.when(jnp.logical_and(p == 0, m > 1))
    def _():
        pl.semaphore_wait(from_right, 1)

    @pl.when(jnp.logical_and(p == m - 1, m > 1))
    def _():
        pl.semaphore_wait(from_left, 1)

    span(1, m, lambda t: norm_z(t).start())
    span(2, m - 2, cross_step)
    line_step(m - 1)
    cross_b().start()

    @pl.when(p == m - 1)
    def _():
        cross_e().start()

    if m > 3:
        cross_step(m - 2)
    if m > 1:
        bytes_of(line_sq.at[pl.ds(0, m - 1)], nz_send, nz_recv).wait_recv()
    everything = line_sq[0]
    for j in range(1, m):
        everything = everything + line_sq[j]
    sq_out[...] = everything
    for copy in state[:3]:
        copy.wait()
    cross_step(m - 1)
    cross_b().wait_recv()
    mine = pl.ds(pl.multiple_of(x * line_rows, 8), line_rows)
    summed[cross_rows:] = pack_b[p, mine] + rx_b[...]

    @pl.when(p == m - 1)
    def _():
        cross_e().wait_recv()
        summed[extra] = pack_a[2 * p + x, extra] + rx_e[...]
        cross_e().wait_send()


    main, tail = pl.ds(0, kept_rows), pl.ds(kept_rows, extra_rows)
    bytes_of(rx_a.at[:, main], x_send, x_recv.at[0, 0]).wait_send()
    if m > 1:
        bytes_of(rx_a.at[pl.ds(0, m - 1), tail], xe_send, x_recv.at[0, 0]).wait_send()
        bytes_of(zin_a.at[pl.ds(0, m - 1), main], za_send, za_recv.at[0, 0]).wait_send()
        bytes_of(zin_b.at[pl.ds(0, m - 1)], zb_send, zb_recv.at[0, 0]).wait_send()
        bytes_of(line_sq.at[pl.ds(0, m - 1)], nz_send, nz_recv).wait_send()

        @pl.when(p == m - 1)
        def _():
            bytes_of(zin_a.at[pl.ds(0, m - 1), tail], zx_send, za_recv.at[0, 0]).wait_send()

        @pl.when(p < m - 1)
        def _():
            if m > 2:
                bytes_of(zin_a.at[pl.ds(0, m - 2), tail], zx_send, za_recv.at[0, 0]).wait_send()
            bytes_of(zin_e, ze_send, ze_recv.at[0]).wait_send()

    cross_b().wait_send()
    norm_x().wait_send()
    bytes_of(reps_sq.at[pl.ds(0, reps - 1)], nr_send, nr_recv).wait_send()


def update_kernel(
    n, total_rows, tokens, hot,
    ranks_any, summed, sq, kept, weight, moment, second,
    w_hbm, m_hbm, s_hbm, nc_hbm, sq_hbm,
    ranks, fresh, nc_sem, state_sem, sq_sem, ranks_sem,
):
    width = weight.shape[1]
    blocks = width // LANES
    outs = (w_hbm, m_hbm, s_hbm)
    copies = []

    def send(src, dst, sem):
        copies.append(pltpu.make_async_copy(src, dst, sem))
        copies[-1].start()

    order = pltpu.make_async_copy(ranks_any, ranks, ranks_sem)
    order.start()
    send(kept, nc_hbm.at[0], nc_sem)
    send(sq, sq_hbm, sq_sem)
    order.wait()
    block = [block_of(ranks, blocks, r) for r in range(blocks)]
    where = [pl.ds(pl.multiple_of(b * LANES, LANES), LANES) for b in block]
    for r in range(hot, blocks):
        for i, src in enumerate((weight, moment, second)):
            send(src.at[:, where[r]], outs[i].at[:, where[r]], state_sem.at[i, r])
    for r in range(hot):
        cols = slice(r * LANES, (r + 1) * LANES)
        rms = jnp.sqrt(sq[pl.ds(block[r], 1), :] / jnp.float32(total_rows * n * tokens))
        clip = 1.0 / jnp.maximum(jnp.float32(1.0), rms)
        grad = summed[:, cols] * clip / jnp.float32(n)
        moved = 0.9 * moment[:, where[r]] + 0.1 * grad
        squared = 0.95 * second[:, where[r]] + 0.05 * grad * grad
        fresh[1, :, cols] = moved
        fresh[2, :, cols] = squared
        step = 0.05 * (moved / (1.0 - 0.9**10)) / (
            jnp.sqrt(squared / (1.0 - 0.95**10)) + 1e-08
        )
        fresh[0, :, cols] = weight[:, where[r]] - step
        for i in range(3):
            send(fresh.at[i, :, pl.ds(r * LANES, LANES)], outs[i].at[:, where[r]], state_sem.at[i, r])
    for copy in copies:
        copy.wait()


def body(n, reps, features, out_grads, cold_sums, weight, moment, second, ranks):
    tokens, rows = features.shape
    width = out_grads.shape[1]
    blocks = ranks.shape[0]
    hot = blocks // 2
    packed = hot * LANES
    m = n // 2
    own = rows // n
    chunk = max(own, LANES)
    chunks = rows // chunk
    cross_rows, line_rows, pieces = split_of(own)
    extra_rows = pieces[-1][1]
    pieces = len(pieces)
    f32, bf16 = jnp.float32, jnp.bfloat16
    vmem = pl.BlockSpec(memory_space=pltpu.VMEM)
    hbm = pl.BlockSpec(memory_space=pl.ANY)
    dma = pltpu.SemaphoreType.DMA
    summed, sq, kept, w, mo, se = pl.pallas_call(
        functools.partial(exchange_kernel, n, reps, hot),
        out_shape=(
            pltpu.VMEM((own, packed), f32),
            pltpu.VMEM((blocks, LANES), f32),
            pltpu.VMEM(cold_sums.shape[1:], bf16),
            pltpu.VMEM(weight.shape, f32),
            pltpu.VMEM(weight.shape, f32),
            pltpu.VMEM(weight.shape, f32),
        ),
        in_specs=[pl.BlockSpec(memory_space=pltpu.HBM)] * 7,
        out_specs=(vmem,) * 6,
        scratch_shapes=[
            pltpu.SMEM(ranks.shape, ranks.dtype),
            pltpu.VMEM((chunks, tokens, chunk), bf16),
            pltpu.VMEM((tokens, width), bf16),
            pltpu.VMEM((chunks, chunk, width), bf16),
            pltpu.VMEM((n, cross_rows, packed), f32),
            pltpu.VMEM((m, 2 * line_rows, packed), f32),
            pltpu.VMEM((m, cross_rows, packed), f32),
            pltpu.VMEM((line_rows, packed), f32),
            pltpu.VMEM((extra_rows, packed), f32),
            pltpu.VMEM((m + 1, cross_rows, packed), f32),
            pltpu.VMEM((m + 1, 2 * line_rows, packed), f32),
            pltpu.VMEM((2, extra_rows, packed), f32),
            pltpu.VMEM((blocks, 8, LANES), f32),
            pltpu.VMEM((reps, blocks, LANES), f32),
            pltpu.VMEM((2, blocks, LANES), f32),
            pltpu.VMEM((m, blocks, LANES), f32),
            dma,
            dma,
            dma((m, pieces)),
            dma,
            dma,
            dma((2,)),
            dma,
            dma,
            dma,
            dma((m + 1, pieces)),
            dma,
            dma((m + 1, 2)),
            dma,
            dma,
            dma,
            dma,
            dma,
            dma,
            dma,
            dma,
            pltpu.SemaphoreType.REGULAR,
            pltpu.SemaphoreType.REGULAR,
        ],
        compiler_params=pltpu.CompilerParams(
            collective_id=0, has_side_effects=True, vmem_limit_bytes=VMEM_GRANT
        ),
        name="exchange",
    )(ranks, features, out_grads, cold_sums, weight, moment, second)
    new_weight, new_moment, new_second, new_cold, column_sq = pl.pallas_call(
        functools.partial(update_kernel, n, rows * reps, tokens, hot),
        out_shape=(
            jax.ShapeDtypeStruct(weight.shape, f32),
            jax.ShapeDtypeStruct(weight.shape, f32),
            jax.ShapeDtypeStruct(weight.shape, f32),
            jax.ShapeDtypeStruct(cold_sums.shape, bf16),
            jax.ShapeDtypeStruct((blocks, LANES), f32),
        ),
        in_specs=[hbm] + [vmem] * 6,
        out_specs=(hbm,) * 5,
        scratch_shapes=[
            pltpu.SMEM(ranks.shape, ranks.dtype),
            pltpu.VMEM((3, weight.shape[0], packed), f32),
            dma,
            dma((3, blocks)),
            dma,
            dma,
        ],
        compiler_params=pltpu.CompilerParams(vmem_limit_bytes=VMEM_GRANT // 2),
        name="update",
    )(ranks, summed, sq, kept, w, mo, se)
    return new_weight, new_moment, new_second, new_cold, column_sq.reshape(width)


def solution(mesh):
    owned = P(("rep", "dp"), None)
    placed = (P("dp", "rep"), P("dp", None), P("dp", "rep", None), owned, owned, owned, P())
    return jax.shard_map(
        functools.partial(body, mesh.shape["dp"], mesh.shape["rep"]),
        mesh=mesh,
        in_specs=placed,
        out_specs=(owned, owned, owned, P("dp", "rep", None), P()),
        check_vma=False,
    )
```

```python
import functools
import jax
import jax.numpy as jnp
from jax import lax
from jax.experimental import pallas as pl
from jax.experimental.pallas import tpu as pltpu
from jax.sharding import PartitionSpec as P

LANES = 128
GROUP = 32
EXTRA = 86
LAG = 2
FRONT = 6
VMEM_GRANT = 55 * 2**20
MESH = pl.DeviceIdType.MESH


def split_of(own):
    line = 8 * max(round(own / 48), 1)
    cross = own - line
    extra = 8 * max(round(own / EXTRA), 1)
    head = 8 * ((cross - extra + 8) // 16)
    return cross, line, ((0, head), (head, cross - extra - head), (cross - extra, extra))


def block_of(ranks, blocks, rank):
    found = 0
    for b in range(blocks):
        gap = ranks[b] - rank
        found = found + b * (1 - jnp.minimum(gap * gap, 1))
    return found


def exchange_kernel(n, reps, hot, *refs):
    rows = refs[1].shape[1]
    own = rows // n
    chunks = rows // max(own, LANES)
    m = n // 2
    pieces = len(split_of(own)[2])
    dma = pltpu.SemaphoreType.DMA
    regular = pltpu.SemaphoreType.REGULAR
    pl.run_scoped(
        functools.partial(exchange_body, n, reps, hot, *refs),
        dma,
        dma,
        dma((m, pieces)),
        dma,
        dma,
        dma((2,)),
        dma,
        dma,
        dma,
        dma((m + 1, pieces)),
        dma,
        dma((m + 1, 2)),
        dma,
        dma,
        dma,
        dma,
        dma,
        dma,
        dma,
        dma,
        regular,
        regular,
        dma((2, chunks)),
        dma((5,)),
    )


def exchange_body(
    n, reps, hot,
    ranks_hbm, feat, og, cold, weight, moment, second,
    summed, sq_out, kept, w_out, m_out, s_out,
    ranks, feat_v, og_v, cold_v, pack_a, pack_b, rx_a, rx_b, rx_e, zin_a, zin_b, zin_e, sq, reps_sq, pair_sq, line_sq,
    x_send, xe_send, x_recv, zx_send, ze_send, ze_recv, be_send, be_recv, za_send, za_recv, zb_send, zb_recv, b_send, b_recv,
    nr_send, nr_recv, nx_send, nx_recv, nz_send, nz_recv, from_left, from_right,
    in_sem, state_sem,
):
    m = n // 2
    tokens = feat.shape[0]
    rows, width = cold.shape[1], cold.shape[2]
    blocks = width // LANES
    packed = hot * LANES
    own = rows // n
    chunk = max(own, LANES)
    chunks = rows // chunk
    inner = chunk // own
    cross_rows, line_rows, pieces = split_of(own)
    subs_all = range(len(pieces))
    kept_rows, extra_rows = pieces[-1]
    extra = slice(kept_rows, cross_rows)
    me = lax.axis_index("dp")
    rep = lax.axis_index("rep")
    x = me % 2
    p = me // 2
    partner = me + 1 - 2 * x

    half = max(m // 2, 1)
    flip = p // half if m > 1 else 0
    pr = p + flip * (m - 1 - 2 * p)
    lone = m - 1 - 2 * pr

    def dest(k):
        late = (k - lone + 2 * m) // (2 * m)
        pair = late * (k - lone)
        odd = pair % 2
        near = (1 - late) * (m - 1 - k) + late * ((1 - odd) * (pair // 2) + odd * (2 * pr - pair // 2))
        return near + flip * (m - 1 - 2 * near)

    def chunk_at(i):
        if chunk != own:
            return i
        side = i % 2
        return 2 * dest(i // 2) + (1 - side) * (1 - x) + side * x

    def span(lo, hi, step):
        if hi - lo <= 8:
            for k in range(lo, hi):
                step(k)
        else:
            lax.fori_loop(lo, hi, lambda k, carry: step(k) or carry, 0)

    def rolled(lo, hi, step):
        lax.fori_loop(lo, hi, lambda k, carry: step(k) or carry, 0)

    barrier = pltpu.get_barrier_semaphore()

    def feat_copy(i):
        cols = pl.ds(pl.multiple_of(chunk_at(i) * chunk, LANES), chunk)
        return pltpu.make_async_copy(feat.at[:, cols], feat_v.at[i], in_sem.at[0, i])

    def cold_copy(i):
        at = pl.ds(pl.multiple_of(chunk_at(i) * chunk, LANES), chunk)
        return pltpu.make_async_copy(cold.at[0, at], cold_v.at[i], in_sem.at[1, i])

    state = [
        pltpu.make_async_copy(src, dst, state_sem.at[i])
        for i, (src, dst) in enumerate(
            ((weight, w_out), (moment, m_out), (second, s_out), (og, og_v), (ranks_hbm, ranks))
        )
    ]
    def fetch(i):
        feat_copy(i).start()
        cold_copy(i).start()

    state[3].start()
    state[4].start()
    fetch(0)
    pl.semaphore_signal(barrier, inc=1, device_id={"dp": partner}, device_id_type=MESH)

    @pl.when(p > 0)
    def _():
        pl.semaphore_signal(barrier, inc=1, device_id={"dp": me - 2}, device_id_type=MESH)

    @pl.when(p < m - 1)
    def _():
        pl.semaphore_signal(barrier, inc=1, device_id={"dp": me + 2}, device_id_type=MESH)

    span(1, reps, lambda t: pl.semaphore_signal(
        barrier, inc=1, device_id={"rep": (rep + t) % reps}, device_id_type=MESH))
    rolled(1, chunks, fetch)

    sq[...] = jnp.zeros_like(sq)

    def cross(k, sub):
        d = dest(k)
        at = pl.ds(*pieces[sub])
        return pltpu.make_async_remote_copy(
            src_ref=pack_a.at[2 * d + 1 - x, at], dst_ref=rx_a.at[d, at],
            send_sem=xe_send if sub == subs_all[-1] else x_send, recv_sem=x_recv.at[d, sub],
            device_id={"dp": partner}, device_id_type=MESH,
        )

    def start_cross(k, sub):
        if sub == subs_all[-1]:
            @pl.when(dest(k) != m - 1)
            def _():
                cross(k, sub).start()
        else:
            cross(k, sub).start()

    def along_a(d, sub, right):
        at = pl.ds(*pieces[sub])
        slot = d + 1 if right else d
        return pltpu.make_async_remote_copy(
            src_ref=pack_a.at[2 * d + x, at], dst_ref=zin_a.at[slot, at],
            send_sem=zx_send if sub == subs_all[-1] else za_send, recv_sem=za_recv.at[slot, sub],
            device_id={"dp": me + 2 if right else me - 2}, device_id_type=MESH,
        )

    def along_e(s):
        return pltpu.make_async_remote_copy(
            src_ref=pack_a.at[2 * (m - 1) + s, pl.ds(kept_rows, extra_rows)], dst_ref=zin_e.at[s],
            send_sem=ze_send, recv_sem=ze_recv.at[s],
            device_id={"dp": me + 2}, device_id_type=MESH,
        )

    def cross_e():
        return pltpu.make_async_remote_copy(
            src_ref=pack_a.at[2 * (m - 1) + 1 - x, pl.ds(kept_rows, extra_rows)], dst_ref=rx_e,
            send_sem=be_send, recv_sem=be_recv,
            device_id={"dp": partner}, device_id_type=MESH,
        )

    def along_b(d, s, right):
        slot = d + 1 if right else d
        at = pl.ds(pl.multiple_of(s * line_rows, 8), line_rows)
        return pltpu.make_async_remote_copy(
            src_ref=pack_b.at[d, at], dst_ref=zin_b.at[slot, at],
            send_sem=zb_send, recv_sem=zb_recv.at[slot, s],
            device_id={"dp": me + 2 if right else me - 2}, device_id_type=MESH,
        )

    def cross_b():
        return pltpu.make_async_remote_copy(
            src_ref=pack_b.at[p, pl.ds(pl.multiple_of((1 - x) * line_rows, 8), line_rows)],
            dst_ref=rx_b, send_sem=b_send, recv_sem=b_recv,
            device_id={"dp": partner}, device_id_type=MESH,
        )

    def norm_rep(t):
        return pltpu.make_async_remote_copy(
            src_ref=reps_sq.at[rep], dst_ref=reps_sq.at[rep], send_sem=nr_send, recv_sem=nr_recv,
            device_id={"rep": (rep + t) % reps}, device_id_type=MESH,
        )

    def norm_x():
        return pltpu.make_async_remote_copy(
            src_ref=pair_sq.at[x], dst_ref=pair_sq.at[x], send_sem=nx_send, recv_sem=nx_recv,
            device_id={"dp": partner}, device_id_type=MESH,
        )

    def norm_z(t):
        return pltpu.make_async_remote_copy(
            src_ref=line_sq.at[p], dst_ref=line_sq.at[p], send_sem=nz_send, recv_sem=nz_recv,
            device_id={"dp": 2 * ((p + t) % m) + x}, device_id_type=MESH,
        )

    def bytes_of(ref, send_sem, recv_sem):
        return pltpu.make_async_remote_copy(
            src_ref=ref, dst_ref=ref, send_sem=send_sem, recv_sem=recv_sem,
            device_id={"dp": partner}, device_id_type=MESH,
        )

    def token(right):
        pl.semaphore_signal(
            from_left if right else from_right, inc=1,
            device_id={"dp": me + 2 if right else me - 2}, device_id_type=MESH,
        )

    def raw_b(d, s):
        @pl.when(jnp.logical_and(d > p, p == 0))
        def _():
            along_b(d, s, True).start()

        @pl.when((d == m - 1) & (d > p) & (p == 0))
        def _():
            along_e(s).start()

        @pl.when(jnp.logical_and(d < p, p == m - 1))
        def _():
            along_b(d, s, False).start()

    def cross_step(k, subs=subs_all):
        d = dest(k)
        for sub in subs:
            if sub == subs_all[-1]:
                @pl.when(d != m - 1)
                def _():
                    cross_piece(k, d, sub)
            else:
                cross_piece(k, d, sub)

    def cross_piece(k, d, sub):
        at = slice(pieces[sub][0], sum(pieces[sub]))
        cross(k, sub).wait_recv()
        pack_a[2 * d + x, at] += rx_a[d, at]

        @pl.when(jnp.logical_and(d >= p, p > 0))
        def _():
            along_a(d, sub, True).wait_recv()
            pack_a[2 * d + x, at] += zin_a[d + 1, at]

        @pl.when(jnp.logical_and(d <= p, p < m - 1))
        def _():
            along_a(d, sub, False).wait_recv()
            pack_a[2 * d + x, at] += zin_a[d, at]

        @pl.when(d > p)
        def _():
            along_a(d, sub, True).start()

        @pl.when(d < p)
        def _():
            along_a(d, sub, False).start()

        @pl.when(d == p)
        def _():
            summed[at] = pack_a[2 * d + x, at]

    def fill(i, first=0, last=chunk):
        c = chunk_at(i)
        grad = lax.dot_general(
            feat_v[i, :, first:last], og_v[...], (((0,), (0,)), ((), ())),
            preferred_element_type=jnp.float32,
        )
        squares = [sq[b] for b in range(blocks)]
        for g in range(first, last, GROUP):
            values = []
            for b in range(blocks):
                cols = slice(b * LANES, (b + 1) * LANES)
                value = grad[g - first:g - first + GROUP, cols]
                value += cold_v[i, g:g + GROUP, cols].astype(jnp.float32)
                for h in range(0, GROUP, 8):
                    squares[b] += value[h:h + 8] * value[h:h + 8]
                values.append(value)
            at = pl.ds(pl.multiple_of(c * chunk + g, 16), GROUP)
            for b in range(blocks):
                kept[at, b * LANES:(b + 1) * LANES] = jnp.where(
                    ranks[b] < hot, jnp.zeros_like(values[b]), values[b]).astype(jnp.bfloat16)
            for r in range(hot):
                cols = slice(r * LANES, (r + 1) * LANES)
                held = values[0]
                for b in range(1, blocks):
                    held = jnp.where(ranks[b] == r, values[b], held)
                for h in range(0, GROUP, 8):
                    owner = c * inner + (g + h) // own
                    row = (g + h) % own
                    if row < cross_rows:
                        pack_a[owner, row:row + 8, cols] = held[h:h + 8]
                    else:
                        to = pl.ds(pl.multiple_of((owner % 2) * line_rows + row - cross_rows, 8), 8)
                        pack_b[owner // 2, to, cols] = held[h:h + 8]
        for b in range(blocks):
            sq[b] = squares[b]

    def step(i):
        feat_copy(i).wait()
        cold_copy(i).wait()
        fill(i)
        if chunk == own:
            send_cross(i)
            raw_b(dest(i // 2), chunk_at(i) % 2)

    def send_cross(i):
        k = (i - lag) // 2
        for sub in subs_all:
            @pl.when((i >= lag) & ((i - lag) % 2 == 0) & (k * len(pieces) + sub < FRONT))
            def _():
                start_cross(k, sub)

    state[4].wait()
    state[3].wait()
    feat_copy(0).wait()
    cold_copy(0).wait()
    early = LANES if chunk == own else chunk
    fill(0, 0, early)
    greeted = (p + m - 1) // m + (2 * m - 2 - p) // m + 1 + (reps - 1)
    pl.semaphore_wait(barrier, greeted)

    @pl.when(jnp.logical_and(p == 0, m > 1))
    def _():
        token(True)

    @pl.when(jnp.logical_and(p == m - 1, m > 1))
    def _():
        token(False)

    lag = rep % 2 * LAG
    if chunk == own:
        ready = [sub for sub in subs_all if sum(pieces[sub]) <= early]
        rest_of = [sub for sub in subs_all if sum(pieces[sub]) > early]

        def start_early(subs):
            @pl.when(lag == 0)
            def _():
                for sub in subs:
                    start_cross(0, sub)

        start_early(ready)
        if early < chunk:
            fill(0, early, chunk)
        start_early(rest_of)
        raw_b(dest(0), 1 - x)
    rolled(1, chunks, step)
    for copy in state[:3]:
        copy.start()
    if chunk != own:
        def launch(k):
            for sub in subs_all:
                @pl.when(k * len(pieces) + sub < FRONT)
                def _():
                    start_cross(k, sub)
            for s in range(2):
                raw_b(dest(k), s)

        rolled(0, m, launch)
    for r in range(blocks):
        reps_sq[rep, r:r + 1] = jnp.sum(sq[r], axis=0, keepdims=True)
    span(1, reps, lambda t: norm_rep(t).start())

    def line_step(k):
        d = dest(k)
        for s in range(2):
            at = slice(s * line_rows, (s + 1) * line_rows)

            @pl.when(jnp.logical_and(d >= p, p > 0))
            def _():
                along_b(d, s, True).wait_recv()
                pack_b[d, at] += zin_b[d + 1, at]

            @pl.when(jnp.logical_and(d <= p, p < m - 1))
            def _():
                along_b(d, s, False).wait_recv()
                pack_b[d, at] += zin_b[d, at]

            @pl.when(jnp.logical_and(d > p, p > 0))
            def _():
                along_b(d, s, True).start()

            @pl.when(jnp.logical_and(d < p, p < m - 1))
            def _():
                along_b(d, s, False).start()

            @pl.when((d == m - 1) & (p > 0))
            def _():
                along_e(s).wait_recv()
                pack_a[2 * d + s, extra] += zin_e[s]

            @pl.when((d == m - 1) & (p > 0) & (p < m - 1))
            def _():
                along_e(s).start()

    def rest(k):
        for sub in subs_all:
            @pl.when(k * len(pieces) + sub >= FRONT)
            def _():
                start_cross(k, sub)

    span(0, m - 1, line_step)

    @pl.when(jnp.logical_and(p > 0, p < m - 1))
    def _():
        pl.semaphore_wait(from_right, 1)
        token(False)
        pl.semaphore_wait(from_left, 1)
        token(True)

    if m > 1:
        cross_step(0, range(1))
    bytes_of(reps_sq.at[pl.ds(0, reps - 1)], nr_send, nr_recv).wait_recv()
    total = reps_sq[0]
    for j in range(1, reps):
        total = total + reps_sq[j]
    pair_sq[x] = total
    norm_x().start()
    rolled(0, m, rest)
    if m > 1:
        cross_step(0, subs_all[1:])
    if m > 2:
        cross_step(1)
    norm_x().wait_recv()
    line_sq[p] = pair_sq[0] + pair_sq[1]

    @pl.when(jnp.logical_and(p == 0, m > 1))
    def _():
        pl.semaphore_wait(from_right, 1)

    @pl.when(jnp.logical_and(p == m - 1, m > 1))
    def _():
        pl.semaphore_wait(from_left, 1)

    span(1, m, lambda t: norm_z(t).start())
    span(2, m - 2, cross_step)
    line_step(m - 1)
    cross_b().start()

    @pl.when(p == m - 1)
    def _():
        cross_e().start()

    if m > 3:
        cross_step(m - 2)
    if m > 1:
        bytes_of(line_sq.at[pl.ds(0, m - 1)], nz_send, nz_recv).wait_recv()
    everything = line_sq[0]
    for j in range(1, m):
        everything = everything + line_sq[j]
    sq_out[...] = everything
    for copy in state[:3]:
        copy.wait()
    cross_step(m - 1)
    cross_b().wait_recv()
    mine = pl.ds(pl.multiple_of(x * line_rows, 8), line_rows)
    summed[cross_rows:] = pack_b[p, mine] + rx_b[...]

    @pl.when(p == m - 1)
    def _():
        cross_e().wait_recv()
        summed[extra] = pack_a[2 * p + x, extra] + rx_e[...]
        cross_e().wait_send()


    main, tail = pl.ds(0, kept_rows), pl.ds(kept_rows, extra_rows)
    bytes_of(rx_a.at[:, main], x_send, x_recv.at[0, 0]).wait_send()
    if m > 1:
        bytes_of(rx_a.at[pl.ds(0, m - 1), tail], xe_send, x_recv.at[0, 0]).wait_send()
        bytes_of(zin_a.at[pl.ds(0, m - 1), main], za_send, za_recv.at[0, 0]).wait_send()
        bytes_of(zin_b.at[pl.ds(0, m - 1)], zb_send, zb_recv.at[0, 0]).wait_send()
        bytes_of(line_sq.at[pl.ds(0, m - 1)], nz_send, nz_recv).wait_send()

        @pl.when(p == m - 1)
        def _():
            bytes_of(zin_a.at[pl.ds(0, m - 1), tail], zx_send, za_recv.at[0, 0]).wait_send()

        @pl.when(p < m - 1)
        def _():
            if m > 2:
                bytes_of(zin_a.at[pl.ds(0, m - 2), tail], zx_send, za_recv.at[0, 0]).wait_send()
            bytes_of(zin_e, ze_send, ze_recv.at[0]).wait_send()

    cross_b().wait_send()
    norm_x().wait_send()
    bytes_of(reps_sq.at[pl.ds(0, reps - 1)], nr_send, nr_recv).wait_send()


def update_kernel(n, total_rows, tokens, hot, *refs):
    blocks = refs[4].shape[1] // LANES
    dma = pltpu.SemaphoreType.DMA
    pl.run_scoped(
        functools.partial(update_body, n, total_rows, tokens, hot, *refs),
        dma, dma((3, blocks)), dma, dma,
    )


def update_body(
    n, total_rows, tokens, hot,
    ranks_any, summed, sq, kept, weight, moment, second,
    w_hbm, m_hbm, s_hbm, nc_hbm, sq_hbm,
    ranks, fresh, nc_sem, state_sem, sq_sem, ranks_sem,
):
    width = weight.shape[1]
    blocks = width // LANES
    outs = (w_hbm, m_hbm, s_hbm)
    copies = []

    def send(src, dst, sem):
        copies.append(pltpu.make_async_copy(src, dst, sem))
        copies[-1].start()

    order = pltpu.make_async_copy(ranks_any, ranks, ranks_sem)
    order.start()
    send(kept, nc_hbm.at[0], nc_sem)
    send(sq, sq_hbm, sq_sem)
    order.wait()
    block = [block_of(ranks, blocks, r) for r in range(blocks)]
    where = [pl.ds(pl.multiple_of(b * LANES, LANES), LANES) for b in block]
    for r in range(hot, blocks):
        for i, src in enumerate((weight, moment, second)):
            send(src.at[:, where[r]], outs[i].at[:, where[r]], state_sem.at[i, r])
    for r in range(hot):
        cols = slice(r * LANES, (r + 1) * LANES)
        rms = jnp.sqrt(sq[pl.ds(block[r], 1), :] / jnp.float32(total_rows * n * tokens))
        clip = 1.0 / jnp.maximum(jnp.float32(1.0), rms)
        grad = summed[:, cols] * clip / jnp.float32(n)
        moved = 0.9 * moment[:, where[r]] + 0.1 * grad
        squared = 0.95 * second[:, where[r]] + 0.05 * grad * grad
        fresh[1, :, cols] = moved
        fresh[2, :, cols] = squared
        step = 0.05 * (moved / (1.0 - 0.9**10)) / (
            jnp.sqrt(squared / (1.0 - 0.95**10)) + 1e-08
        )
        fresh[0, :, cols] = weight[:, where[r]] - step
        for i in range(3):
            send(fresh.at[i, :, pl.ds(r * LANES, LANES)], outs[i].at[:, where[r]], state_sem.at[i, r])
    for copy in copies:
        copy.wait()


def body(n, reps, features, out_grads, cold_sums, weight, moment, second, ranks):
    tokens, rows = features.shape
    width = out_grads.shape[1]
    blocks = ranks.shape[0]
    hot = blocks // 2
    packed = hot * LANES
    m = n // 2
    own = rows // n
    chunk = max(own, LANES)
    chunks = rows // chunk
    cross_rows, line_rows, pieces = split_of(own)
    extra_rows = pieces[-1][1]
    f32, bf16 = jnp.float32, jnp.bfloat16
    vmem = pl.BlockSpec(memory_space=pltpu.VMEM)
    hbm = pl.BlockSpec(memory_space=pl.ANY)
    summed, sq, kept, w, mo, se = pl.pallas_call(
        functools.partial(exchange_kernel, n, reps, hot),
        out_shape=(
            pltpu.VMEM((own, packed), f32),
            pltpu.VMEM((blocks, LANES), f32),
            pltpu.VMEM(cold_sums.shape[1:], bf16),
            pltpu.VMEM(weight.shape, f32),
            pltpu.VMEM(weight.shape, f32),
            pltpu.VMEM(weight.shape, f32),
        ),
        in_specs=[pl.BlockSpec(memory_space=pltpu.HBM)] * 7,
        out_specs=(vmem,) * 6,
        scratch_shapes=[
            pltpu.SMEM(ranks.shape, ranks.dtype),
            pltpu.VMEM((chunks, tokens, chunk), bf16),
            pltpu.VMEM((tokens, width), bf16),
            pltpu.VMEM((chunks, chunk, width), bf16),
            pltpu.VMEM((n, cross_rows, packed), f32),
            pltpu.VMEM((m, 2 * line_rows, packed), f32),
            pltpu.VMEM((m, cross_rows, packed), f32),
            pltpu.VMEM((line_rows, packed), f32),
            pltpu.VMEM((extra_rows, packed), f32),
            pltpu.VMEM((m + 1, cross_rows, packed), f32),
            pltpu.VMEM((m + 1, 2 * line_rows, packed), f32),
            pltpu.VMEM((2, extra_rows, packed), f32),
            pltpu.VMEM((blocks, 8, LANES), f32),
            pltpu.VMEM((reps, blocks, LANES), f32),
            pltpu.VMEM((2, blocks, LANES), f32),
            pltpu.VMEM((m, blocks, LANES), f32),
        ],
        compiler_params=pltpu.CompilerParams(
            collective_id=0, has_side_effects=True, vmem_limit_bytes=VMEM_GRANT
        ),
        name="exchange",
    )(ranks, features, out_grads, cold_sums, weight, moment, second)
    new_weight, new_moment, new_second, new_cold, column_sq = pl.pallas_call(
        functools.partial(update_kernel, n, rows * reps, tokens, hot),
        out_shape=(
            jax.ShapeDtypeStruct(weight.shape, f32),
            jax.ShapeDtypeStruct(weight.shape, f32),
            jax.ShapeDtypeStruct(weight.shape, f32),
            jax.ShapeDtypeStruct(cold_sums.shape, bf16),
            jax.ShapeDtypeStruct((blocks, LANES), f32),
        ),
        in_specs=[hbm] + [vmem] * 6,
        out_specs=(hbm,) * 5,
        scratch_shapes=[
            pltpu.SMEM(ranks.shape, ranks.dtype),
            pltpu.VMEM((3, weight.shape[0], packed), f32),
        ],
        compiler_params=pltpu.CompilerParams(vmem_limit_bytes=VMEM_GRANT // 2),
        name="update",
    )(ranks, summed, sq, kept, w, mo, se)
    return new_weight, new_moment, new_second, new_cold, column_sq.reshape(width)


def solution(mesh):
    owned = P(("rep", "dp"), None)
    placed = (P("dp", "rep"), P("dp", None), P("dp", "rep", None), owned, owned, owned, P())
    return jax.shard_map(
        functools.partial(body, mesh.shape["dp"], mesh.shape["rep"]),
        mesh=mesh,
        in_specs=placed,
        out_specs=(owned, owned, owned, P("dp", "rep", None), P()),
        check_vma=False,
    )
```

```python
import functools
import jax
import jax.numpy as jnp
from jax import lax
from jax.experimental import pallas as pl
from jax.experimental.pallas import tpu as pltpu
from jax.sharding import PartitionSpec as P

LANES = 128
GROUP = 32
EXTRA = 86
LAG = 1
FRONT = 6
VMEM_GRANT = 55 * 2**20
MESH = pl.DeviceIdType.MESH


def split_of(own):
    line = 8 * max(round(own / 48), 1)
    cross = own - line
    extra = 8 * max(round(own / EXTRA), 1)
    head = 8 * ((cross - extra + 8) // 16)
    return cross, line, ((0, head), (head, cross - extra - head), (cross - extra, extra))


def block_of(ranks, blocks, rank):
    found = 0
    for b in range(blocks):
        gap = ranks[b] - rank
        found = found + b * (1 - jnp.minimum(gap * gap, 1))
    return found


def exchange_kernel(n, reps, hot, *refs):
    rows = refs[1].shape[1]
    own = rows // n
    chunks = rows // max(own, LANES)
    m = n // 2
    pieces = len(split_of(own)[2])
    dma = pltpu.SemaphoreType.DMA
    regular = pltpu.SemaphoreType.REGULAR
    pl.run_scoped(
        functools.partial(exchange_body, n, reps, hot, *refs),
        dma,
        dma,
        dma((m, pieces)),
        dma,
        dma,
        dma((2,)),
        dma,
        dma,
        dma,
        dma((m + 1, pieces)),
        dma,
        dma((m + 1, 2)),
        dma,
        dma,
        dma,
        dma,
        dma,
        dma,
        dma,
        dma,
        regular,
        regular,
        dma((2, chunks)),
        dma((5,)),
        dma((2, 2)),
    )


def exchange_body(
    n, reps, hot,
    ranks_hbm, feat, og, cold, weight, moment, second,
    summed, sq_out, kept, w_out, m_out, s_out,
    ranks, feat_v, og_v, cold_v, pack_a, pack_b, rx_a, rx_b, rx_e, zin_a, zin_b, zin_e, sq, reps_sq, pair_sq, line_sq,
    x_send, xe_send, x_recv, zx_send, ze_send, ze_recv, be_send, be_recv, za_send, za_recv, zb_send, zb_recv, b_send, b_recv,
    nr_send, nr_recv, nx_send, nx_recv, nz_send, nz_recv, from_left, from_right,
    in_sem, state_sem, first_sem,
):
    m = n // 2
    tokens = feat.shape[0]
    rows, width = cold.shape[1], cold.shape[2]
    blocks = width // LANES
    packed = hot * LANES
    own = rows // n
    chunk = max(own, LANES)
    chunks = rows // chunk
    inner = chunk // own
    cross_rows, line_rows, pieces = split_of(own)
    subs_all = range(len(pieces))
    kept_rows, extra_rows = pieces[-1]
    extra = slice(kept_rows, cross_rows)
    me = lax.axis_index("dp")
    rep = lax.axis_index("rep")
    x = me % 2
    p = me // 2
    partner = me + 1 - 2 * x

    half = max(m // 2, 1)
    flip = p // half if m > 1 else 0
    pr = p + flip * (m - 1 - 2 * p)
    lone = m - 1 - 2 * pr

    def dest(k):
        late = (k - lone + 2 * m) // (2 * m)
        pair = late * (k - lone)
        odd = pair % 2
        near = (1 - late) * (m - 1 - k) + late * ((1 - odd) * (pair // 2) + odd * (2 * pr - pair // 2))
        return near + flip * (m - 1 - 2 * near)

    def chunk_at(i):
        if chunk != own:
            return i
        side = i % 2
        return 2 * dest(i // 2) + (1 - side) * (1 - x) + side * x

    def span(lo, hi, step):
        if hi - lo <= 8:
            for k in range(lo, hi):
                step(k)
        else:
            lax.fori_loop(lo, hi, lambda k, carry: step(k) or carry, 0)

    def rolled(lo, hi, step):
        lax.fori_loop(lo, hi, lambda k, carry: step(k) or carry, 0)

    barrier = pltpu.get_barrier_semaphore()

    def feat_copy(i):
        cols = pl.ds(pl.multiple_of(chunk_at(i) * chunk, LANES), chunk)
        return pltpu.make_async_copy(feat.at[:, cols], feat_v.at[i], in_sem.at[0, i])

    def cold_copy(i):
        at = pl.ds(pl.multiple_of(chunk_at(i) * chunk, LANES), chunk)
        return pltpu.make_async_copy(cold.at[0, at], cold_v.at[i], in_sem.at[1, i])

    state = [
        pltpu.make_async_copy(src, dst, state_sem.at[i])
        for i, (src, dst) in enumerate(
            ((weight, w_out), (moment, m_out), (second, s_out), (og, og_v), (ranks_hbm, ranks))
        )
    ]
    def fetch(i):
        feat_copy(i).start()
        cold_copy(i).start()

    early = LANES if chunk == own else chunk
    start = chunk_at(0) * chunk

    def first_feat(lo, hi):
        cols = pl.ds(pl.multiple_of(start + lo, LANES), hi - lo)
        return pltpu.make_async_copy(
            feat.at[:, cols], feat_v.at[0, :, pl.ds(lo, hi - lo)], first_sem.at[0, lo // early])

    def first_cold(lo, hi):
        at = pl.ds(pl.multiple_of(start + lo, LANES), hi - lo)
        return pltpu.make_async_copy(
            cold.at[0, at], cold_v.at[0, pl.ds(lo, hi - lo)], first_sem.at[1, lo // early])

    first_feat(0, early).start()
    state[3].start()
    first_cold(0, early).start()
    state[4].start()
    if early < chunk:
        first_feat(early, chunk).start()
        first_cold(early, chunk).start()
    pl.semaphore_signal(barrier, inc=1, device_id={"dp": partner}, device_id_type=MESH)

    @pl.when(p > 0)
    def _():
        pl.semaphore_signal(barrier, inc=1, device_id={"dp": me - 2}, device_id_type=MESH)

    @pl.when(p < m - 1)
    def _():
        pl.semaphore_signal(barrier, inc=1, device_id={"dp": me + 2}, device_id_type=MESH)

    span(1, reps, lambda t: pl.semaphore_signal(
        barrier, inc=1, device_id={"rep": (rep + t) % reps}, device_id_type=MESH))
    rolled(1, chunks, fetch)

    sq[...] = jnp.zeros_like(sq)

    def cross(k, sub):
        d = dest(k)
        at = pl.ds(*pieces[sub])
        return pltpu.make_async_remote_copy(
            src_ref=pack_a.at[2 * d + 1 - x, at], dst_ref=rx_a.at[d, at],
            send_sem=xe_send if sub == subs_all[-1] else x_send, recv_sem=x_recv.at[d, sub],
            device_id={"dp": partner}, device_id_type=MESH,
        )

    def start_cross(k, sub):
        if sub == subs_all[-1]:
            @pl.when(dest(k) != m - 1)
            def _():
                cross(k, sub).start()
        else:
            cross(k, sub).start()

    def along_a(d, sub, right):
        at = pl.ds(*pieces[sub])
        slot = d + 1 if right else d
        return pltpu.make_async_remote_copy(
            src_ref=pack_a.at[2 * d + x, at], dst_ref=zin_a.at[slot, at],
            send_sem=zx_send if sub == subs_all[-1] else za_send, recv_sem=za_recv.at[slot, sub],
            device_id={"dp": me + 2 if right else me - 2}, device_id_type=MESH,
        )

    def along_e(s):
        return pltpu.make_async_remote_copy(
            src_ref=pack_a.at[2 * (m - 1) + s, pl.ds(kept_rows, extra_rows)], dst_ref=zin_e.at[s],
            send_sem=ze_send, recv_sem=ze_recv.at[s],
            device_id={"dp": me + 2}, device_id_type=MESH,
        )

    def cross_e():
        return pltpu.make_async_remote_copy(
            src_ref=pack_a.at[2 * (m - 1) + 1 - x, pl.ds(kept_rows, extra_rows)], dst_ref=rx_e,
            send_sem=be_send, recv_sem=be_recv,
            device_id={"dp": partner}, device_id_type=MESH,
        )

    def along_b(d, s, right):
        slot = d + 1 if right else d
        at = pl.ds(pl.multiple_of(s * line_rows, 8), line_rows)
        return pltpu.make_async_remote_copy(
            src_ref=pack_b.at[d, at], dst_ref=zin_b.at[slot, at],
            send_sem=zb_send, recv_sem=zb_recv.at[slot, s],
            device_id={"dp": me + 2 if right else me - 2}, device_id_type=MESH,
        )

    def cross_b():
        return pltpu.make_async_remote_copy(
            src_ref=pack_b.at[p, pl.ds(pl.multiple_of((1 - x) * line_rows, 8), line_rows)],
            dst_ref=rx_b, send_sem=b_send, recv_sem=b_recv,
            device_id={"dp": partner}, device_id_type=MESH,
        )

    def norm_rep(t):
        return pltpu.make_async_remote_copy(
            src_ref=reps_sq.at[rep], dst_ref=reps_sq.at[rep], send_sem=nr_send, recv_sem=nr_recv,
            device_id={"rep": (rep + t) % reps}, device_id_type=MESH,
        )

    def norm_x():
        return pltpu.make_async_remote_copy(
            src_ref=pair_sq.at[x], dst_ref=pair_sq.at[x], send_sem=nx_send, recv_sem=nx_recv,
            device_id={"dp": partner}, device_id_type=MESH,
        )

    def norm_z(t):
        return pltpu.make_async_remote_copy(
            src_ref=line_sq.at[p], dst_ref=line_sq.at[p], send_sem=nz_send, recv_sem=nz_recv,
            device_id={"dp": 2 * ((p + t) % m) + x}, device_id_type=MESH,
        )

    def bytes_of(ref, send_sem, recv_sem):
        return pltpu.make_async_remote_copy(
            src_ref=ref, dst_ref=ref, send_sem=send_sem, recv_sem=recv_sem,
            device_id={"dp": partner}, device_id_type=MESH,
        )

    def token(right):
        pl.semaphore_signal(
            from_left if right else from_right, inc=1,
            device_id={"dp": me + 2 if right else me - 2}, device_id_type=MESH,
        )

    def raw_b(d, s):
        @pl.when(jnp.logical_and(d > p, p == 0))
        def _():
            along_b(d, s, True).start()

        @pl.when((d == m - 1) & (d > p) & (p == 0))
        def _():
            along_e(s).start()

        @pl.when(jnp.logical_and(d < p, p == m - 1))
        def _():
            along_b(d, s, False).start()

    def cross_step(k, subs=subs_all):
        d = dest(k)
        for sub in subs:
            if sub == subs_all[-1]:
                @pl.when(d != m - 1)
                def _():
                    cross_piece(k, d, sub)
            else:
                cross_piece(k, d, sub)

    def cross_piece(k, d, sub):
        at = slice(pieces[sub][0], sum(pieces[sub]))
        cross(k, sub).wait_recv()
        pack_a[2 * d + x, at] += rx_a[d, at]

        @pl.when(jnp.logical_and(d >= p, p > 0))
        def _():
            along_a(d, sub, True).wait_recv()
            pack_a[2 * d + x, at] += zin_a[d + 1, at]

        @pl.when(jnp.logical_and(d <= p, p < m - 1))
        def _():
            along_a(d, sub, False).wait_recv()
            pack_a[2 * d + x, at] += zin_a[d, at]

        @pl.when(d > p)
        def _():
            along_a(d, sub, True).start()

        @pl.when(d < p)
        def _():
            along_a(d, sub, False).start()

        @pl.when(d == p)
        def _():
            summed[at] = pack_a[2 * d + x, at]

    def product(i, first=0, last=chunk):
        return lax.dot_general(
            feat_v[i, :, first:last], og_v[...], (((0,), (0,)), ((), ())),
            preferred_element_type=jnp.float32,
        )

    def sums(i, grad, first, g):
        return [
            grad[g - first:g - first + GROUP, b * LANES:(b + 1) * LANES]
            + cold_v[i, g:g + GROUP, b * LANES:(b + 1) * LANES].astype(jnp.float32)
            for b in range(blocks)
        ]

    def fill_hot(i, values, g):
        c = chunk_at(i)
        for r in range(hot):
            cols = slice(r * LANES, (r + 1) * LANES)
            held = values[0]
            for b in range(1, blocks):
                held = jnp.where(ranks[b] == r, values[b], held)
            for h in range(0, GROUP, 8):
                owner = c * inner + (g + h) // own
                row = (g + h) % own
                if row < cross_rows:
                    pack_a[owner, row:row + 8, cols] = held[h:h + 8]
                else:
                    to = pl.ds(pl.multiple_of((owner % 2) * line_rows + row - cross_rows, 8), 8)
                    pack_b[owner // 2, to, cols] = held[h:h + 8]

    def fill_cold(i, values, g, squares):
        at = pl.ds(pl.multiple_of(chunk_at(i) * chunk + g, 16), GROUP)
        for b in range(blocks):
            for h in range(0, GROUP, 8):
                squares[b] += values[b][h:h + 8] * values[b][h:h + 8]
            kept[at, b * LANES:(b + 1) * LANES] = jnp.where(
                ranks[b] < hot, jnp.zeros_like(values[b]), values[b]).astype(jnp.bfloat16)

    def fill(i, grad, first=0, last=chunk, hot_rows=True, cold_rows=True):
        squares = [sq[b] for b in range(blocks)]
        for g in range(first, last, GROUP):
            values = sums(i, grad, first, g)
            if cold_rows:
                fill_cold(i, values, g, squares)
            if hot_rows:
                fill_hot(i, values, g)
        if cold_rows:
            for b in range(blocks):
                sq[b] = squares[b]

    def step(i):
        feat_copy(i).wait()
        cold_copy(i).wait()
        fill(i, product(i))
        if chunk == own:
            send_cross(i)
            raw_b(dest(i // 2), chunk_at(i) % 2)

    def send_cross(i):
        k = (i - lag) // 2
        for sub in subs_all:
            @pl.when((i >= lag) & ((i - lag) % 2 == 0) & (k * len(pieces) + sub < FRONT))
            def _():
                start_cross(k, sub)

    state[4].wait()
    state[3].wait()
    first_feat(0, early).wait()
    first_cold(0, early).wait()
    grad = product(0, 0, early)
    fill(0, grad, 0, early, cold_rows=False)
    greeted = (p + m - 1) // m + (2 * m - 2 - p) // m + 1 + (reps - 1)
    pl.semaphore_wait(barrier, greeted)

    @pl.when(jnp.logical_and(p == 0, m > 1))
    def _():
        token(True)

    @pl.when(jnp.logical_and(p == m - 1, m > 1))
    def _():
        token(False)

    lag = rep % 2 * LAG
    if chunk == own:
        ready = [sub for sub in subs_all if sum(pieces[sub]) <= early]
        rest_of = [sub for sub in subs_all if sum(pieces[sub]) > early]

        def start_early(subs):
            @pl.when(lag == 0)
            def _():
                for sub in subs:
                    start_cross(0, sub)

        start_early(ready)
    fill(0, grad, 0, early, hot_rows=False)
    if chunk == own:
        if early < chunk:
            first_feat(early, chunk).wait()
            first_cold(early, chunk).wait()
            fill(0, product(0, early, chunk), early, chunk)
        start_early(rest_of)
        raw_b(dest(0), 1 - x)
    rolled(1, chunks, step)
    for copy in state[:3]:
        copy.start()
    if chunk != own:
        def launch(k):
            for sub in subs_all:
                @pl.when(k * len(pieces) + sub < FRONT)
                def _():
                    start_cross(k, sub)
            for s in range(2):
                raw_b(dest(k), s)

        rolled(0, m, launch)
    for r in range(blocks):
        reps_sq[rep, r:r + 1] = jnp.sum(sq[r], axis=0, keepdims=True)
    span(1, reps, lambda t: norm_rep(t).start())

    def line_step(k):
        d = dest(k)
        for s in range(2):
            at = slice(s * line_rows, (s + 1) * line_rows)

            @pl.when(jnp.logical_and(d >= p, p > 0))
            def _():
                along_b(d, s, True).wait_recv()
                pack_b[d, at] += zin_b[d + 1, at]

            @pl.when(jnp.logical_and(d <= p, p < m - 1))
            def _():
                along_b(d, s, False).wait_recv()
                pack_b[d, at] += zin_b[d, at]

            @pl.when(jnp.logical_and(d > p, p > 0))
            def _():
                along_b(d, s, True).start()

            @pl.when(jnp.logical_and(d < p, p < m - 1))
            def _():
                along_b(d, s, False).start()

            @pl.when((d == m - 1) & (p > 0))
            def _():
                along_e(s).wait_recv()
                pack_a[2 * d + s, extra] += zin_e[s]

            @pl.when((d == m - 1) & (p > 0) & (p < m - 1))
            def _():
                along_e(s).start()

    def rest(k):
        for sub in subs_all:
            @pl.when(k * len(pieces) + sub >= FRONT)
            def _():
                start_cross(k, sub)

    span(0, m - 1, line_step)

    @pl.when(jnp.logical_and(p > 0, p < m - 1))
    def _():
        pl.semaphore_wait(from_right, 1)
        token(False)
        pl.semaphore_wait(from_left, 1)
        token(True)

    if m > 1:
        cross_step(0, range(1))
    bytes_of(reps_sq.at[pl.ds(0, reps - 1)], nr_send, nr_recv).wait_recv()
    total = reps_sq[0]
    for j in range(1, reps):
        total = total + reps_sq[j]
    pair_sq[x] = total
    norm_x().start()
    rolled(0, m, rest)
    if m > 1:
        cross_step(0, subs_all[1:])
    if m > 2:
        cross_step(1)
    norm_x().wait_recv()
    line_sq[p] = pair_sq[0] + pair_sq[1]

    @pl.when(jnp.logical_and(p == 0, m > 1))
    def _():
        pl.semaphore_wait(from_right, 1)

    @pl.when(jnp.logical_and(p == m - 1, m > 1))
    def _():
        pl.semaphore_wait(from_left, 1)

    span(1, m, lambda t: norm_z(t).start())
    span(2, m - 2, cross_step)
    line_step(m - 1)
    cross_b().start()

    @pl.when(p == m - 1)
    def _():
        cross_e().start()

    if m > 3:
        cross_step(m - 2)
    if m > 1:
        bytes_of(line_sq.at[pl.ds(0, m - 1)], nz_send, nz_recv).wait_recv()
    everything = line_sq[0]
    for j in range(1, m):
        everything = everything + line_sq[j]
    sq_out[...] = everything
    for copy in state[:3]:
        copy.wait()
    cross_step(m - 1)
    cross_b().wait_recv()
    mine = pl.ds(pl.multiple_of(x * line_rows, 8), line_rows)
    summed[cross_rows:] = pack_b[p, mine] + rx_b[...]

    @pl.when(p == m - 1)
    def _():
        cross_e().wait_recv()
        summed[extra] = pack_a[2 * p + x, extra] + rx_e[...]
        cross_e().wait_send()


    main, tail = pl.ds(0, kept_rows), pl.ds(kept_rows, extra_rows)
    bytes_of(rx_a.at[:, main], x_send, x_recv.at[0, 0]).wait_send()
    if m > 1:
        bytes_of(rx_a.at[pl.ds(0, m - 1), tail], xe_send, x_recv.at[0, 0]).wait_send()
        bytes_of(zin_a.at[pl.ds(0, m - 1), main], za_send, za_recv.at[0, 0]).wait_send()
        bytes_of(zin_b.at[pl.ds(0, m - 1)], zb_send, zb_recv.at[0, 0]).wait_send()
        bytes_of(line_sq.at[pl.ds(0, m - 1)], nz_send, nz_recv).wait_send()

        @pl.when(p == m - 1)
        def _():
            bytes_of(zin_a.at[pl.ds(0, m - 1), tail], zx_send, za_recv.at[0, 0]).wait_send()

        @pl.when(p < m - 1)
        def _():
            if m > 2:
                bytes_of(zin_a.at[pl.ds(0, m - 2), tail], zx_send, za_recv.at[0, 0]).wait_send()
            bytes_of(zin_e, ze_send, ze_recv.at[0]).wait_send()

    cross_b().wait_send()
    norm_x().wait_send()
    bytes_of(reps_sq.at[pl.ds(0, reps - 1)], nr_send, nr_recv).wait_send()


def update_kernel(n, total_rows, tokens, hot, *refs):
    blocks = refs[4].shape[1] // LANES
    dma = pltpu.SemaphoreType.DMA
    pl.run_scoped(
        functools.partial(update_body, n, total_rows, tokens, hot, *refs),
        dma, dma((3, blocks)), dma, dma,
    )


def update_body(
    n, total_rows, tokens, hot,
    ranks_any, summed, sq, kept, weight, moment, second,
    w_hbm, m_hbm, s_hbm, nc_hbm, sq_hbm,
    ranks, fresh, nc_sem, state_sem, sq_sem, ranks_sem,
):
    width = weight.shape[1]
    blocks = width // LANES
    outs = (w_hbm, m_hbm, s_hbm)
    copies = []

    def send(src, dst, sem):
        copies.append(pltpu.make_async_copy(src, dst, sem))
        copies[-1].start()

    order = pltpu.make_async_copy(ranks_any, ranks, ranks_sem)
    order.start()
    send(kept, nc_hbm.at[0], nc_sem)
    send(sq, sq_hbm, sq_sem)
    order.wait()
    block = [block_of(ranks, blocks, r) for r in range(blocks)]
    where = [pl.ds(pl.multiple_of(b * LANES, LANES), LANES) for b in block]
    for r in range(hot, blocks):
        for i, src in enumerate((weight, moment, second)):
            send(src.at[:, where[r]], outs[i].at[:, where[r]], state_sem.at[i, r])
    for r in range(hot):
        cols = slice(r * LANES, (r + 1) * LANES)
        rms = jnp.sqrt(sq[pl.ds(block[r], 1), :] / jnp.float32(total_rows * n * tokens))
        clip = 1.0 / jnp.maximum(jnp.float32(1.0), rms)
        grad = summed[:, cols] * clip / jnp.float32(n)
        moved = 0.9 * moment[:, where[r]] + 0.1 * grad
        squared = 0.95 * second[:, where[r]] + 0.05 * grad * grad
        fresh[1, :, cols] = moved
        fresh[2, :, cols] = squared
        step = 0.05 * (moved / (1.0 - 0.9**10)) / (
            jnp.sqrt(squared / (1.0 - 0.95**10)) + 1e-08
        )
        fresh[0, :, cols] = weight[:, where[r]] - step
        for i in range(3):
            send(fresh.at[i, :, pl.ds(r * LANES, LANES)], outs[i].at[:, where[r]], state_sem.at[i, r])
    for copy in copies:
        copy.wait()


def body(n, reps, features, out_grads, cold_sums, weight, moment, second, ranks):
    tokens, rows = features.shape
    width = out_grads.shape[1]
    blocks = ranks.shape[0]
    hot = blocks // 2
    packed = hot * LANES
    m = n // 2
    own = rows // n
    chunk = max(own, LANES)
    chunks = rows // chunk
    cross_rows, line_rows, pieces = split_of(own)
    extra_rows = pieces[-1][1]
    f32, bf16 = jnp.float32, jnp.bfloat16
    vmem = pl.BlockSpec(memory_space=pltpu.VMEM)
    hbm = pl.BlockSpec(memory_space=pl.ANY)
    summed, sq, kept, w, mo, se = pl.pallas_call(
        functools.partial(exchange_kernel, n, reps, hot),
        out_shape=(
            pltpu.VMEM((own, packed), f32),
            pltpu.VMEM((blocks, LANES), f32),
            pltpu.VMEM(cold_sums.shape[1:], bf16),
            pltpu.VMEM(weight.shape, f32),
            pltpu.VMEM(weight.shape, f32),
            pltpu.VMEM(weight.shape, f32),
        ),
        in_specs=[pl.BlockSpec(memory_space=pltpu.HBM)] * 7,
        out_specs=(vmem,) * 6,
        scratch_shapes=[
            pltpu.SMEM(ranks.shape, ranks.dtype),
            pltpu.VMEM((chunks, tokens, chunk), bf16),
            pltpu.VMEM((tokens, width), bf16),
            pltpu.VMEM((chunks, chunk, width), bf16),
            pltpu.VMEM((n, cross_rows, packed), f32),
            pltpu.VMEM((m, 2 * line_rows, packed), f32),
            pltpu.VMEM((m, cross_rows, packed), f32),
            pltpu.VMEM((line_rows, packed), f32),
            pltpu.VMEM((extra_rows, packed), f32),
            pltpu.VMEM((m + 1, cross_rows, packed), f32),
            pltpu.VMEM((m + 1, 2 * line_rows, packed), f32),
            pltpu.VMEM((2, extra_rows, packed), f32),
            pltpu.VMEM((blocks, 8, LANES), f32),
            pltpu.VMEM((reps, blocks, LANES), f32),
            pltpu.VMEM((2, blocks, LANES), f32),
            pltpu.VMEM((m, blocks, LANES), f32),
        ],
        compiler_params=pltpu.CompilerParams(
            collective_id=0, has_side_effects=True, vmem_limit_bytes=VMEM_GRANT
        ),
        name="exchange",
    )(ranks, features, out_grads, cold_sums, weight, moment, second)
    new_weight, new_moment, new_second, new_cold, column_sq = pl.pallas_call(
        functools.partial(update_kernel, n, rows * reps, tokens, hot),
        out_shape=(
            jax.ShapeDtypeStruct(weight.shape, f32),
            jax.ShapeDtypeStruct(weight.shape, f32),
            jax.ShapeDtypeStruct(weight.shape, f32),
            jax.ShapeDtypeStruct(cold_sums.shape, bf16),
            jax.ShapeDtypeStruct((blocks, LANES), f32),
        ),
        in_specs=[hbm] + [vmem] * 6,
        out_specs=(hbm,) * 5,
        scratch_shapes=[
            pltpu.SMEM(ranks.shape, ranks.dtype),
            pltpu.VMEM((3, weight.shape[0], packed), f32),
        ],
        compiler_params=pltpu.CompilerParams(vmem_limit_bytes=VMEM_GRANT // 2),
        name="update",
    )(ranks, summed, sq, kept, w, mo, se)
    return new_weight, new_moment, new_second, new_cold, column_sq.reshape(width)


def solution(mesh):
    owned = P(("rep", "dp"), None)
    placed = (P("dp", "rep"), P("dp", None), P("dp", "rep", None), owned, owned, owned, P())
    return jax.shard_map(
        functools.partial(body, mesh.shape["dp"], mesh.shape["rep"]),
        mesh=mesh,
        in_specs=placed,
        out_specs=(owned, owned, owned, P("dp", "rep", None), P()),
        check_vma=False,
    )
```

```python
import functools
import jax
import jax.numpy as jnp
from jax import lax
from jax.experimental import pallas as pl
from jax.experimental.pallas import tpu as pltpu
from jax.sharding import PartitionSpec as P

LANES = 128
GROUP = 32
EXTRA = 86
LAG = 0
FRONT = 6
VMEM_GRANT = 55 * 2**20
MESH = pl.DeviceIdType.MESH


def split_of(own):
    line = 8 * max(round(own / 48), 1)
    cross = own - line
    extra = 8 * max(round(own / EXTRA), 1)
    head = 8 * ((cross - extra + 8) // 16)
    if own > LANES:
        head = min(head, LANES - line)
    return cross, line, ((0, head), (head, cross - extra - head), (cross - extra, extra))


def block_of(ranks, blocks, rank):
    found = 0
    for b in range(blocks):
        gap = ranks[b] - rank
        found = found + b * (1 - jnp.minimum(gap * gap, 1))
    return found


def exchange_kernel(n, reps, hot, *refs):
    rows = refs[1].shape[1]
    own = rows // n
    chunks = rows // max(own, LANES)
    m = n // 2
    pieces = len(split_of(own)[2])
    dma = pltpu.SemaphoreType.DMA
    regular = pltpu.SemaphoreType.REGULAR
    pl.run_scoped(
        functools.partial(exchange_body, n, reps, hot, *refs),
        dma,
        dma,
        dma((m, pieces)),
        dma,
        dma,
        dma((2,)),
        dma,
        dma,
        dma,
        dma((m + 1, pieces)),
        dma,
        dma((m + 1, 2)),
        dma,
        dma,
        dma,
        dma,
        dma,
        dma,
        dma,
        dma,
        regular,
        regular,
        dma((2, chunks)),
        dma((5,)),
        dma((2, 2)),
    )


def exchange_body(
    n, reps, hot,
    ranks_hbm, feat, og, cold, weight, moment, second,
    summed, sq_out, kept, w_out, m_out, s_out,
    ranks, feat_v, og_v, cold_v, pack_a, pack_b, rx_a, rx_b, rx_e, zin_a, zin_b, zin_e, sq, reps_sq, pair_sq, line_sq,
    x_send, xe_send, x_recv, zx_send, ze_send, ze_recv, be_send, be_recv, za_send, za_recv, zb_send, zb_recv, b_send, b_recv,
    nr_send, nr_recv, nx_send, nx_recv, nz_send, nz_recv, from_left, from_right,
    in_sem, state_sem, first_sem,
):
    m = n // 2
    tokens = feat.shape[0]
    rows, width = cold.shape[1], cold.shape[2]
    blocks = width // LANES
    packed = hot * LANES
    own = rows // n
    chunk = max(own, LANES)
    chunks = rows // chunk
    inner = chunk // own
    cross_rows, line_rows, pieces = split_of(own)
    subs_all = range(len(pieces))
    kept_rows, extra_rows = pieces[-1]
    extra = slice(kept_rows, cross_rows)
    head_rows = pieces[0][1]
    me = lax.axis_index("dp")
    rep = lax.axis_index("rep")
    x = me % 2
    p = me // 2
    partner = me + 1 - 2 * x

    half = max(m // 2, 1)
    flip = p // half if m > 1 else 0
    pr = p + flip * (m - 1 - 2 * p)
    lone = m - 1 - 2 * pr

    def dest(k):
        late = (k - lone + 2 * m) // (2 * m)
        pair = late * (k - lone)
        odd = pair % 2
        near = (1 - late) * (m - 1 - k) + late * ((1 - odd) * (pair // 2) + odd * (2 * pr - pair // 2))
        return near + flip * (m - 1 - 2 * near)

    def chunk_at(i):
        if chunk != own:
            return i
        side = i % 2
        return 2 * dest(i // 2) + (1 - side) * (1 - x) + side * x

    def span(lo, hi, step):
        if hi - lo <= 8:
            for k in range(lo, hi):
                step(k)
        else:
            lax.fori_loop(lo, hi, lambda k, carry: step(k) or carry, 0)

    def rolled(lo, hi, step):
        lax.fori_loop(lo, hi, lambda k, carry: step(k) or carry, 0)

    barrier = pltpu.get_barrier_semaphore()

    def feat_copy(i):
        cols = pl.ds(pl.multiple_of(chunk_at(i) * chunk, LANES), chunk)
        return pltpu.make_async_copy(feat.at[:, cols], feat_v.at[i], in_sem.at[0, i])

    def cold_copy(i):
        at = pl.ds(pl.multiple_of(chunk_at(i) * chunk, LANES), chunk)
        return pltpu.make_async_copy(cold.at[0, at], cold_v.at[i], in_sem.at[1, i])

    state = [
        pltpu.make_async_copy(src, dst, state_sem.at[i])
        for i, (src, dst) in enumerate(
            ((weight, w_out), (moment, m_out), (second, s_out), (og, og_v), (ranks_hbm, ranks))
        )
    ]
    def fetch(i):
        feat_copy(i).start()
        cold_copy(i).start()

    early = LANES if chunk == own else chunk
    start = chunk_at(0) * chunk

    def first_feat(lo, hi):
        cols = pl.ds(pl.multiple_of(start + lo, LANES), hi - lo)
        return pltpu.make_async_copy(
            feat.at[:, cols], feat_v.at[0, :, pl.ds(lo, hi - lo)], first_sem.at[0, lo // early])

    def first_cold(lo, hi):
        at = pl.ds(pl.multiple_of(start + lo, LANES), hi - lo)
        return pltpu.make_async_copy(
            cold.at[0, at], cold_v.at[0, pl.ds(lo, hi - lo)], first_sem.at[1, lo // early])

    first_feat(0, early).start()
    state[3].start()
    first_cold(0, early).start()
    state[4].start()
    if early < chunk:
        first_feat(early, chunk).start()
        first_cold(early, chunk).start()
    pl.semaphore_signal(barrier, inc=1, device_id={"dp": partner}, device_id_type=MESH)

    @pl.when(p > 0)
    def _():
        pl.semaphore_signal(barrier, inc=1, device_id={"dp": me - 2}, device_id_type=MESH)

    @pl.when(p < m - 1)
    def _():
        pl.semaphore_signal(barrier, inc=1, device_id={"dp": me + 2}, device_id_type=MESH)

    span(1, reps, lambda t: pl.semaphore_signal(
        barrier, inc=1, device_id={"rep": (rep + t) % reps}, device_id_type=MESH))
    rolled(1, chunks, fetch)

    sq[...] = jnp.zeros_like(sq)

    def cross(k, sub):
        d = dest(k)
        at = pl.ds(*pieces[sub])
        return pltpu.make_async_remote_copy(
            src_ref=pack_a.at[2 * d + 1 - x, at], dst_ref=rx_a.at[d, at],
            send_sem=xe_send if sub == subs_all[-1] else x_send, recv_sem=x_recv.at[d, sub],
            device_id={"dp": partner}, device_id_type=MESH,
        )

    def start_cross(k, sub):
        if sub == subs_all[-1]:
            @pl.when(dest(k) != m - 1)
            def _():
                cross(k, sub).start()
        else:
            cross(k, sub).start()

    def along_a(d, sub, right):
        at = pl.ds(*pieces[sub])
        slot = d + 1 if right else d
        return pltpu.make_async_remote_copy(
            src_ref=pack_a.at[2 * d + x, at], dst_ref=zin_a.at[slot, at],
            send_sem=zx_send if sub == subs_all[-1] else za_send, recv_sem=za_recv.at[slot, sub],
            device_id={"dp": me + 2 if right else me - 2}, device_id_type=MESH,
        )

    def along_e(s):
        return pltpu.make_async_remote_copy(
            src_ref=pack_a.at[2 * (m - 1) + s, pl.ds(kept_rows, extra_rows)], dst_ref=zin_e.at[s],
            send_sem=ze_send, recv_sem=ze_recv.at[s],
            device_id={"dp": me + 2}, device_id_type=MESH,
        )

    def cross_e():
        return pltpu.make_async_remote_copy(
            src_ref=pack_a.at[2 * (m - 1) + 1 - x, pl.ds(kept_rows, extra_rows)], dst_ref=rx_e,
            send_sem=be_send, recv_sem=be_recv,
            device_id={"dp": partner}, device_id_type=MESH,
        )

    def along_b(d, s, right):
        slot = d + 1 if right else d
        at = pl.ds(pl.multiple_of(s * line_rows, 8), line_rows)
        return pltpu.make_async_remote_copy(
            src_ref=pack_b.at[d, at], dst_ref=zin_b.at[slot, at],
            send_sem=zb_send, recv_sem=zb_recv.at[slot, s],
            device_id={"dp": me + 2 if right else me - 2}, device_id_type=MESH,
        )

    def cross_b():
        return pltpu.make_async_remote_copy(
            src_ref=pack_b.at[p, pl.ds(pl.multiple_of((1 - x) * line_rows, 8), line_rows)],
            dst_ref=rx_b, send_sem=b_send, recv_sem=b_recv,
            device_id={"dp": partner}, device_id_type=MESH,
        )

    def norm_rep(t):
        return pltpu.make_async_remote_copy(
            src_ref=reps_sq.at[rep], dst_ref=reps_sq.at[rep], send_sem=nr_send, recv_sem=nr_recv,
            device_id={"rep": (rep + t) % reps}, device_id_type=MESH,
        )

    def norm_x():
        return pltpu.make_async_remote_copy(
            src_ref=pair_sq.at[x], dst_ref=pair_sq.at[x], send_sem=nx_send, recv_sem=nx_recv,
            device_id={"dp": partner}, device_id_type=MESH,
        )

    def norm_z(t):
        return pltpu.make_async_remote_copy(
            src_ref=line_sq.at[p], dst_ref=line_sq.at[p], send_sem=nz_send, recv_sem=nz_recv,
            device_id={"dp": 2 * ((p + t) % m) + x}, device_id_type=MESH,
        )

    def bytes_of(ref, send_sem, recv_sem):
        return pltpu.make_async_remote_copy(
            src_ref=ref, dst_ref=ref, send_sem=send_sem, recv_sem=recv_sem,
            device_id={"dp": partner}, device_id_type=MESH,
        )

    def token(right):
        pl.semaphore_signal(
            from_left if right else from_right, inc=1,
            device_id={"dp": me + 2 if right else me - 2}, device_id_type=MESH,
        )

    def raw_b(d, s):
        @pl.when(jnp.logical_and(d > p, p == 0))
        def _():
            along_b(d, s, True).start()

    def raw_e(d, s):
        @pl.when((d == m - 1) & (d > p) & (p == 0))
        def _():
            along_e(s).start()

        @pl.when(jnp.logical_and(d < p, p == m - 1))
        def _():
            along_b(d, s, False).start()

    def cross_step(k, subs=subs_all):
        d = dest(k)
        for sub in subs:
            if sub == subs_all[-1]:
                @pl.when(d != m - 1)
                def _():
                    cross_piece(k, d, sub)
            else:
                cross_piece(k, d, sub)

    def cross_piece(k, d, sub):
        at = slice(pieces[sub][0], sum(pieces[sub]))
        cross(k, sub).wait_recv()
        pack_a[2 * d + x, at] += rx_a[d, at]

        @pl.when(jnp.logical_and(d >= p, p > 0))
        def _():
            along_a(d, sub, True).wait_recv()
            pack_a[2 * d + x, at] += zin_a[d + 1, at]

        @pl.when(jnp.logical_and(d <= p, p < m - 1))
        def _():
            along_a(d, sub, False).wait_recv()
            pack_a[2 * d + x, at] += zin_a[d, at]

        @pl.when(d > p)
        def _():
            along_a(d, sub, True).start()

        @pl.when(d < p)
        def _():
            along_a(d, sub, False).start()

        @pl.when(d == p)
        def _():
            moved = line_rows if sub else 0
            summed[at.start + moved:at.stop + moved] = pack_a[2 * d + x, at]

    def product(i, first=0, last=chunk):
        return lax.dot_general(
            feat_v[i, :, first:last], og_v[...], (((0,), (0,)), ((), ())),
            preferred_element_type=jnp.float32,
        )

    def sums(i, grad, first, g):
        return [
            grad[g - first:g - first + GROUP, b * LANES:(b + 1) * LANES]
            + cold_v[i, g:g + GROUP, b * LANES:(b + 1) * LANES].astype(jnp.float32)
            for b in range(blocks)
        ]

    def fill_hot(i, values, g):
        c = chunk_at(i)
        for r in range(hot):
            cols = slice(r * LANES, (r + 1) * LANES)
            held = values[0]
            for b in range(1, blocks):
                held = jnp.where(ranks[b] == r, values[b], held)
            for h in range(0, GROUP, 8):
                owner = c * inner + (g + h) // own
                row = (g + h) % own
                if head_rows <= row < head_rows + line_rows:
                    to = pl.ds(pl.multiple_of((owner % 2) * line_rows + row - head_rows, 8), 8)
                    pack_b[owner // 2, to, cols] = held[h:h + 8]
                else:
                    row = row if row < head_rows else row - line_rows
                    pack_a[owner, row:row + 8, cols] = held[h:h + 8]

    def fill_cold(i, values, g, squares):
        at = pl.ds(pl.multiple_of(chunk_at(i) * chunk + g, 16), GROUP)
        for b in range(blocks):
            for h in range(0, GROUP, 8):
                squares[b] += values[b][h:h + 8] * values[b][h:h + 8]
            kept[at, b * LANES:(b + 1) * LANES] = jnp.where(
                ranks[b] < hot, jnp.zeros_like(values[b]), values[b]).astype(jnp.bfloat16)

    def fill(i, grad, first=0, last=chunk, hot_rows=True, cold_rows=True):
        squares = [sq[b] for b in range(blocks)]
        for g in range(first, last, GROUP):
            values = sums(i, grad, first, g)
            if cold_rows:
                fill_cold(i, values, g, squares)
            if hot_rows:
                fill_hot(i, values, g)
        if cold_rows:
            for b in range(blocks):
                sq[b] = squares[b]

    def step(i):
        feat_copy(i).wait()
        cold_copy(i).wait()
        fill(i, product(i))
        if chunk == own:
            send_cross(i)
            raw_b(dest(i // 2), chunk_at(i) % 2)
            raw_e(dest(i // 2), chunk_at(i) % 2)

    def send_cross(i):
        k = (i - lag) // 2
        for sub in subs_all:
            @pl.when((i >= lag) & ((i - lag) % 2 == 0) & (k * len(pieces) + sub < FRONT))
            def _():
                start_cross(k, sub)

    state[4].wait()
    state[3].wait()
    first_feat(0, early).wait()
    first_cold(0, early).wait()
    grad = product(0, 0, early)
    fill(0, grad, 0, early, cold_rows=False)
    greeted = (p + m - 1) // m + (2 * m - 2 - p) // m + 1 + (reps - 1)
    pl.semaphore_wait(barrier, greeted)

    @pl.when(jnp.logical_and(p == 0, m > 1))
    def _():
        token(True)

    @pl.when(jnp.logical_and(p == m - 1, m > 1))
    def _():
        token(False)

    lag = rep % 2 * LAG
    if chunk == own:
        ready = [sub for sub in subs_all if sum(pieces[sub]) <= early]
        rest_of = [sub for sub in subs_all if sum(pieces[sub]) > early]

        def start_early(subs):
            @pl.when(lag == 0)
            def _():
                for sub in subs:
                    start_cross(0, sub)

        start_early(ready)
        raw_b(dest(0), 1 - x)
    fill(0, grad, 0, early, hot_rows=False)
    if chunk == own:
        if early < chunk:
            first_feat(early, chunk).wait()
            first_cold(early, chunk).wait()
            fill(0, product(0, early, chunk), early, chunk)
        start_early(rest_of)
        raw_e(dest(0), 1 - x)
    rolled(1, chunks, step)
    for copy in state[:3]:
        copy.start()
    if chunk != own:
        def launch(k):
            for sub in subs_all:
                @pl.when(k * len(pieces) + sub < FRONT)
                def _():
                    start_cross(k, sub)
            for s in range(2):
                raw_b(dest(k), s)
                raw_e(dest(k), s)

        rolled(0, m, launch)
    for r in range(blocks):
        reps_sq[rep, r:r + 1] = jnp.sum(sq[r], axis=0, keepdims=True)
    span(1, reps, lambda t: norm_rep(t).start())

    def line_step(k):
        d = dest(k)
        for s in range(2):
            at = slice(s * line_rows, (s + 1) * line_rows)

            @pl.when(jnp.logical_and(d >= p, p > 0))
            def _():
                along_b(d, s, True).wait_recv()
                pack_b[d, at] += zin_b[d + 1, at]

            @pl.when(jnp.logical_and(d <= p, p < m - 1))
            def _():
                along_b(d, s, False).wait_recv()
                pack_b[d, at] += zin_b[d, at]

            @pl.when(jnp.logical_and(d > p, p > 0))
            def _():
                along_b(d, s, True).start()

            @pl.when(jnp.logical_and(d < p, p < m - 1))
            def _():
                along_b(d, s, False).start()

            @pl.when((d == m - 1) & (p > 0))
            def _():
                along_e(s).wait_recv()
                pack_a[2 * d + s, extra] += zin_e[s]

            @pl.when((d == m - 1) & (p > 0) & (p < m - 1))
            def _():
                along_e(s).start()

    def rest(k):
        for sub in subs_all:
            @pl.when(k * len(pieces) + sub >= FRONT)
            def _():
                start_cross(k, sub)

    span(0, m - 1, line_step)

    @pl.when(jnp.logical_and(p > 0, p < m - 1))
    def _():
        pl.semaphore_wait(from_right, 1)
        token(False)
        pl.semaphore_wait(from_left, 1)
        token(True)

    if m > 1:
        cross_step(0, range(1))
    bytes_of(reps_sq.at[pl.ds(0, reps - 1)], nr_send, nr_recv).wait_recv()
    total = reps_sq[0]
    for j in range(1, reps):
        total = total + reps_sq[j]
    pair_sq[x] = total
    norm_x().start()
    rolled(0, m, rest)
    if m > 1:
        cross_step(0, subs_all[1:])
    if m > 2:
        cross_step(1)
    norm_x().wait_recv()
    line_sq[p] = pair_sq[0] + pair_sq[1]

    @pl.when(jnp.logical_and(p == 0, m > 1))
    def _():
        pl.semaphore_wait(from_right, 1)

    @pl.when(jnp.logical_and(p == m - 1, m > 1))
    def _():
        pl.semaphore_wait(from_left, 1)

    span(1, m, lambda t: norm_z(t).start())
    span(2, m - 2, cross_step)
    line_step(m - 1)
    cross_b().start()

    @pl.when(p == m - 1)
    def _():
        cross_e().start()

    if m > 3:
        cross_step(m - 2)
    if m > 1:
        bytes_of(line_sq.at[pl.ds(0, m - 1)], nz_send, nz_recv).wait_recv()
    everything = line_sq[0]
    for j in range(1, m):
        everything = everything + line_sq[j]
    sq_out[...] = everything
    for copy in state[:3]:
        copy.wait()
    cross_step(m - 1)
    cross_b().wait_recv()
    mine = pl.ds(pl.multiple_of(x * line_rows, 8), line_rows)
    summed[head_rows:head_rows + line_rows] = pack_b[p, mine] + rx_b[...]

    @pl.when(p == m - 1)
    def _():
        cross_e().wait_recv()
        summed[own - extra_rows:] = pack_a[2 * p + x, extra] + rx_e[...]
        cross_e().wait_send()


    main, tail = pl.ds(0, kept_rows), pl.ds(kept_rows, extra_rows)
    bytes_of(rx_a.at[:, main], x_send, x_recv.at[0, 0]).wait_send()
    if m > 1:
        bytes_of(rx_a.at[pl.ds(0, m - 1), tail], xe_send, x_recv.at[0, 0]).wait_send()
        bytes_of(zin_a.at[pl.ds(0, m - 1), main], za_send, za_recv.at[0, 0]).wait_send()
        bytes_of(zin_b.at[pl.ds(0, m - 1)], zb_send, zb_recv.at[0, 0]).wait_send()
        bytes_of(line_sq.at[pl.ds(0, m - 1)], nz_send, nz_recv).wait_send()

        @pl.when(p == m - 1)
        def _():
            bytes_of(zin_a.at[pl.ds(0, m - 1), tail], zx_send, za_recv.at[0, 0]).wait_send()

        @pl.when(p < m - 1)
        def _():
            if m > 2:
                bytes_of(zin_a.at[pl.ds(0, m - 2), tail], zx_send, za_recv.at[0, 0]).wait_send()
            bytes_of(zin_e, ze_send, ze_recv.at[0]).wait_send()

    cross_b().wait_send()
    norm_x().wait_send()
    bytes_of(reps_sq.at[pl.ds(0, reps - 1)], nr_send, nr_recv).wait_send()


def update_kernel(n, total_rows, tokens, hot, *refs):
    blocks = refs[4].shape[1] // LANES
    dma = pltpu.SemaphoreType.DMA
    pl.run_scoped(
        functools.partial(update_body, n, total_rows, tokens, hot, *refs),
        dma, dma((3, blocks)), dma, dma,
    )


def update_body(
    n, total_rows, tokens, hot,
    ranks_any, summed, sq, kept, weight, moment, second,
    w_hbm, m_hbm, s_hbm, nc_hbm, sq_hbm,
    ranks, fresh, nc_sem, state_sem, sq_sem, ranks_sem,
):
    width = weight.shape[1]
    blocks = width // LANES
    outs = (w_hbm, m_hbm, s_hbm)
    copies = []

    def send(src, dst, sem):
        copies.append(pltpu.make_async_copy(src, dst, sem))
        copies[-1].start()

    order = pltpu.make_async_copy(ranks_any, ranks, ranks_sem)
    order.start()
    send(kept, nc_hbm.at[0], nc_sem)
    send(sq, sq_hbm, sq_sem)
    order.wait()
    block = [block_of(ranks, blocks, r) for r in range(blocks)]
    where = [pl.ds(pl.multiple_of(b * LANES, LANES), LANES) for b in block]
    for r in range(hot, blocks):
        for i, src in enumerate((weight, moment, second)):
            send(src.at[:, where[r]], outs[i].at[:, where[r]], state_sem.at[i, r])
    for r in range(hot):
        cols = slice(r * LANES, (r + 1) * LANES)
        rms = jnp.sqrt(sq[pl.ds(block[r], 1), :] / jnp.float32(total_rows * n * tokens))
        clip = 1.0 / jnp.maximum(jnp.float32(1.0), rms)
        grad = summed[:, cols] * clip / jnp.float32(n)
        moved = 0.9 * moment[:, where[r]] + 0.1 * grad
        squared = 0.95 * second[:, where[r]] + 0.05 * grad * grad
        fresh[1, :, cols] = moved
        fresh[2, :, cols] = squared
        step = 0.05 * (moved / (1.0 - 0.9**10)) / (
            jnp.sqrt(squared / (1.0 - 0.95**10)) + 1e-08
        )
        fresh[0, :, cols] = weight[:, where[r]] - step
        for i in range(3):
            send(fresh.at[i, :, pl.ds(r * LANES, LANES)], outs[i].at[:, where[r]], state_sem.at[i, r])
    for copy in copies:
        copy.wait()


def body(n, reps, features, out_grads, cold_sums, weight, moment, second, ranks):
    tokens, rows = features.shape
    width = out_grads.shape[1]
    blocks = ranks.shape[0]
    hot = blocks // 2
    packed = hot * LANES
    m = n // 2
    own = rows // n
    chunk = max(own, LANES)
    chunks = rows // chunk
    cross_rows, line_rows, pieces = split_of(own)
    extra_rows = pieces[-1][1]
    f32, bf16 = jnp.float32, jnp.bfloat16
    vmem = pl.BlockSpec(memory_space=pltpu.VMEM)
    hbm = pl.BlockSpec(memory_space=pl.ANY)
    summed, sq, kept, w, mo, se = pl.pallas_call(
        functools.partial(exchange_kernel, n, reps, hot),
        out_shape=(
            pltpu.VMEM((own, packed), f32),
            pltpu.VMEM((blocks, LANES), f32),
            pltpu.VMEM(cold_sums.shape[1:], bf16),
            pltpu.VMEM(weight.shape, f32),
            pltpu.VMEM(weight.shape, f32),
            pltpu.VMEM(weight.shape, f32),
        ),
        in_specs=[pl.BlockSpec(memory_space=pltpu.HBM)] * 7,
        out_specs=(vmem,) * 6,
        scratch_shapes=[
            pltpu.SMEM(ranks.shape, ranks.dtype),
            pltpu.VMEM((chunks, tokens, chunk), bf16),
            pltpu.VMEM((tokens, width), bf16),
            pltpu.VMEM((chunks, chunk, width), bf16),
            pltpu.VMEM((n, cross_rows, packed), f32),
            pltpu.VMEM((m, 2 * line_rows, packed), f32),
            pltpu.VMEM((m, cross_rows, packed), f32),
            pltpu.VMEM((line_rows, packed), f32),
            pltpu.VMEM((extra_rows, packed), f32),
            pltpu.VMEM((m + 1, cross_rows, packed), f32),
            pltpu.VMEM((m + 1, 2 * line_rows, packed), f32),
            pltpu.VMEM((2, extra_rows, packed), f32),
            pltpu.VMEM((blocks, 8, LANES), f32),
            pltpu.VMEM((reps, blocks, LANES), f32),
            pltpu.VMEM((2, blocks, LANES), f32),
            pltpu.VMEM((m, blocks, LANES), f32),
        ],
        compiler_params=pltpu.CompilerParams(
            collective_id=0, has_side_effects=True, vmem_limit_bytes=VMEM_GRANT
        ),
        name="exchange",
    )(ranks, features, out_grads, cold_sums, weight, moment, second)
    new_weight, new_moment, new_second, new_cold, column_sq = pl.pallas_call(
        functools.partial(update_kernel, n, rows * reps, tokens, hot),
        out_shape=(
            jax.ShapeDtypeStruct(weight.shape, f32),
            jax.ShapeDtypeStruct(weight.shape, f32),
            jax.ShapeDtypeStruct(weight.shape, f32),
            jax.ShapeDtypeStruct(cold_sums.shape, bf16),
            jax.ShapeDtypeStruct((blocks, LANES), f32),
        ),
        in_specs=[hbm] + [vmem] * 6,
        out_specs=(hbm,) * 5,
        scratch_shapes=[
            pltpu.SMEM(ranks.shape, ranks.dtype),
            pltpu.VMEM((3, weight.shape[0], packed), f32),
        ],
        compiler_params=pltpu.CompilerParams(vmem_limit_bytes=VMEM_GRANT // 2),
        name="update",
    )(ranks, summed, sq, kept, w, mo, se)
    return new_weight, new_moment, new_second, new_cold, column_sq.reshape(width)


def solution(mesh):
    owned = P(("rep", "dp"), None)
    placed = (P("dp", "rep"), P("dp", None), P("dp", "rep", None), owned, owned, owned, P())
    return jax.shard_map(
        functools.partial(body, mesh.shape["dp"], mesh.shape["rep"]),
        mesh=mesh,
        in_specs=placed,
        out_specs=(owned, owned, owned, P("dp", "rep", None), P()),
        check_vma=False,
    )
```

```python
import functools
import jax
import jax.numpy as jnp
from jax import lax
from jax.experimental import pallas as pl
from jax.experimental.pallas import tpu as pltpu
from jax.sharding import PartitionSpec as P

LANES = 128
GROUP = 32
EXTRA = 64
LAG = 0
FRONT = 6
VMEM_GRANT = 55 * 2**20
MESH = pl.DeviceIdType.MESH


def split_of(own):
    line = 8 * max(round(own / 48), 1)
    cross = own - line
    extra = 8 * max(round(own / EXTRA), 1)
    head = 8 * ((cross - extra + 8) // 16)
    if own > LANES:
        head = min(head, LANES - line)
    return cross, line, ((0, head), (head, cross - extra - head), (cross - extra, extra))


def block_of(ranks, blocks, rank):
    found = 0
    for b in range(blocks):
        gap = ranks[b] - rank
        found = found + b * (1 - jnp.minimum(gap * gap, 1))
    return found


def exchange_kernel(n, reps, hot, *refs):
    rows = refs[1].shape[1]
    own = rows // n
    chunks = rows // max(own, LANES)
    m = n // 2
    pieces = len(split_of(own)[2])
    dma = pltpu.SemaphoreType.DMA
    regular = pltpu.SemaphoreType.REGULAR
    pl.run_scoped(
        functools.partial(exchange_body, n, reps, hot, *refs),
        dma,
        dma,
        dma((m, pieces)),
        dma,
        dma,
        dma((2,)),
        dma,
        dma,
        dma,
        dma((m + 1, pieces)),
        dma,
        dma((m + 1, 2)),
        dma,
        dma,
        dma,
        dma,
        dma,
        dma,
        dma,
        dma,
        regular,
        regular,
        dma((2, chunks)),
        dma((5,)),
        dma((2, 2)),
    )


def exchange_body(
    n, reps, hot,
    ranks_hbm, feat, og, cold, weight, moment, second,
    summed, sq_out, kept, w_out, m_out, s_out,
    ranks, feat_v, og_v, cold_v, pack_a, pack_b, rx_a, rx_b, rx_e, zin_a, zin_b, zin_e, sq, reps_sq, pair_sq, line_sq,
    x_send, xe_send, x_recv, zx_send, ze_send, ze_recv, be_send, be_recv, za_send, za_recv, zb_send, zb_recv, b_send, b_recv,
    nr_send, nr_recv, nx_send, nx_recv, nz_send, nz_recv, from_left, from_right,
    in_sem, state_sem, first_sem,
):
    m = n // 2
    tokens = feat.shape[0]
    rows, width = cold.shape[1], cold.shape[2]
    blocks = width // LANES
    packed = hot * LANES
    own = rows // n
    chunk = max(own, LANES)
    chunks = rows // chunk
    inner = chunk // own
    cross_rows, line_rows, pieces = split_of(own)
    subs_all = range(len(pieces))
    kept_rows, extra_rows = pieces[-1]
    extra = slice(kept_rows, cross_rows)
    head_rows = pieces[0][1]
    me = lax.axis_index("dp")
    rep = lax.axis_index("rep")
    x = me % 2
    p = me // 2
    partner = me + 1 - 2 * x

    half = max(m // 2, 1)
    flip = p // half if m > 1 else 0
    pr = p + flip * (m - 1 - 2 * p)
    lone = m - 1 - 2 * pr

    def dest(k):
        late = (k - lone + 2 * m) // (2 * m)
        pair = late * (k - lone)
        odd = pair % 2
        near = (1 - late) * (m - 1 - k) + late * ((1 - odd) * (pair // 2) + odd * (2 * pr - pair // 2))
        return near + flip * (m - 1 - 2 * near)

    def chunk_at(i):
        if chunk != own:
            return i
        side = i % 2
        return 2 * dest(i // 2) + (1 - side) * (1 - x) + side * x

    def span(lo, hi, step):
        if hi - lo <= 8:
            for k in range(lo, hi):
                step(k)
        else:
            lax.fori_loop(lo, hi, lambda k, carry: step(k) or carry, 0)

    def rolled(lo, hi, step):
        lax.fori_loop(lo, hi, lambda k, carry: step(k) or carry, 0)

    barrier = pltpu.get_barrier_semaphore()

    def feat_copy(i):
        cols = pl.ds(pl.multiple_of(chunk_at(i) * chunk, LANES), chunk)
        return pltpu.make_async_copy(feat.at[:, cols], feat_v.at[i], in_sem.at[0, i])

    def cold_copy(i):
        at = pl.ds(pl.multiple_of(chunk_at(i) * chunk, LANES), chunk)
        return pltpu.make_async_copy(cold.at[0, at], cold_v.at[i], in_sem.at[1, i])

    state = [
        pltpu.make_async_copy(src, dst, state_sem.at[i])
        for i, (src, dst) in enumerate(
            ((weight, w_out), (moment, m_out), (second, s_out), (og, og_v), (ranks_hbm, ranks))
        )
    ]
    def fetch(i):
        feat_copy(i).start()
        cold_copy(i).start()

    early = LANES if chunk == own else chunk
    start = chunk_at(0) * chunk

    def first_feat(lo, hi):
        cols = pl.ds(pl.multiple_of(start + lo, LANES), hi - lo)
        return pltpu.make_async_copy(
            feat.at[:, cols], feat_v.at[0, :, pl.ds(lo, hi - lo)], first_sem.at[0, lo // early])

    def first_cold(lo, hi):
        at = pl.ds(pl.multiple_of(start + lo, LANES), hi - lo)
        return pltpu.make_async_copy(
            cold.at[0, at], cold_v.at[0, pl.ds(lo, hi - lo)], first_sem.at[1, lo // early])

    first_feat(0, early).start()
    state[3].start()
    first_cold(0, early).start()
    state[4].start()
    if early < chunk:
        first_feat(early, chunk).start()
        first_cold(early, chunk).start()
    pl.semaphore_signal(barrier, inc=1, device_id={"dp": partner}, device_id_type=MESH)

    @pl.when(p > 0)
    def _():
        pl.semaphore_signal(barrier, inc=1, device_id={"dp": me - 2}, device_id_type=MESH)

    @pl.when(p < m - 1)
    def _():
        pl.semaphore_signal(barrier, inc=1, device_id={"dp": me + 2}, device_id_type=MESH)

    span(1, reps, lambda t: pl.semaphore_signal(
        barrier, inc=1, device_id={"rep": (rep + t) % reps}, device_id_type=MESH))
    rolled(1, chunks, fetch)

    sq[...] = jnp.zeros_like(sq)

    def cross(k, sub):
        d = dest(k)
        at = pl.ds(*pieces[sub])
        return pltpu.make_async_remote_copy(
            src_ref=pack_a.at[2 * d + 1 - x, at], dst_ref=rx_a.at[d, at],
            send_sem=xe_send if sub == subs_all[-1] else x_send, recv_sem=x_recv.at[d, sub],
            device_id={"dp": partner}, device_id_type=MESH,
        )

    def start_cross(k, sub):
        if sub == subs_all[-1]:
            @pl.when(dest(k) != m - 1)
            def _():
                cross(k, sub).start()
        else:
            cross(k, sub).start()

    def along_a(d, sub, right):
        at = pl.ds(*pieces[sub])
        slot = d + 1 if right else d
        return pltpu.make_async_remote_copy(
            src_ref=pack_a.at[2 * d + x, at], dst_ref=zin_a.at[slot, at],
            send_sem=zx_send if sub == subs_all[-1] else za_send, recv_sem=za_recv.at[slot, sub],
            device_id={"dp": me + 2 if right else me - 2}, device_id_type=MESH,
        )

    def along_e(s):
        return pltpu.make_async_remote_copy(
            src_ref=pack_a.at[2 * (m - 1) + s, pl.ds(kept_rows, extra_rows)], dst_ref=zin_e.at[s],
            send_sem=ze_send, recv_sem=ze_recv.at[s],
            device_id={"dp": me + 2}, device_id_type=MESH,
        )

    def cross_e():
        return pltpu.make_async_remote_copy(
            src_ref=pack_a.at[2 * (m - 1) + 1 - x, pl.ds(kept_rows, extra_rows)], dst_ref=rx_e,
            send_sem=be_send, recv_sem=be_recv,
            device_id={"dp": partner}, device_id_type=MESH,
        )

    def along_b(d, s, right):
        slot = d + 1 if right else d
        at = pl.ds(pl.multiple_of(s * line_rows, 8), line_rows)
        return pltpu.make_async_remote_copy(
            src_ref=pack_b.at[d, at], dst_ref=zin_b.at[slot, at],
            send_sem=zb_send, recv_sem=zb_recv.at[slot, s],
            device_id={"dp": me + 2 if right else me - 2}, device_id_type=MESH,
        )

    def cross_b():
        return pltpu.make_async_remote_copy(
            src_ref=pack_b.at[p, pl.ds(pl.multiple_of((1 - x) * line_rows, 8), line_rows)],
            dst_ref=rx_b, send_sem=b_send, recv_sem=b_recv,
            device_id={"dp": partner}, device_id_type=MESH,
        )

    def norm_rep(t):
        return pltpu.make_async_remote_copy(
            src_ref=reps_sq.at[rep], dst_ref=reps_sq.at[rep], send_sem=nr_send, recv_sem=nr_recv,
            device_id={"rep": (rep + t) % reps}, device_id_type=MESH,
        )

    def norm_x():
        return pltpu.make_async_remote_copy(
            src_ref=pair_sq.at[x], dst_ref=pair_sq.at[x], send_sem=nx_send, recv_sem=nx_recv,
            device_id={"dp": partner}, device_id_type=MESH,
        )

    def norm_z(t):
        return pltpu.make_async_remote_copy(
            src_ref=line_sq.at[p], dst_ref=line_sq.at[p], send_sem=nz_send, recv_sem=nz_recv,
            device_id={"dp": 2 * ((p + t) % m) + x}, device_id_type=MESH,
        )

    def bytes_of(ref, send_sem, recv_sem):
        return pltpu.make_async_remote_copy(
            src_ref=ref, dst_ref=ref, send_sem=send_sem, recv_sem=recv_sem,
            device_id={"dp": partner}, device_id_type=MESH,
        )

    def token(right):
        pl.semaphore_signal(
            from_left if right else from_right, inc=1,
            device_id={"dp": me + 2 if right else me - 2}, device_id_type=MESH,
        )

    def raw_b(d, s):
        @pl.when(jnp.logical_and(d > p, p == 0))
        def _():
            along_b(d, s, True).start()

    def raw_e(d, s):
        @pl.when((d == m - 1) & (d > p) & (p == 0))
        def _():
            along_e(s).start()

        @pl.when(jnp.logical_and(d < p, p == m - 1))
        def _():
            along_b(d, s, False).start()

    def cross_step(k, subs=subs_all):
        d = dest(k)
        for sub in subs:
            if sub == subs_all[-1]:
                @pl.when(d != m - 1)
                def _():
                    cross_piece(k, d, sub)
            else:
                cross_piece(k, d, sub)

    def cross_piece(k, d, sub):
        at = slice(pieces[sub][0], sum(pieces[sub]))
        cross(k, sub).wait_recv()
        pack_a[2 * d + x, at] += rx_a[d, at]

        @pl.when(jnp.logical_and(d >= p, p > 0))
        def _():
            along_a(d, sub, True).wait_recv()
            pack_a[2 * d + x, at] += zin_a[d + 1, at]

        @pl.when(jnp.logical_and(d <= p, p < m - 1))
        def _():
            along_a(d, sub, False).wait_recv()
            pack_a[2 * d + x, at] += zin_a[d, at]

        @pl.when(d > p)
        def _():
            along_a(d, sub, True).start()

        @pl.when(d < p)
        def _():
            along_a(d, sub, False).start()

        @pl.when(d == p)
        def _():
            moved = line_rows if sub else 0
            summed[at.start + moved:at.stop + moved] = pack_a[2 * d + x, at]

    def product(i, first=0, last=chunk):
        return lax.dot_general(
            feat_v[i, :, first:last], og_v[...], (((0,), (0,)), ((), ())),
            preferred_element_type=jnp.float32,
        )

    def sums(i, grad, first, g):
        return [
            grad[g - first:g - first + GROUP, b * LANES:(b + 1) * LANES]
            + cold_v[i, g:g + GROUP, b * LANES:(b + 1) * LANES].astype(jnp.float32)
            for b in range(blocks)
        ]

    def fill_hot(i, values, g):
        c = chunk_at(i)
        for r in range(hot):
            cols = slice(r * LANES, (r + 1) * LANES)
            held = values[0]
            for b in range(1, blocks):
                held = jnp.where(ranks[b] == r, values[b], held)
            for h in range(0, GROUP, 8):
                owner = c * inner + (g + h) // own
                row = (g + h) % own
                if head_rows <= row < head_rows + line_rows:
                    to = pl.ds(pl.multiple_of((owner % 2) * line_rows + row - head_rows, 8), 8)
                    pack_b[owner // 2, to, cols] = held[h:h + 8]
                else:
                    row = row if row < head_rows else row - line_rows
                    pack_a[owner, row:row + 8, cols] = held[h:h + 8]

    def fill_cold(i, values, g, squares):
        at = pl.ds(pl.multiple_of(chunk_at(i) * chunk + g, 16), GROUP)
        for b in range(blocks):
            for h in range(0, GROUP, 8):
                squares[b] += values[b][h:h + 8] * values[b][h:h + 8]
            kept[at, b * LANES:(b + 1) * LANES] = jnp.where(
                ranks[b] < hot, jnp.zeros_like(values[b]), values[b]).astype(jnp.bfloat16)

    def fill(i, grad, first=0, last=chunk, hot_rows=True, cold_rows=True):
        squares = [sq[b] for b in range(blocks)]
        for g in range(first, last, GROUP):
            values = sums(i, grad, first, g)
            if cold_rows:
                fill_cold(i, values, g, squares)
            if hot_rows:
                fill_hot(i, values, g)
        if cold_rows:
            for b in range(blocks):
                sq[b] = squares[b]

    def step(i):
        feat_copy(i).wait()
        cold_copy(i).wait()
        fill(i, product(i))
        if chunk == own:
            send_cross(i)
            raw_b(dest(i // 2), chunk_at(i) % 2)
            raw_e(dest(i // 2), chunk_at(i) % 2)

    def send_cross(i):
        k = (i - lag) // 2
        for sub in subs_all:
            @pl.when((i >= lag) & ((i - lag) % 2 == 0) & (k * len(pieces) + sub < FRONT))
            def _():
                start_cross(k, sub)

    state[4].wait()
    state[3].wait()
    first_feat(0, early).wait()
    first_cold(0, early).wait()
    grad = product(0, 0, early)
    fill(0, grad, 0, early, cold_rows=False)
    greeted = (p + m - 1) // m + (2 * m - 2 - p) // m + 1 + (reps - 1)
    pl.semaphore_wait(barrier, greeted)

    @pl.when(jnp.logical_and(p == 0, m > 1))
    def _():
        token(True)

    @pl.when(jnp.logical_and(p == m - 1, m > 1))
    def _():
        token(False)

    lag = rep % 2 * LAG
    if chunk == own:
        ready = [sub for sub in subs_all if sum(pieces[sub]) <= early]
        rest_of = [sub for sub in subs_all if sum(pieces[sub]) > early]

        def start_early(subs):
            @pl.when(lag == 0)
            def _():
                for sub in subs:
                    start_cross(0, sub)

        start_early(ready)
        raw_b(dest(0), 1 - x)
    fill(0, grad, 0, early, hot_rows=False)
    if chunk == own:
        if early < chunk:
            first_feat(early, chunk).wait()
            first_cold(early, chunk).wait()
            fill(0, product(0, early, chunk), early, chunk)
        start_early(rest_of)
        raw_e(dest(0), 1 - x)
    rolled(1, chunks, step)
    for copy in state[:3]:
        copy.start()
    if chunk != own:
        def launch(k):
            for sub in subs_all:
                @pl.when(k * len(pieces) + sub < FRONT)
                def _():
                    start_cross(k, sub)
            for s in range(2):
                raw_b(dest(k), s)
                raw_e(dest(k), s)

        rolled(0, m, launch)
    for r in range(blocks):
        reps_sq[rep, r:r + 1] = jnp.sum(sq[r], axis=0, keepdims=True)
    span(1, reps, lambda t: norm_rep(t).start())

    def line_step(k):
        d = dest(k)
        for s in range(2):
            at = slice(s * line_rows, (s + 1) * line_rows)

            @pl.when(jnp.logical_and(d >= p, p > 0))
            def _():
                along_b(d, s, True).wait_recv()
                pack_b[d, at] += zin_b[d + 1, at]

            @pl.when(jnp.logical_and(d <= p, p < m - 1))
            def _():
                along_b(d, s, False).wait_recv()
                pack_b[d, at] += zin_b[d, at]

            @pl.when(jnp.logical_and(d > p, p > 0))
            def _():
                along_b(d, s, True).start()

            @pl.when(jnp.logical_and(d < p, p < m - 1))
            def _():
                along_b(d, s, False).start()

            @pl.when((d == m - 1) & (p > 0))
            def _():
                along_e(s).wait_recv()
                pack_a[2 * d + s, extra] += zin_e[s]

            @pl.when((d == m - 1) & (p > 0) & (p < m - 1))
            def _():
                along_e(s).start()

    def rest(k):
        for sub in subs_all:
            @pl.when(k * len(pieces) + sub >= FRONT)
            def _():
                start_cross(k, sub)

    span(0, m - 1, line_step)

    @pl.when(jnp.logical_and(p > 0, p < m - 1))
    def _():
        pl.semaphore_wait(from_right, 1)
        token(False)
        pl.semaphore_wait(from_left, 1)
        token(True)

    if m > 1:
        cross_step(0, range(1))
    bytes_of(reps_sq.at[pl.ds(0, reps - 1)], nr_send, nr_recv).wait_recv()
    total = reps_sq[0]
    for j in range(1, reps):
        total = total + reps_sq[j]
    pair_sq[x] = total
    norm_x().start()
    rolled(0, m, rest)
    if m > 1:
        cross_step(0, subs_all[1:])
    if m > 2:
        cross_step(1)
    norm_x().wait_recv()
    line_sq[p] = pair_sq[0] + pair_sq[1]

    @pl.when(jnp.logical_and(p == 0, m > 1))
    def _():
        pl.semaphore_wait(from_right, 1)

    @pl.when(jnp.logical_and(p == m - 1, m > 1))
    def _():
        pl.semaphore_wait(from_left, 1)

    span(1, m, lambda t: norm_z(t).start())
    span(2, m - 2, cross_step)
    line_step(m - 1)
    cross_b().start()

    @pl.when(p == m - 1)
    def _():
        cross_e().start()

    if m > 3:
        cross_step(m - 2)
    if m > 1:
        bytes_of(line_sq.at[pl.ds(0, m - 1)], nz_send, nz_recv).wait_recv()
    everything = line_sq[0]
    for j in range(1, m):
        everything = everything + line_sq[j]
    sq_out[...] = everything
    for copy in state[:3]:
        copy.wait()
    cross_step(m - 1)
    cross_b().wait_recv()
    mine = pl.ds(pl.multiple_of(x * line_rows, 8), line_rows)
    summed[head_rows:head_rows + line_rows] = pack_b[p, mine] + rx_b[...]

    @pl.when(p == m - 1)
    def _():
        cross_e().wait_recv()
        summed[own - extra_rows:] = pack_a[2 * p + x, extra] + rx_e[...]
        cross_e().wait_send()


    main, tail = pl.ds(0, kept_rows), pl.ds(kept_rows, extra_rows)
    bytes_of(rx_a.at[:, main], x_send, x_recv.at[0, 0]).wait_send()
    if m > 1:
        bytes_of(rx_a.at[pl.ds(0, m - 1), tail], xe_send, x_recv.at[0, 0]).wait_send()
        bytes_of(zin_a.at[pl.ds(0, m - 1), main], za_send, za_recv.at[0, 0]).wait_send()
        bytes_of(zin_b.at[pl.ds(0, m - 1)], zb_send, zb_recv.at[0, 0]).wait_send()
        bytes_of(line_sq.at[pl.ds(0, m - 1)], nz_send, nz_recv).wait_send()

        @pl.when(p == m - 1)
        def _():
            bytes_of(zin_a.at[pl.ds(0, m - 1), tail], zx_send, za_recv.at[0, 0]).wait_send()

        @pl.when(p < m - 1)
        def _():
            if m > 2:
                bytes_of(zin_a.at[pl.ds(0, m - 2), tail], zx_send, za_recv.at[0, 0]).wait_send()
            bytes_of(zin_e, ze_send, ze_recv.at[0]).wait_send()

    cross_b().wait_send()
    norm_x().wait_send()
    bytes_of(reps_sq.at[pl.ds(0, reps - 1)], nr_send, nr_recv).wait_send()


def update_kernel(n, total_rows, tokens, hot, *refs):
    blocks = refs[4].shape[1] // LANES
    dma = pltpu.SemaphoreType.DMA
    pl.run_scoped(
        functools.partial(update_body, n, total_rows, tokens, hot, *refs),
        dma, dma((3, blocks)), dma, dma,
    )


def update_body(
    n, total_rows, tokens, hot,
    ranks_any, summed, sq, kept, weight, moment, second,
    w_hbm, m_hbm, s_hbm, nc_hbm, sq_hbm,
    ranks, fresh, nc_sem, state_sem, sq_sem, ranks_sem,
):
    width = weight.shape[1]
    blocks = width // LANES
    outs = (w_hbm, m_hbm, s_hbm)
    copies = []

    def send(src, dst, sem):
        copies.append(pltpu.make_async_copy(src, dst, sem))
        copies[-1].start()

    order = pltpu.make_async_copy(ranks_any, ranks, ranks_sem)
    order.start()
    send(kept, nc_hbm.at[0], nc_sem)
    send(sq, sq_hbm, sq_sem)
    order.wait()
    block = [block_of(ranks, blocks, r) for r in range(blocks)]
    where = [pl.ds(pl.multiple_of(b * LANES, LANES), LANES) for b in block]
    for r in range(hot, blocks):
        for i, src in enumerate((weight, moment, second)):
            send(src.at[:, where[r]], outs[i].at[:, where[r]], state_sem.at[i, r])
    for r in range(hot):
        cols = slice(r * LANES, (r + 1) * LANES)
        rms = jnp.sqrt(sq[pl.ds(block[r], 1), :] / jnp.float32(total_rows * n * tokens))
        clip = 1.0 / jnp.maximum(jnp.float32(1.0), rms)
        grad = summed[:, cols] * clip / jnp.float32(n)
        moved = 0.9 * moment[:, where[r]] + 0.1 * grad
        squared = 0.95 * second[:, where[r]] + 0.05 * grad * grad
        fresh[1, :, cols] = moved
        fresh[2, :, cols] = squared
        step = 0.05 * (moved / (1.0 - 0.9**10)) / (
            jnp.sqrt(squared / (1.0 - 0.95**10)) + 1e-08
        )
        fresh[0, :, cols] = weight[:, where[r]] - step
        for i in range(3):
            send(fresh.at[i, :, pl.ds(r * LANES, LANES)], outs[i].at[:, where[r]], state_sem.at[i, r])
    for copy in copies:
        copy.wait()


def body(n, reps, features, out_grads, cold_sums, weight, moment, second, ranks):
    tokens, rows = features.shape
    width = out_grads.shape[1]
    blocks = ranks.shape[0]
    hot = blocks // 2
    packed = hot * LANES
    m = n // 2
    own = rows // n
    chunk = max(own, LANES)
    chunks = rows // chunk
    cross_rows, line_rows, pieces = split_of(own)
    extra_rows = pieces[-1][1]
    f32, bf16 = jnp.float32, jnp.bfloat16
    vmem = pl.BlockSpec(memory_space=pltpu.VMEM)
    hbm = pl.BlockSpec(memory_space=pl.ANY)
    summed, sq, kept, w, mo, se = pl.pallas_call(
        functools.partial(exchange_kernel, n, reps, hot),
        out_shape=(
            pltpu.VMEM((own, packed), f32),
            pltpu.VMEM((blocks, LANES), f32),
            pltpu.VMEM(cold_sums.shape[1:], bf16),
            pltpu.VMEM(weight.shape, f32),
            pltpu.VMEM(weight.shape, f32),
            pltpu.VMEM(weight.shape, f32),
        ),
        in_specs=[pl.BlockSpec(memory_space=pltpu.HBM)] * 7,
        out_specs=(vmem,) * 6,
        scratch_shapes=[
            pltpu.SMEM(ranks.shape, ranks.dtype),
            pltpu.VMEM((chunks, tokens, chunk), bf16),
            pltpu.VMEM((tokens, width), bf16),
            pltpu.VMEM((chunks, chunk, width), bf16),
            pltpu.VMEM((n, cross_rows, packed), f32),
            pltpu.VMEM((m, 2 * line_rows, packed), f32),
            pltpu.VMEM((m, cross_rows, packed), f32),
            pltpu.VMEM((line_rows, packed), f32),
            pltpu.VMEM((extra_rows, packed), f32),
            pltpu.VMEM((m + 1, cross_rows, packed), f32),
            pltpu.VMEM((m + 1, 2 * line_rows, packed), f32),
            pltpu.VMEM((2, extra_rows, packed), f32),
            pltpu.VMEM((blocks, 8, LANES), f32),
            pltpu.VMEM((reps, blocks, LANES), f32),
            pltpu.VMEM((2, blocks, LANES), f32),
            pltpu.VMEM((m, blocks, LANES), f32),
        ],
        compiler_params=pltpu.CompilerParams(
            collective_id=0, has_side_effects=True, vmem_limit_bytes=VMEM_GRANT
        ),
        name="exchange",
    )(ranks, features, out_grads, cold_sums, weight, moment, second)
    new_weight, new_moment, new_second, new_cold, column_sq = pl.pallas_call(
        functools.partial(update_kernel, n, rows * reps, tokens, hot),
        out_shape=(
            jax.ShapeDtypeStruct(weight.shape, f32),
            jax.ShapeDtypeStruct(weight.shape, f32),
            jax.ShapeDtypeStruct(weight.shape, f32),
            jax.ShapeDtypeStruct(cold_sums.shape, bf16),
            jax.ShapeDtypeStruct((blocks, LANES), f32),
        ),
        in_specs=[hbm] + [vmem] * 6,
        out_specs=(hbm,) * 5,
        scratch_shapes=[
            pltpu.SMEM(ranks.shape, ranks.dtype),
            pltpu.VMEM((3, weight.shape[0], packed), f32),
        ],
        compiler_params=pltpu.CompilerParams(vmem_limit_bytes=VMEM_GRANT // 2),
        name="update",
    )(ranks, summed, sq, kept, w, mo, se)
    return new_weight, new_moment, new_second, new_cold, column_sq.reshape(width)


def solution(mesh):
    owned = P(("rep", "dp"), None)
    placed = (P("dp", "rep"), P("dp", None), P("dp", "rep", None), owned, owned, owned, P())
    return jax.shard_map(
        functools.partial(body, mesh.shape["dp"], mesh.shape["rep"]),
        mesh=mesh,
        in_specs=placed,
        out_specs=(owned, owned, owned, P("dp", "rep", None), P()),
        check_vma=False,
    )
```
